32 devices in a mesh: section: 2 (over core), dp: 4 (over z), tensor: 4 (over y, x).
Axes of the slice: x: 2, y: 2, z: 4, core: 2. Of those that a mesh axis runs over, the one named last changes fastest.
Arguments:
- tokens: bfloat16 [2, 4, 2048, 1024], P(None, 'dp', 'tensor'), may hold values from -6 to 6
- cotangent: bfloat16 [2, 4, 2048, 1024], P(None, 'dp', 'tensor'), may hold values from -6 to 6
- doc_ids: int32 [2, 4, 2048], P(None, 'dp'), may hold values from 0 to 3, never falling along the last dimension, each value on 1 to 1024 neighbouring positions
- global_flags: int32 [2, 4, 32], P(None, 'dp'), may hold values from 0 to 2047, as said below
- w_attn: bfloat16 [2, 1024, 6, 1024], P('section', None, None, 'tensor'), may hold values from -1 to 1
- w_out: bfloat16 [2, 1024, 1024], P('section', 'tensor'), may hold values from -0.75 to 0.75
- w_up: bfloat16 [2, 1024, 4096], P('section', None, 'tensor'), may hold values from -0.1875 to 0.1875
- w_down: bfloat16 [2, 4096, 1024], P('section', 'tensor'), may hold values from -0.125 to 0.125
- ln_gain: float32 [2, 2, 1024], P('section'), may hold values from 0.5 to 1.5
- ln_bias: float32 [2, 2, 1024], P('section'), may hold values from -1.5 to 1.5
Outputs:
- layer_out: bfloat16 [2, 2, 4, 2048, 1024], P('section', None, 'dp', 'tensor')
- input_grad: bfloat16 [2, 2, 4, 2048, 1024], P('section', None, 'dp', 'tensor')
- grad_w_attn: float32 [2, 1024, 6, 1024], P('section', None, None, 'tensor')
- grad_w_out: float32 [2, 1024, 1024], P('section', 'tensor')
- grad_w_up: float32 [2, 1024, 4096], P('section', None, 'tensor')
- grad_w_down: float32 [2, 4096, 1024], P('section', 'tensor')
- grad_ln_gain: float32 [2, 2, 1024], P('section')
- grad_ln_bias: float32 [2, 2, 1024], P('section')
- clipped_qk: float32 [2, 1024, 4, 1024], P('section', None, None, 'tensor')
The draws below stay inside these ranges and needn't reach their ends.
Inputs may be any that keep to these rules, and one draw needn't show every extreme that they name: `doc_ids`: ids never fall along a sequence. `global_flags`: the 32 positions of a sequence are distinct and rise.
All inputs are finite; a program needn't handle non-finite values.
Results may differ from the reference program's by a relative error of at most 0.03.
Values may be sent and summed in bfloat16 or wider, within the bound.
No kernel may reach another device: no remote copies, remote signals or barrier semaphores. Data moves between devices by JAX's collectives and lax.ppermute only.
A program may use at most 320 MiB of HBM per device.

```python
import math
import jax
import jax.numpy as jnp
import numpy as np
from jax import lax

D = 1024
HEADS = 16
HEAD = 64
FF = 4096
HALF = 512
QBLOCK = 512
GLOBS = 32
SEQ_LEN = 2048
MICRO = 2
LAYERS = 2
SEQS = 4


def draw_w_attn(key, part):
    normal_part = jax.random.truncated_normal(key, -2.5, 2.5, (LAYERS, D, 6, D), jnp.float32) * D ** (-0.5)
    spread = jnp.exp(jax.random.uniform(jax.random.fold_in(key, 11), (LAYERS, 1, 2, HEADS, 1), jnp.float32, 0.0, math.log(3.0)))
    per_column = jnp.broadcast_to(spread, (LAYERS, 1, 2, HEADS, HEAD)).reshape(LAYERS, 1, 2, D)
    unit_scale = jnp.ones((LAYERS, 1, D), jnp.float32)
    factor = jnp.stack([per_column[:, :, 0], unit_scale, unit_scale, per_column[:, :, 1], unit_scale, unit_scale], 2)
    return (normal_part * factor).astype(jnp.bfloat16)


def draw_global_flags(key, part):
    ranks = jax.random.randint(key, (MICRO, SEQS, SEQ_LEN), 0, 1 << 16, jnp.int32)
    scores = ranks * SEQ_LEN + jnp.arange(SEQ_LEN, dtype=jnp.int32)
    chosen = lax.top_k(scores, GLOBS)[1]
    return jnp.sort(chosen, -1).astype(jnp.int32)


def level_of(key, dims, shards, smallest, high):
    factor_of, own = 1.0, jax.random.fold_in(key, 6)
    for position, blocks in shards:
        steps = jnp.exp(jax.random.uniform(jax.random.fold_in(own, position), (blocks,), jnp.float32, smallest / len(shards), high / len(shards)))
        factor_of = factor_of * jnp.repeat(steps, dims[position] // blocks).reshape([-1 if axis == position else 1 for axis in range(len(dims))])
    return factor_of


def profile(amount, total, reach, skew):
    weights = [(1 << 20) // math.isqrt(grade ** skew) + 1 for grade in range(2, amount + 1)]
    rest, counts = total - reach - (amount - 1), [1] * (amount - 1)
    while rest > 0:
        movable = [i for i in range(amount - 1) if counts[i] < reach]
        pool, left = sum([weights[i] for i in movable]), rest
        for i in movable:
            more = min(reach - counts[i], max(1, left * weights[i] // pool), rest)
            counts[i] = counts[i] + more
            rest = rest - more
    return np.array([reach] + counts)


def uneven(stream_key, number_of, total, bound, lean):
    if number_of == 2:
        one = jax.random.randint(stream_key, (), max(1, total - bound), min(bound, total - 1) + 1)
        return jnp.stack([one, total - one])
    sizes = jnp.asarray(profile(number_of, total, bound, lean), jnp.int32)
    twos = (number_of - 1) // 2
    donor, taker = sizes[1:1 + 2 * twos:2], sizes[2:2 + 2 * twos:2]
    margin = jnp.minimum(donor - 1, bound - taker)
    shifted = jax.random.randint(jax.random.fold_in(stream_key, 1), (twos,), 0, 1 << 20) % (margin + 1)
    sizes = sizes.at[1:1 + 2 * twos:2].set(donor - shifted).at[2:2 + 2 * twos:2].set(taker + shifted)
    return sizes[jax.random.permutation(jax.random.fold_in(stream_key, 2), number_of)]


def normal_values(stream_key, shape, deviation, reach, pieces=(), kind=jnp.bfloat16):
    values = jax.random.normal(stream_key, shape, jnp.float32) * deviation
    if len(pieces) > 0:
        values = level_of(stream_key, shape, pieces, -0.22, 0.18) * values
    return jnp.clip(values, min=-reach, max=reach).astype(kind)


def setup_inputs(seed: int = 0) -> dict:
    streams_of = jax.random.split(jax.random.key(seed), 11)
    return {
        "tokens": normal_values(streams_of[0], (MICRO, SEQS, SEQ_LEN, D), 1.0, 6.0, ((1, 4), (2, 4))),
        "cotangent": normal_values(streams_of[1], (MICRO, SEQS, SEQ_LEN, D), 1.0, 6.0, ((1, 4), (2, 4))),
        "doc_ids": jax.vmap(lambda own: jnp.searchsorted(jnp.cumsum(uneven(own, 4, SEQ_LEN, SEQ_LEN // 2, 0)), jnp.arange(SEQ_LEN), side="right"))(jax.random.split(streams_of[2], MICRO * SEQS)).reshape((MICRO, SEQS, SEQ_LEN)).astype(jnp.int32),
        "global_flags": draw_global_flags(jax.random.fold_in(streams_of[10], 71), 0),
        "w_attn": draw_w_attn(jax.random.fold_in(streams_of[10], 71), 0),
        "w_out": normal_values(streams_of[5], (LAYERS, D, D), (D // 16) ** -0.5, 0.75, ((0, 2), (1, 4))),
        "w_up": normal_values(streams_of[6], (LAYERS, D, FF), D ** -0.5, 0.1875, ((0, 2), (2, 4))),
        "w_down": normal_values(streams_of[7], (LAYERS, FF, D), (FF // 2) ** -0.5, 0.125, ((0, 2), (1, 4))),
        "ln_gain": jnp.clip(1.0 + 0.1 * jax.random.normal(streams_of[8], (LAYERS, 2, D), jnp.float32), 0.5, 1.5),
        "ln_bias": normal_values(streams_of[9], (LAYERS, 2, D), 0.3, 1.5, ((0, 2),), jnp.float32),
    }


@jax.custom_vjp
def low(v):
    return lax.optimization_barrier(v.astype(jnp.bfloat16)).astype(jnp.float32)

@jax.custom_vjp
def low_back(v):
    return v

def low_keep(v):
    return (low(v), None)

def low_pass(kept, grad):
    return (grad,)

def back_keep(v):
    return (v, None)

def back_low(kept, grad):
    return (low(grad),)
low.defvjp(low_keep, low_pass)
low_back.defvjp(back_keep, back_low)
masked_fill = -1e+30
clip_limit = 10.0
highest = lax.Precision.HIGHEST

def layer_norm(resid, gain, shift):
    centred = resid - lax.optimization_barrier(jnp.mean(resid, -1, keepdims=True))
    spread = lax.optimization_barrier(jnp.mean(centred * centred, -1, keepdims=True))
    return centred * lax.rsqrt(spread + 1e-05) * gain + shift

def global_rows(positions):
    return jnp.any(positions[:, None] == jnp.arange(SEQ_LEN, dtype=jnp.int32)[None, :], 0)

def block_masks(first_row, docs_row, glob_row):
    rows = first_row + jnp.arange(QBLOCK, dtype=jnp.int32)
    cols = jnp.arange(SEQ_LEN, dtype=jnp.int32)
    row_docs = lax.dynamic_slice_in_dim(docs_row, first_row, QBLOCK, 0)
    same_doc = row_docs[:, None] == docs_row[None, :]
    near = jnp.abs(rows[:, None] - cols[None, :]) <= HALF
    local_mask = same_doc & (near | glob_row[None, :])
    row_glob = lax.dynamic_slice_in_dim(glob_row, first_row, QBLOCK, 0)
    return (local_mask, same_doc, row_glob)

def attention_ref(parts, docs_row, glob_row):
    score_scale = HEAD ** (-0.5)
    starts = jnp.arange(SEQ_LEN // QBLOCK, dtype=jnp.int32) * QBLOCK

    def one_block(first_row):
        local_mask, same_doc, row_glob = block_masks(first_row, docs_row, glob_row)
        query_rows = lax.dynamic_slice_in_dim(parts, first_row, QBLOCK, 0)
        results = []
        for branch, key_mask in ((0, local_mask), (3, same_doc)):
            scores = low_back(jnp.einsum('qhe,khe->hqk', query_rows[:, branch], parts[:, branch + 1], precision=highest) * score_scale)
            masked = jnp.where(key_mask[None], scores, masked_fill)
            row_max = lax.optimization_barrier(jnp.max(masked, -1, keepdims=True))
            exponent = jnp.exp(masked - row_max)
            attn_probs = low(exponent / lax.optimization_barrier(jnp.sum(exponent, -1, keepdims=True)))
            context = jnp.einsum('hqk,khe->qhe', attn_probs, parts[:, branch + 2], precision=highest)
            results.append((context, row_max[..., 0]))
        (local_ctx, local_max), (global_ctx, global_max) = results
        context = jnp.where(row_glob[:, None, None], global_ctx, local_ctx)
        peak_logits = jnp.stack([lax.optimization_barrier(jnp.max(local_max, -1)), lax.optimization_barrier(jnp.max(jnp.where(row_glob[None, :], global_max, masked_fill), -1))])
        return (context, peak_logits)
    context, peak_logits = lax.map(jax.checkpoint(one_block), starts)
    return (context.reshape(SEQ_LEN, D), lax.optimization_barrier(jnp.max(peak_logits, 0)))

def layer_fn(layer_in, attn_w, out_w, up_w, down_w, gains, shifts, docs_row, glob_row):
    projected = low_back(low(jnp.einsum('ld,dke->lke', layer_in, attn_w, precision=highest)))
    parts = projected.reshape(SEQ_LEN, 6, HEADS, HEAD)
    context, peak_logits = attention_ref(parts, docs_row, glob_row)
    context = low_back(low(context))
    attn_branch = low_back(jnp.dot(context, out_w, precision=highest, preferred_element_type=jnp.float32))
    hidden = layer_norm(layer_in + attn_branch, gains[0], shifts[0])
    up_value = low_back(jnp.dot(low(hidden), up_w, precision=highest, preferred_element_type=jnp.float32))
    activated = low(jax.nn.gelu(up_value, approximate=False))
    mlp_branch = low_back(jnp.dot(activated, down_w, precision=highest, preferred_element_type=jnp.float32))
    return (layer_norm(hidden + mlp_branch, gains[1], shifts[1]), peak_logits)

def sequence_fn(params, seq_in, seq_probe, docs_row, flags_row):
    attn_w, out_w, up_w, down_w, gains, shifts = params
    glob_row = global_rows(flags_row)
    current = seq_in
    kept_outs = []
    peak_list = []
    final_out = current
    for layer_index in range(LAYERS):
        layer_in = low_back(current) + seq_probe[layer_index]
        result, peak_logits = layer_fn(layer_in, attn_w[layer_index], out_w[layer_index], up_w[layer_index], down_w[layer_index], gains[layer_index], shifts[layer_index], docs_row, glob_row)
        peak_list.append(peak_logits)
        if layer_index + 1 < LAYERS:
            current = low(result)
            kept_outs.append(current)
        else:
            final_out = result
    return (final_out, jnp.stack(kept_outs), jnp.stack(peak_list))

def reference(tokens, cotangent, doc_ids, global_flags, w_attn, w_out, w_up, w_down, ln_gain, ln_bias):
    seq_count = MICRO * SEQS
    inputs = tokens.astype(jnp.float32).reshape(seq_count, SEQ_LEN, D)
    docs_all = doc_ids.reshape(seq_count, SEQ_LEN).astype(jnp.int32)
    flags_all = global_flags.reshape(seq_count, GLOBS).astype(jnp.int32)
    params = tuple((item.astype(jnp.float32) for item in (w_attn, w_out, w_up, w_down, ln_gain, ln_bias)))
    probes = jnp.zeros((seq_count, LAYERS, SEQ_LEN, D), jnp.float32)
    sequence = jax.checkpoint(sequence_fn)

    def whole(weights, probe_all):

        def one_seq(carry, items):
            seq_in, seq_probe, docs_row, flags_row = items
            final_out, kept_outs, peak_logits = sequence(weights, seq_in, seq_probe, docs_row, flags_row)
            return (carry, (final_out, kept_outs, peak_logits))
        _, (finals, kept_outs, peak_logits) = lax.scan(one_seq, jnp.zeros((), jnp.float32), (inputs, probe_all, docs_all, flags_all))
        return (finals, (kept_outs, peak_logits))
    finals, back_fn, (kept_outs, peak_logits) = jax.vjp(whole, params, probes, has_aux=True)
    grads, probe_grads = back_fn(cotangent.astype(jnp.float32).reshape(seq_count, SEQ_LEN, D))
    layer_out = jnp.concatenate([kept_outs.transpose(1, 0, 2, 3), finals[None]], 0)
    layer_out = layer_out.reshape(LAYERS, MICRO, SEQS, SEQ_LEN, D).astype(jnp.bfloat16)
    input_grad = probe_grads.transpose(1, 0, 2, 3).reshape(LAYERS, MICRO, SEQS, SEQ_LEN, D).astype(jnp.bfloat16)
    peaks_all = lax.optimization_barrier(jnp.max(peak_logits, 0))
    factors = jnp.sqrt(clip_limit / jnp.maximum(peaks_all, clip_limit))
    columns = jnp.repeat(factors, HEAD, axis=2)
    attn_full = params[0]
    clipped_qk = jnp.stack([attn_full[:, :, 0] * columns[:, 0][:, None, :], attn_full[:, :, 1] * columns[:, 0][:, None, :], attn_full[:, :, 3] * columns[:, 1][:, None, :], attn_full[:, :, 4] * columns[:, 1][:, None, :]], 2)
    return (layer_out, input_grad, grads[0], grads[1], grads[2], grads[3], grads[4], grads[5], clipped_qk)
```

```python
import math
from functools import partial

import jax
import jax.numpy as jnp
from jax import lax
from jax.experimental import pallas as pl
from jax.experimental.pallas import tpu as pltpu
from jax.sharding import PartitionSpec as P

HEAD = 64
HALF = 512
QTILE = 256
KTILE = 256
VMEM_BYTES = 56 * 1024 * 1024

masked_fill = -1e30
clip_limit = 10.0
score_scale = HEAD ** (-0.5)

NN = (((1,), (0,)), ((), ()))
NT = (((1,), (1,)), ((), ()))
TN = (((0,), (0,)), ((), ()))


def mm(left, right, dims=NN, out=jnp.float32):
    return lax.dot_general(left, right, dims, preferred_element_type=jnp.float32).astype(out)


def tile_bias(first_key, first_query, key_docs, query_docs, keys, queries):
    key_pos = first_key + lax.broadcasted_iota(jnp.int32, (keys, queries), 0)
    query_pos = first_query + lax.broadcasted_iota(jnp.int32, (keys, queries), 1)
    gap = jnp.abs(key_pos - query_pos)
    return jnp.where((key_docs == query_docs) & (gap <= HALF), 0.0, masked_fill)


def far_bias(glob_pos, first_query, glob_docs, query_docs, globs, queries):
    query_pos = first_query + lax.broadcasted_iota(jnp.int32, (globs, queries), 1)
    gap = jnp.abs(glob_pos - query_pos)
    return jnp.where((glob_docs == query_docs) & (gap > HALF), 0.0, masked_fill)


def one_hot_rows(glob_pos, length):
    globs = glob_pos.shape[0]
    hit = lax.broadcasted_iota(jnp.int32, (globs, length), 1) == glob_pos
    return jnp.where(hit, 1.0, 0.0).astype(jnp.bfloat16)


def true_unit(place, order_ref, plan):
    inner, parts, _ = plan
    part, rest = place // (2 * inner), place % (2 * inner)
    side = (rest % 2) ^ order_ref[0]
    lane = (rest // 2) ^ order_ref[1]
    return (side * inner + lane) * parts + part


def local_unit(unit, order_ref, plan):
    inner, parts, _ = plan
    block, part = lax.div(unit, parts), lax.rem(unit, parts)
    side = lax.div(block, inner) ^ order_ref[0]
    lane = lax.rem(block, inner) ^ order_ref[1]
    return part * (2 * inner) + lane * 2 + side


def join_pieces(order_ref, pieces, joined_ref, sems, plan):
    rows = plan[2]
    copies = []
    place = 0
    for piece in pieces:
        for index in range(piece.shape[0] // rows):
            start = pl.multiple_of(true_unit(place, order_ref, plan) * rows, rows)
            copies.append(
                pltpu.make_async_copy(
                    piece.at[pl.ds(index * rows, rows), :],
                    joined_ref.at[pl.ds(start, rows), :],
                    sems.at[place],
                )
            )
            place += 1
    for copy in copies:
        copy.start()
    for copy in copies:
        copy.wait()


def store_local(out_ref, tile, cols, value, order_ref, plan):
    rows = plan[2]
    size = min(rows, value.shape[0])
    for index in range(value.shape[0] // size):
        row = tile * value.shape[0] + index * size
        place = local_unit(lax.div(row, rows), order_ref, plan)
        start = pl.multiple_of(place * rows + lax.rem(row, rows), size)
        out_ref[pl.ds(start, size), cols] = value[index * size : (index + 1) * size]


def diagonal_sum(blocks, heads, rows):
    owner = lax.broadcasted_iota(jnp.int32, (rows, heads * HEAD), 1) // HEAD
    total = jnp.zeros((rows, heads * HEAD), jnp.float32)
    for head in range(heads):
        total = total + jnp.where(owner == head, blocks[head * rows : (head + 1) * rows], 0.0)
    return total


def attend_kernel(
    heads,
    plan,
    count,
    order_ref,
    first_ref,
    last_ref,
    *refs,
):
    pieces, refs = refs[:count], refs[count:]
    attend_body(heads, plan, order_ref, first_ref, last_ref, pieces, *refs)


def attend_body(
    heads,
    plan,
    order_ref,
    first_ref,
    last_ref,
    pieces,
    doc_row_ref,
    doc_col_ref,
    pos_col_ref,
    gdoc_col_ref,
    gdoc_row_ref,
    ctx_ref,
    lse_ref,
    glse_ref,
    peak_ref,
    gpeak_ref,
    proj,
    values_t,
    hot,
    far_keys,
    far_values_t,
    gctx_t,
    gstack,
    gscores,
    wide,
    acc,
    top,
    total,
    sems,
):
    length = proj.shape[0]
    width = heads * HEAD
    globs = pos_col_ref.shape[0]
    step = pl.program_id(0)

    @pl.when(step == 0)
    def _():
        join_pieces(order_ref, pieces, proj, sems, plan)
        wide[...] = jnp.zeros_like(wide)
        gstack[...] = jnp.zeros_like(gstack)
        hot[...] = one_hot_rows(pos_col_ref[...], length)
        hot_all = hot[...]
        far_keys[...] = mm(hot_all, proj[:, width : 2 * width], out=jnp.bfloat16)
        far_values_t[...] = mm(hot_all, proj[:, 2 * width : 3 * width]).T.astype(jnp.bfloat16)
        queries = (mm(hot_all, proj[:, 3 * width : 4 * width]) * score_scale).astype(jnp.bfloat16)
        for head in range(heads):
            cols = slice(head * HEAD, (head + 1) * HEAD)
            gstack[head * globs : (head + 1) * globs, cols] = queries[:, cols]

        def score_tile(tile, best):
            rows = pl.ds(pl.multiple_of(tile * KTILE, KTILE), KTILE)
            values_t[:, rows] = proj[rows, 2 * width : 3 * width].T
            scores = mm(proj[rows, 4 * width : 5 * width], gstack[...], NT)
            scores = jnp.where(doc_col_ref[rows, :] == gdoc_row_ref[...], scores, masked_fill)
            gscores[rows, :] = scores
            return jnp.maximum(best, jnp.max(scores, 0, keepdims=True))

        best = lax.fori_loop(
            0, length // KTILE, score_tile, jnp.full((1, heads * globs), masked_fill, jnp.float32)
        )

        def sum_tile(tile, sums):
            rows = pl.ds(pl.multiple_of(tile * KTILE, KTILE), KTILE)
            weights = jnp.exp(gscores[rows, :] - best)
            gscores[rows, :] = weights
            return sums + jnp.sum(weights, 0, keepdims=True)

        sums = lax.fori_loop(
            0, length // KTILE, sum_tile, jnp.zeros((1, heads * globs), jnp.float32)
        )

        def value_tile(tile, blocks):
            rows = pl.ds(pl.multiple_of(tile * KTILE, KTILE), KTILE)
            probs = (gscores[rows, :] / sums).T.astype(jnp.bfloat16)
            return blocks + mm(probs, proj[rows, 5 * width : 6 * width])

        blocks = lax.fori_loop(
            0, length // KTILE, value_tile, jnp.zeros((heads * globs, width), jnp.float32)
        )
        gctx_t[...] = diagonal_sum(blocks, heads, globs).T.astype(jnp.bfloat16)
        glse_ref[...] = best + jnp.log(sums)
        gpeak_ref[...] = best

    start = pl.multiple_of(step * QTILE, QTILE)
    query_rows = pl.ds(start, QTILE)
    query_t = proj[query_rows, 0:width].T * score_scale
    for head in range(heads):
        rows = slice(head * HEAD, (head + 1) * HEAD)
        wide[rows, head * QTILE : (head + 1) * QTILE] = query_t[rows].astype(jnp.bfloat16)
    query_docs = doc_row_ref[:, query_rows]

    scores = mm(far_keys[...], wide[...])
    bias = far_bias(pos_col_ref[...], start, gdoc_col_ref[...], query_docs, globs, QTILE)
    for head in range(heads):
        cols = slice(head * QTILE, (head + 1) * QTILE)
        rows = slice(head * HEAD, (head + 1) * HEAD)
        part = scores[:, cols] + bias
        best = jnp.max(part, 0, keepdims=True)
        weights = jnp.exp(part - best)
        top[:, cols] = best
        total[:, cols] = jnp.sum(weights, 0, keepdims=True)
        acc[rows, :] = mm(far_values_t[rows, :], weights.astype(jnp.bfloat16))

    def key_tile(tile, carry):
        key_start = pl.multiple_of(tile * KTILE, KTILE)
        keys = pl.ds(key_start, KTILE)
        scores = mm(proj[keys, width : 2 * width], wide[...])
        bias = tile_bias(key_start, start, doc_col_ref[keys, :], query_docs, KTILE, QTILE)
        for head in range(heads):
            cols = slice(head * QTILE, (head + 1) * QTILE)
            rows = slice(head * HEAD, (head + 1) * HEAD)
            part = scores[:, cols] + bias
            old = top[:, cols]
            best = jnp.maximum(old, jnp.max(part, 0, keepdims=True))
            weights = jnp.exp(part - best)
            shrink = jnp.exp(old - best)
            top[:, cols] = best
            total[:, cols] = total[:, cols] * shrink + jnp.sum(weights, 0, keepdims=True)
            acc[rows, :] = acc[rows, :] * shrink + mm(
                values_t[rows, keys], weights.astype(jnp.bfloat16)
            )
        return carry

    lax.fori_loop(first_ref[step], last_ref[step], key_tile, 0)

    hot_tile = hot[:, query_rows]
    is_glob = jnp.max(hot_tile.astype(jnp.float32), 0, keepdims=True) > 0.5
    for head in range(heads):
        cols = slice(head * QTILE, (head + 1) * QTILE)
        rows = slice(head * HEAD, (head + 1) * HEAD)
        acc[rows, :] = acc[rows, :] / total[:, cols]
        lse_ref[head : head + 1, :] = top[:, cols] + jnp.log(total[:, cols])
    merged = jnp.where(is_glob, mm(gctx_t[...], hot_tile), acc[...])
    store_local(ctx_ref, step, slice(None), merged.T.astype(jnp.bfloat16), order_ref, plan)

    @pl.when(step == 0)
    def _():
        peak_ref[...] = top[...]

    @pl.when(step > 0)
    def _():
        peak_ref[...] = jnp.maximum(peak_ref[...], top[...])


def whole_block(shape):
    return pl.BlockSpec(shape, lambda *_: (0,) * len(shape), pipeline_mode=pl.Buffered(1))


def attend(proj, info, plan):
    length = sum(piece.shape[0] for piece in proj)
    columns = proj[0].shape[1]
    heads = columns // (6 * HEAD)
    width = heads * HEAD
    order, first, last, doc_row, doc_col, pos_col, gdoc_col, gdoc_row, _ = info
    globs = pos_col.shape[0]
    tiles = length // QTILE
    bf16, f32 = jnp.bfloat16, jnp.float32

    anywhere = pl.BlockSpec(memory_space=pl.ANY)
    return pl.pallas_call(
        partial(attend_kernel, heads, plan, len(proj)),
        out_shape=(
            jax.ShapeDtypeStruct((length, width), bf16),
            jax.ShapeDtypeStruct((heads, length), f32),
            jax.ShapeDtypeStruct((1, heads * globs), f32),
            jax.ShapeDtypeStruct((1, heads * QTILE), f32),
            jax.ShapeDtypeStruct((1, heads * globs), f32),
        ),
        grid_spec=pltpu.PrefetchScalarGridSpec(
            num_scalar_prefetch=3,
            grid=(tiles,),
            in_specs=[anywhere] * len(proj) + [
                whole_block((1, length)),
                whole_block((length, 1)),
                whole_block((globs, 1)),
                whole_block((globs, 1)),
                whole_block((1, heads * globs)),
            ],
            out_specs=(
                whole_block((length, width)),
                pl.BlockSpec((heads, QTILE), lambda step, *_: (0, step)),
                pl.BlockSpec((1, heads * globs), lambda *_: (0, 0)),
                pl.BlockSpec((1, heads * QTILE), lambda *_: (0, 0)),
                pl.BlockSpec((1, heads * globs), lambda *_: (0, 0)),
            ),
            scratch_shapes=[
                pltpu.VMEM((length, columns), bf16),
                pltpu.VMEM((width, length), bf16),
                pltpu.VMEM((globs, length), bf16),
                pltpu.VMEM((globs, width), bf16),
                pltpu.VMEM((width, globs), bf16),
                pltpu.VMEM((width, globs), bf16),
                pltpu.VMEM((heads * globs, width), bf16),
                pltpu.VMEM((length, heads * globs), f32),
                pltpu.VMEM((width, heads * QTILE), bf16),
                pltpu.VMEM((width, QTILE), f32),
                pltpu.VMEM((1, heads * QTILE), f32),
                pltpu.VMEM((1, heads * QTILE), f32),
                pltpu.SemaphoreType.DMA((length // plan[2],)),
            ],
        ),
        compiler_params=pltpu.CompilerParams(
            dimension_semantics=("arbitrary",), vmem_limit_bytes=VMEM_BYTES
        ),
        cost_estimate=pl.CostEstimate(
            flops=20 * length * 1024 * width, bytes_accessed=14 * length * width,
            transcendentals=length * 1024 * heads,
        ),
        name="attend",
    )(order, first, last, *proj, doc_row, doc_col, pos_col, gdoc_col, gdoc_row)


def attend_back_kernel(
    heads,
    plan,
    counts,
    order_ref,
    first_ref,
    last_ref,
    *refs,
):
    pieces, refs = refs[: counts[0]], refs[counts[0] :]
    grad_pieces, refs = refs[: counts[1]], refs[counts[1] :]
    attend_back_body(heads, plan, order_ref, first_ref, last_ref, pieces, grad_pieces, *refs)


def attend_back_body(
    heads,
    plan,
    order_ref,
    first_ref,
    last_ref,
    pieces,
    grad_pieces,
    ctx_piece_ref,
    lse_ref,
    glse_ref,
    doc_row_ref,
    doc_col_ref,
    pos_col_ref,
    gdoc_col_ref,
    gdoc_row_ref,
    plain_col_ref,
    out_ref,
    proj,
    ctx,
    grad,
    keys_t,
    hot,
    far_keys,
    far_keys_t,
    far_values,
    far_key_grad,
    far_value_grad,
    key_grad,
    value_grad,
    gquery,
    gout,
    gquery_grad,
    wide,
    wide_grad,
    stack,
    stack_grad,
    probs_low,
    grads_low,
    query_grad_t,
    proj_sems,
    ctx_sems,
    grad_sems,
):
    length = proj.shape[0]
    width = heads * HEAD
    globs = pos_col_ref.shape[0]
    tiles = length // KTILE
    step = pl.program_id(0)
    bf16 = jnp.bfloat16

    def store(tile, block, value):
        cols = slice(block * width, (block + 1) * width)
        store_local(out_ref, tile, cols, value.astype(bf16), order_ref, plan)

    @pl.when(step == 0)
    def _():
        join_pieces(order_ref, pieces, proj, proj_sems, plan)
        join_pieces(order_ref, [ctx_piece_ref], ctx, ctx_sems, plan)
        join_pieces(order_ref, grad_pieces, grad, grad_sems, plan)
        for ref in (wide, wide_grad, stack, stack_grad, gquery, gout):
            ref[...] = jnp.zeros_like(ref)
        for ref in (key_grad, value_grad, far_key_grad, far_value_grad):
            ref[...] = jnp.zeros_like(ref)
        gquery_grad[...] = jnp.zeros_like(gquery_grad)
        hot[...] = one_hot_rows(pos_col_ref[...], length)
        hot_all = hot[...]
        near = mm(hot_all, proj[:, width : 2 * width])
        far_keys[...] = near.astype(bf16)
        far_keys_t[...] = near.T.astype(bf16)
        far_values[...] = mm(hot_all, proj[:, 2 * width : 3 * width], out=bf16)
        queries = (mm(hot_all, proj[:, 3 * width : 4 * width]) * score_scale).astype(bf16)
        out_grad = mm(hot_all, grad[...])
        glob_ctx = mm(hot_all, ctx[...])
        product = out_grad * glob_ctx
        owner = lax.broadcasted_iota(jnp.int32, (globs, width), 1) // HEAD
        dots = []
        for head in range(heads):
            cols = slice(head * HEAD, (head + 1) * HEAD)
            rows = slice(head * globs, (head + 1) * globs)
            gquery[rows, cols] = queries[:, cols]
            gout[rows, cols] = out_grad[:, cols].astype(bf16)
            own = jnp.where(owner == head, product, 0.0)
            dots.append(jnp.sum(own, 1, keepdims=True))
        dot_row = jnp.broadcast_to(jnp.concatenate(dots, 0), (heads * globs, 128)).T[0:1]

        def glob_tile(tile, carry):
            rows = pl.ds(pl.multiple_of(tile * KTILE, KTILE), KTILE)
            keys_t[:, rows] = proj[rows, width : 2 * width].T
            scores = mm(proj[rows, 4 * width : 5 * width], gquery[...], NT)
            scores = jnp.where(doc_col_ref[rows, :] == gdoc_row_ref[...], scores, masked_fill)
            probs = jnp.exp(scores - glse_ref[...])
            grad_p = mm(proj[rows, 5 * width : 6 * width], gout[...], NT)
            grad_s = probs * (grad_p - dot_row)
            store(tile, 5, mm(probs.astype(bf16), gout[...]))
            store(tile, 4, mm(grad_s.astype(bf16), gquery[...]))
            gquery_grad[...] += mm(grad_s.T.astype(bf16), proj[rows, 4 * width : 5 * width])
            return carry

        lax.fori_loop(0, tiles, glob_tile, 0)
        query_grad = diagonal_sum(gquery_grad[...], heads, globs) * score_scale
        query_grad = query_grad.astype(bf16)

        def spread_tile(tile, carry):
            rows = pl.ds(pl.multiple_of(tile * KTILE, KTILE), KTILE)
            store(tile, 3, mm(hot[:, rows], query_grad, TN))
            return carry

        lax.fori_loop(0, tiles, spread_tile, 0)

    start = pl.multiple_of(step * QTILE, QTILE)
    query_rows = pl.ds(start, QTILE)
    query = proj[query_rows, 0:width].astype(jnp.float32) * score_scale
    query_t = query.T.astype(bf16)
    query = query.astype(bf16)
    grad_out = grad[query_rows, :].astype(jnp.float32) * plain_col_ref[query_rows, :]
    grad_out_t = grad_out.T
    product_t = grad_out_t * ctx[query_rows, :].astype(jnp.float32).T
    grad_out = grad_out.astype(bf16)
    grad_out_t = grad_out_t.astype(bf16)
    dots = []
    for head in range(heads):
        own = slice(head * HEAD, (head + 1) * HEAD)
        cols = slice(head * QTILE, (head + 1) * QTILE)
        wide[own, cols] = query_t[own]
        wide_grad[own, cols] = grad_out_t[own]
        stack[cols, own] = query[:, own]
        stack_grad[cols, own] = grad_out[:, own]
        dots.append(jnp.sum(product_t[own], 0, keepdims=True))
    query_docs = doc_row_ref[:, query_rows]

    def parts(scores, grad_p, bias, head):
        cols = slice(head * QTILE, (head + 1) * QTILE)
        shift = lse_ref[head : head + 1, query_rows]
        probs = jnp.exp(scores[:, cols] + bias - shift)
        grad_s = probs * (grad_p[:, cols] - dots[head])
        return probs.astype(bf16), grad_s.astype(bf16)

    scores = mm(far_keys[...], wide[...])
    grad_p = mm(far_values[...], wide_grad[...])
    bias = far_bias(pos_col_ref[...], start, gdoc_col_ref[...], query_docs, globs, QTILE)
    for head in range(heads):
        cols = slice(head * QTILE, (head + 1) * QTILE)
        own = slice(head * HEAD, (head + 1) * HEAD)
        probs, grad_s = parts(scores, grad_p, bias, head)
        probs_low[0:globs, cols] = probs
        grads_low[0:globs, cols] = grad_s
        query_grad_t[own, :] = mm(far_keys_t[own, :], grad_s)
    far_value_grad[...] += mm(probs_low[0:globs, :], stack_grad[...])
    far_key_grad[...] += mm(grads_low[0:globs, :], stack[...])

    def key_tile(tile, carry):
        key_start = pl.multiple_of(tile * KTILE, KTILE)
        keys = pl.ds(key_start, KTILE)
        scores = mm(proj[keys, width : 2 * width], wide[...])
        grad_p = mm(proj[keys, 2 * width : 3 * width], wide_grad[...])
        bias = tile_bias(key_start, start, doc_col_ref[keys, :], query_docs, KTILE, QTILE)
        for head in range(heads):
            cols = slice(head * QTILE, (head + 1) * QTILE)
            own = slice(head * HEAD, (head + 1) * HEAD)
            probs, grad_s = parts(scores, grad_p, bias, head)
            probs_low[:, cols] = probs
            grads_low[:, cols] = grad_s
            query_grad_t[own, :] += mm(keys_t[own, keys], grad_s)
        value_grad[keys, :] += mm(probs_low[...], stack_grad[...])
        key_grad[keys, :] += mm(grads_low[...], stack[...])
        return carry

    lax.fori_loop(first_ref[step], last_ref[step], key_tile, 0)
    store(step, 0, (query_grad_t[...] * score_scale).T)

    @pl.when(step == pl.num_programs(0) - 1)
    def _():
        far_key = far_key_grad[...].astype(bf16)
        far_value = far_value_grad[...].astype(bf16)

        def close_tile(tile, carry):
            rows = pl.ds(pl.multiple_of(tile * KTILE, KTILE), KTILE)
            hot_tile = hot[:, rows]
            key_sum = key_grad[rows, :] + mm(hot_tile, far_key, TN)
            value_sum = value_grad[rows, :] + mm(hot_tile, far_value, TN)
            store(tile, 1, key_sum)
            store(tile, 2, value_sum)
            return carry

        lax.fori_loop(0, tiles, close_tile, 0)


def attend_back(proj, context, log_sums, grad_context, info, plan):
    length = context.shape[0]
    columns = proj[0].shape[1]
    heads = columns // (6 * HEAD)
    width = heads * HEAD
    order, first, last, doc_row, doc_col, pos_col, gdoc_col, gdoc_row, plain_col = info
    globs = pos_col.shape[0]
    tiles = length // QTILE
    bf16, f32 = jnp.bfloat16, jnp.float32
    wide = heads * QTILE
    anywhere = pl.BlockSpec(memory_space=pl.ANY)
    return pl.pallas_call(
        partial(attend_back_kernel, heads, plan, (len(proj), len(grad_context))),
        out_shape=jax.ShapeDtypeStruct((length, columns), bf16),
        grid_spec=pltpu.PrefetchScalarGridSpec(
            num_scalar_prefetch=3,
            grid=(tiles,),
            in_specs=[anywhere] * (len(proj) + len(grad_context) + 1) + [
                whole_block((heads, length)),
                whole_block((1, heads * globs)),
                whole_block((1, length)),
                whole_block((length, 1)),
                whole_block((globs, 1)),
                whole_block((globs, 1)),
                whole_block((1, heads * globs)),
                whole_block((length, 1)),
            ],
            out_specs=whole_block((length, columns)),
            scratch_shapes=[
                pltpu.VMEM((length, columns), bf16),
                pltpu.VMEM((length, width), bf16),
                pltpu.VMEM((length, width), bf16),
                pltpu.VMEM((width, length), bf16),
                pltpu.VMEM((globs, length), bf16),
                pltpu.VMEM((globs, width), bf16),
                pltpu.VMEM((width, globs), bf16),
                pltpu.VMEM((globs, width), bf16),
                pltpu.VMEM((globs, width), f32),
                pltpu.VMEM((globs, width), f32),
                pltpu.VMEM((length, width), f32),
                pltpu.VMEM((length, width), f32),
                pltpu.VMEM((heads * globs, width), bf16),
                pltpu.VMEM((heads * globs, width), bf16),
                pltpu.VMEM((heads * globs, width), f32),
                pltpu.VMEM((width, wide), bf16),
                pltpu.VMEM((width, wide), bf16),
                pltpu.VMEM((wide, width), bf16),
                pltpu.VMEM((wide, width), bf16),
                pltpu.VMEM((KTILE, wide), bf16),
                pltpu.VMEM((KTILE, wide), bf16),
                pltpu.VMEM((width, QTILE), f32),
                pltpu.SemaphoreType.DMA((length // plan[2],)),
                pltpu.SemaphoreType.DMA((length // plan[2],)),
                pltpu.SemaphoreType.DMA((length // plan[2],)),
            ],
        ),
        compiler_params=pltpu.CompilerParams(
            dimension_semantics=("arbitrary",), vmem_limit_bytes=VMEM_BYTES
        ),
        cost_estimate=pl.CostEstimate(
            flops=60 * length * 1024 * width, bytes_accessed=28 * length * width,
            transcendentals=length * 1024 * heads,
        ),
        name="attend_back",
    )(
        order, first, last, *proj, *grad_context, context, *log_sums,
        doc_row, doc_col, pos_col, gdoc_col, gdoc_row, plain_col,
    )


def sequence_info(docs_row, glob_pos, order, heads):
    length = docs_row.shape[0]
    tiles = length // QTILE
    firsts = jnp.arange(tiles, dtype=jnp.int32) * QTILE
    tile_docs = docs_row.reshape(tiles, QTILE)
    doc_start = jnp.sum(docs_row[None, :] < tile_docs[:, :1], 1, dtype=jnp.int32)
    doc_end = jnp.sum(docs_row[None, :] <= tile_docs[:, -1:], 1, dtype=jnp.int32)
    first = jnp.maximum(firsts - HALF, doc_start) // KTILE
    last = (jnp.minimum(firsts + QTILE + HALF, doc_end) + KTILE - 1) // KTILE
    hit = glob_pos[:, None] == jnp.arange(length, dtype=jnp.int32)[None, :]
    glob_docs = jnp.sum(jnp.where(hit, docs_row[None, :], 0), 1, dtype=jnp.int32)
    plain_col = jnp.where(jnp.any(hit, 0), 0.0, 1.0)[:, None]
    return (
        order,
        first,
        last,
        docs_row[None, :],
        docs_row[:, None],
        glob_pos[:, None],
        glob_docs[:, None],
        jnp.tile(glob_docs, heads)[None, :],
        plain_col.astype(jnp.float32),
    )


def norm_forward(resid, gain, shift):
    centred = resid - jnp.mean(resid, -1, keepdims=True)
    scale = lax.rsqrt(jnp.mean(centred * centred, -1, keepdims=True) + 1e-05)
    normed = centred * scale
    return normed * gain + shift, normed, scale


def norm_backward(grad, normed, scale, gain):
    weighted = grad * gain
    mean_one = jnp.mean(weighted, -1, keepdims=True)
    mean_two = jnp.mean(weighted * normed, -1, keepdims=True)
    grad_in = (weighted - mean_one - normed * mean_two) * scale
    return grad_in, jnp.stack([jnp.sum(grad * normed, 0), jnp.sum(grad, 0)])


def gelu_pair(up):
    cdf = 0.5 * (1.0 + lax.erf(up * (0.5**0.5)))
    slope = cdf + up * (jnp.exp(-0.5 * up * up) * (1.0 / math.sqrt(2.0 * math.pi)))
    return (up * cdf).astype(jnp.bfloat16), slope.astype(jnp.bfloat16)


def after(value, *others):
    return lax.optimization_barrier((value,) + others)[0]


def shards(tokens, cotangent, doc_ids, global_flags, w_attn, w_out, w_up, w_down, ln_gain, ln_bias):
    bf16, f32 = jnp.bfloat16, jnp.float32
    sections = lax.axis_size("section")
    slots = lax.axis_size("tensor")
    copies = lax.axis_size("dp")
    micro = tokens.shape[0]
    inner = slots // micro
    section = lax.axis_index("section")
    slot = lax.axis_index("tensor")
    row = slot // inner
    lane = slot % inner
    width = tokens.shape[3]
    chunk = tokens.shape[2]
    rows = min(QTILE, chunk)
    parts = chunk // rows
    plan = (inner, parts, rows)
    crossed = inner == 2
    joint = ("section", "tensor")
    groups = [[a * inner + b for b in range(inner)] for a in range(micro)]

    def device(s, a, b):
        return s * slots + a * inner + b

    def route(value, link):
        pairs = []
        for s in range(sections):
            for a in range(micro):
                for b in range(inner):
                    target = link(s, a, b)
                    if target is not None and target != (s, a, b):
                        pairs.append((device(s, a, b), device(*target)))
        return lax.ppermute(value, joint, pairs)

    def other_core(value):
        return lax.ppermute(value, "section", [(0, 1), (1, 0)])

    def other_row(value):
        return route(value, lambda s, a, b: (s, 1 - a, b))

    def other_lane(value):
        return route(value, lambda s, a, b: (s, a, 1 - b))

    class ByLane:
        home = section == row
        swap = staticmethod(other_lane)

        @staticmethod
        def keeper(s, a, b):
            return a

        @staticmethod
        def across(s, a, b):
            return (s, 1 - a, b)

    class ByRow:
        home = section == lane
        swap = staticmethod(other_row)

        @staticmethod
        def keeper(s, a, b):
            return b

        @staticmethod
        def across(s, a, b):
            return (s, a, 1 - b)

    split_attn = ByLane
    split_mlp = ByRow if crossed else ByLane

    def gather(own, split, hop=None):
        near = jnp.concatenate([own, other_core(own)], 0)
        if not crossed:
            if inner == 1:
                return [near]
            return [lax.all_gather(near, "tensor", axis=0, tiled=True, axis_index_groups=groups)]
        if hop is None:
            hop = split.swap(own)
        return [near, jnp.concatenate([hop, other_core(hop)], 0)]

    def scatter(partials, split):
        if not crossed:
            blocks = partials[0].reshape(inner, 2, rows, -1)
            ours, theirs = blocks[:, 0], blocks[:, 1].astype(bf16)
            total = (ours + other_core(theirs).astype(f32)).reshape(inner * rows, -1)
            if inner == 1:
                return total
            return lax.psum_scatter(
                total.astype(bf16), "tensor", scatter_dimension=0, tiled=True,
                axis_index_groups=groups,
            ).astype(f32)
        near, far = partials
        leaving = far[:rows] + other_core(far[rows:].astype(bf16)).astype(f32)
        staying = near[:rows] + other_core(near[rows:].astype(bf16)).astype(f32)
        return staying + split.swap(leaving.astype(bf16)).astype(f32)

    def cut(array):
        per_part = 2 * inner * rows
        per_group = 2 * rows if crossed else per_part
        return [
            [array[p * per_part + g : p * per_part + g + per_group] for g in range(0, per_part, per_group)]
            for p in range(parts)
        ]

    def joined(pieces):
        return jnp.concatenate([piece for part in pieces for piece in part], 0)

    def flat(pieces):
        return [piece for part in pieces for piece in part]

    def part_rows(array):
        return [array[p * rows : (p + 1) * rows] for p in range(parts)]

    def own_rows(array):
        mine = lax.dynamic_index_in_dim(array[:, 0], row, 0, False)
        theirs = lax.dynamic_index_in_dim(array[:, 0], 1 - row, 0, False)
        moved = route(theirs, lambda s, a, b: (s, 1 - a, b) if s == a else None)
        return mine, moved

    def fetch(weight, layer, split):
        def across(s, a, b):
            if s != layer:
                return None
            _, a2, b2 = split.across(s, a, b)
            return (split.keeper(s, a, b), a2, b2)

        def within(s, a, b):
            return (split.keeper(s, a, b), a, b) if s == layer else None

        far = route(weight, across)
        near = route(weight, within)
        return jnp.where(split.home, jnp.where(section == layer, weight, near), far)

    mine, moved = own_rows(tokens)
    own = part_rows(jnp.where(ByLane.home, mine, moved))
    hops = [None] * parts
    if crossed:
        early = route(mine, lambda s, a, b: (s, a, 1 - b) if s == a else None)
        late = route(moved, lambda s, a, b: (s, a, 1 - b) if s != a else None)
        hops = part_rows(jnp.where(ByLane.home, early, late))
    attn_table = w_attn[0].reshape(width, -1)
    weights = [[None] * 4 for _ in range(sections)]
    weights[0][0] = fetch(after(attn_table, moved), 0, split_attn)
    weights[0][1] = fetch(after(w_out[0], weights[0][0]), 0, split_attn)
    weights[0][2] = fetch(after(w_up[0], hops[0]) if crossed else w_up[0], 0, split_mlp)
    weights[0][3] = fetch(after(w_down[0], weights[0][2]), 0, split_mlp)
    weights[1][0] = fetch(after(attn_table, weights[0][1]), 1, split_attn)
    weights[1][1] = fetch(after(w_out[0], weights[1][0]), 1, split_attn)

    heads = w_attn.shape[3] // HEAD
    docs = lax.dynamic_index_in_dim(doc_ids[:, 0], row, 0, False)
    flags = lax.dynamic_index_in_dim(global_flags[:, 0], row, 0, False)
    order = jnp.stack([section, lane if crossed else jnp.zeros_like(lane)]).astype(jnp.int32)
    info = sequence_info(docs, flags, order, heads)

    gains_own = jnp.stack([ln_gain[0], ln_bias[0]])
    gains_other = other_core(gains_own)
    norms = [jnp.where(section == layer, gains_own, gains_other) for layer in range(sections)]

    saved, outputs, peaks = [], [], []
    for layer in range(sections):
        gains, shifts = norms[layer]
        inputs = [gather(own[p], split_attn, hops[p] if layer == 0 else None) for p in range(parts)]
        proj = [[mm(piece, weights[layer][0], NN, bf16) for piece in part] for part in inputs]
        context, lse, glse, peak, gpeak = attend(flat(proj), info, plan)
        peaks.append(
            jnp.stack([jnp.max(peak.reshape(heads, -1), 1), jnp.max(gpeak.reshape(heads, -1), 1)])
        )
        context_parts = cut(context)
        attn_sums = [
            scatter([mm(piece, weights[layer][1]) for piece in part], split_attn)
            for part in context_parts
        ]
        if layer == 0:
            weights[1][2] = fetch(after(w_up[0], attn_sums[-1]), 1, split_mlp)
        hidden_rows, acts, slopes, norms_one, norms_two, outs = [], [], [], [], [], []
        for p in range(parts):
            hidden, normed, scale = norm_forward(
                own[p].astype(f32) + attn_sums[p], gains[0], shifts[0]
            )
            norms_one.append((normed, scale))
            hidden_rows.append(gather(hidden.astype(bf16), split_mlp))
            pairs = [gelu_pair(mm(piece, weights[layer][2])) for piece in hidden_rows[p]]
            acts.append([act for act, _ in pairs])
            slopes.append([slope for _, slope in pairs])
            mlp_sum = scatter([mm(act, weights[layer][3]) for act in acts[p]], split_mlp)
            out, normed, scale = norm_forward(hidden + mlp_sum, gains[1], shifts[1])
            norms_two.append((normed, scale))
            outs.append(out.astype(bf16))
        if layer == 0:
            weights[1][3] = fetch(after(w_down[0], weights[1][2], outs[-1]), 1, split_mlp)
        own = outs
        outputs.append(jnp.concatenate(outs, 0))
        saved.append(
            (inputs, proj, context, (lse, glse), norms_one, hidden_rows, acts, slopes, norms_two)
        )

    def to_owner(grad, split):
        half = grad.shape[0] // 2
        upper, lower = grad[:half], grad[half:]

        def first_link(s, a, b):
            if s == split.keeper(s, a, b):
                return (1 - s, a, b)
            return split.across(s, a, b)

        def second_link(s, a, b):
            if s == split.keeper(s, a, b):
                return None
            _, a2, b2 = split.across(s, a, b)
            return (1 - s, a2, b2)

        first = route(jnp.where(split.home, lower, upper), first_link)
        second = route(lower, second_link)
        part = first.astype(f32) + jnp.where(split.home, upper, second).astype(f32)
        return part.astype(bf16)

    mine, moved = own_rows(after(cotangent, outputs[0]))
    grad_out = part_rows(jnp.where(ByLane.home, mine, moved).astype(f32))
    weight_sums = [[None] * 4 for _ in range(sections)]
    norm_sums = [None] * sections
    input_grads = [None] * sections
    earlier_sums = ()

    def dp_sum(layer, which, terms):
        nonlocal earlier_sums
        terms = lax.optimization_barrier(tuple(terms) + earlier_sums)[: len(terms)]
        sums = lax.psum(tuple(terms), "dp")
        earlier_sums = tuple(sums)
        for index, value in zip(which, sums):
            weight_sums[layer][index] = value

    for layer in reversed(range(sections)):
        attn_w, out_w, up_w, down_w = weights[layer]
        gains, _ = norms[layer]
        inputs, proj, context, log_sums, norms_one, hidden_rows, acts, slopes, norms_two = saved[layer]
        grad_mlp, grad_up, grad_attn, grad_context, grads_one = [], [], [], [], []
        sums_one = sums_two = 0.0
        for p in range(parts):
            grad_two, sums = norm_backward(grad_out[p], *norms_two[p], gains[1])
            sums_two = sums_two + sums
            grad_mlp.append(gather(grad_two.astype(bf16), split_mlp))
            grad_up.append(
                [
                    (mm(piece, down_w, NT) * slope.astype(f32)).astype(bf16)
                    for piece, slope in zip(grad_mlp[p], slopes[p])
                ]
            )
            grad_hidden = scatter([mm(piece, up_w, NT) for piece in grad_up[p]], split_mlp) + grad_two
            grad_one, sums = norm_backward(grad_hidden, *norms_one[p], gains[0])
            sums_one = sums_one + sums
            grads_one.append(grad_one)
            grad_attn.append(gather(grad_one.astype(bf16), split_attn))
            grad_context.append([mm(piece, out_w, NT, bf16) for piece in grad_attn[p]])
        norm_sums[layer] = jnp.stack([sums_one, sums_two])
        grad_mlp, grad_up = joined(grad_mlp), joined(grad_up)
        grad_down_w = mm(joined(acts), grad_mlp, TN, bf16)
        grad_up_w = mm(joined(hidden_rows), grad_up, TN, bf16)
        mlp_terms = (to_owner(grad_up_w, split_mlp), to_owner(grad_down_w, split_mlp))
        dp_sum(layer, (2, 3), mlp_terms)
        grad_proj = attend_back(flat(proj), context, log_sums, flat(grad_context), info, plan)
        grad_attn_w = mm(joined(inputs), grad_proj, TN, bf16)
        grad_out_w = mm(context, joined(grad_attn), TN, bf16)
        attn_terms = (to_owner(grad_attn_w, split_attn), to_owner(grad_out_w, split_attn))
        dp_sum(layer, (0, 1), attn_terms)
        if layer == 0:
            grad_proj = after(grad_proj, grad_attn_w)
        grad_low = []
        for p, part in enumerate(cut(grad_proj)):
            grad_in = scatter([mm(piece, attn_w, NT) for piece in part], split_attn) + grads_one[p]
            grad_low.append(grad_in.astype(bf16))
        grad_out = [piece.astype(f32) for piece in grad_low]
        input_grads[layer] = jnp.concatenate(grad_low, 0)

    def pick(values):
        return jnp.where(section == 0, values[0], values[1])

    def placed_rows(chunks):
        result = []
        for index in range(micro):
            arrived = []
            for layer in range(sections):
                moved = route(chunks[layer], lambda s, a, b: (layer, s, b) if a == index else None)
                stays = (section == layer) & ByLane.home & (row == index)
                arrived.append(jnp.where(stays, chunks[layer], moved))
            result.append(pick(arrived))
        return jnp.stack(result)[None, :, None]

    def placed_weight(index, split):
        terms = [weight_sums[layer][index] for layer in range(sections)]
        mine = pick(terms)
        theirs = other_core(pick(terms[::-1]))
        first = jnp.where(split.home, mine, theirs)
        second = jnp.where(split.home, theirs, mine)
        return jnp.concatenate([first, second], 0).astype(f32)

    def dp_butterfly(value, combine):
        if copies & (copies - 1):
            gathered = lax.all_gather(value, "dp", axis=0)
            total = gathered[0]
            for index in range(1, copies):
                total = combine(total, gathered[index])
            return total
        distance = 1
        while distance < copies:
            pairs = [(d, d ^ distance) for d in range(copies)]
            value = combine(value, lax.ppermute(value, "dp", pairs))
            distance *= 2
        return value

    norm_sum = pick(norm_sums) + other_core(pick(norm_sums[::-1]))
    if crossed:
        norm_sum = norm_sum + other_row(norm_sum)
        norm_sum = norm_sum + other_lane(norm_sum)
    else:
        norm_sum = lax.psum(norm_sum, "tensor")
    norm_sum = dp_butterfly(norm_sum, jnp.add)

    peak_all = jnp.stack(peaks)
    peak_all = jnp.maximum(peak_all, other_row(peak_all))
    peak_all = dp_butterfly(peak_all, jnp.maximum)
    peak_here = jnp.where(ByLane.home, pick(peak_all), other_core(pick(peak_all[::-1])))
    factors = jnp.sqrt(clip_limit / jnp.maximum(peak_here, clip_limit))
    columns = jnp.repeat(factors, HEAD, axis=1)
    attn_local = w_attn[0].astype(f32)
    clipped = jnp.stack(
        [
            attn_local[:, 0] * columns[0][None, :],
            attn_local[:, 1] * columns[0][None, :],
            attn_local[:, 3] * columns[1][None, :],
            attn_local[:, 4] * columns[1][None, :],
        ],
        1,
    )
    return (
        placed_rows(outputs),
        placed_rows(input_grads),
        placed_weight(0, split_attn).reshape(1, width, 6, -1),
        placed_weight(1, split_attn)[None],
        placed_weight(2, split_mlp)[None],
        placed_weight(3, split_mlp)[None],
        norm_sum[:, 0][None],
        norm_sum[:, 1][None],
        clipped[None],
    )


def solution(mesh):
    in_specs = (
        P(None, "dp", "tensor", None),
        P(None, "dp", "tensor", None),
        P(None, "dp", None),
        P(None, "dp", None),
        P("section", None, None, "tensor"),
        P("section", "tensor", None),
        P("section", None, "tensor"),
        P("section", "tensor", None),
        P("section", None, None),
        P("section", None, None),
    )
    out_specs = (
        P("section", None, "dp", "tensor", None),
        P("section", None, "dp", "tensor", None),
        P("section", None, None, "tensor"),
        P("section", "tensor", None),
        P("section", None, "tensor"),
        P("section", "tensor", None),
        P("section", None, None),
        P("section", None, None),
        P("section", None, None, "tensor"),
    )
    return jax.shard_map(shards, mesh=mesh, in_specs=in_specs, out_specs=out_specs, check_vma=False)
```

```python
import math
from functools import partial

import jax
import jax.numpy as jnp
from jax import lax
from jax.experimental import pallas as pl
from jax.experimental.pallas import tpu as pltpu
from jax.sharding import PartitionSpec as P

HEAD = 64
HALF = 512
QTILE = 256
KTILE = 512
VMEM_BYTES = 56 * 1024 * 1024

masked_fill = -1e30
clip_limit = 10.0
score_scale = HEAD ** (-0.5)

NN = (((1,), (0,)), ((), ()))
NT = (((1,), (1,)), ((), ()))
TN = (((0,), (0,)), ((), ()))


def mm(left, right, dims=NN, out=jnp.float32):
    return lax.dot_general(left, right, dims, preferred_element_type=jnp.float32).astype(out)


def tile_bias(first_key, first_query, key_docs, query_docs, keys, queries):
    key_pos = first_key + lax.broadcasted_iota(jnp.int32, (keys, queries), 0)
    query_pos = first_query + lax.broadcasted_iota(jnp.int32, (keys, queries), 1)
    gap = jnp.abs(key_pos - query_pos)
    return jnp.where((key_docs == query_docs) & (gap <= HALF), 0.0, masked_fill)


def far_bias(glob_pos, first_query, glob_docs, query_docs, globs, queries):
    query_pos = first_query + lax.broadcasted_iota(jnp.int32, (globs, queries), 1)
    gap = jnp.abs(glob_pos - query_pos)
    return jnp.where((glob_docs == query_docs) & (gap > HALF), 0.0, masked_fill)


def one_hot_rows(glob_pos, length):
    globs = glob_pos.shape[0]
    hit = lax.broadcasted_iota(jnp.int32, (globs, length), 1) == glob_pos
    return jnp.where(hit, 1.0, 0.0).astype(jnp.bfloat16)


def true_unit(place, order_ref, plan):
    inner, parts, _ = plan
    part, rest = place // (2 * inner), place % (2 * inner)
    side = (rest % 2) ^ order_ref[0]
    lane = (rest // 2) ^ order_ref[1]
    return (side * inner + lane) * parts + part


def local_unit(unit, order_ref, plan):
    inner, parts, _ = plan
    block, part = lax.div(unit, parts), lax.rem(unit, parts)
    side = lax.div(block, inner) ^ order_ref[0]
    lane = lax.rem(block, inner) ^ order_ref[1]
    return part * (2 * inner) + lane * 2 + side


def join_pieces(order_ref, pieces, joined_ref, sems, plan):
    rows = plan[2]
    copies = []
    place = 0
    for piece in pieces:
        for index in range(piece.shape[0] // rows):
            start = pl.multiple_of(true_unit(place, order_ref, plan) * rows, rows)
            copies.append(
                pltpu.make_async_copy(
                    piece.at[pl.ds(index * rows, rows), :],
                    joined_ref.at[pl.ds(start, rows), :],
                    sems.at[place],
                )
            )
            place += 1
    for copy in copies:
        copy.start()
    for copy in copies:
        copy.wait()


def store_local(out_ref, tile, cols, value, order_ref, plan):
    rows = plan[2]
    size = min(rows, value.shape[0])
    for index in range(value.shape[0] // size):
        row = tile * value.shape[0] + index * size
        place = local_unit(lax.div(row, rows), order_ref, plan)
        start = pl.multiple_of(place * rows + lax.rem(row, rows), size)
        out_ref[pl.ds(start, size), cols] = value[index * size : (index + 1) * size]


def diagonal_sum(blocks, heads, rows):
    owner = lax.broadcasted_iota(jnp.int32, (rows, heads * HEAD), 1) // HEAD
    total = jnp.zeros((rows, heads * HEAD), jnp.float32)
    for head in range(heads):
        total = total + jnp.where(owner == head, blocks[head * rows : (head + 1) * rows], 0.0)
    return total


def attend_kernel(
    heads,
    plan,
    count,
    order_ref,
    first_ref,
    last_ref,
    *refs,
):
    pieces, refs = refs[:count], refs[count:]
    attend_body(heads, plan, order_ref, first_ref, last_ref, pieces, *refs)


def attend_body(
    heads,
    plan,
    order_ref,
    first_ref,
    last_ref,
    pieces,
    doc_row_ref,
    doc_col_ref,
    pos_col_ref,
    gdoc_col_ref,
    gdoc_row_ref,
    ctx_ref,
    lse_ref,
    glse_ref,
    peak_ref,
    gpeak_ref,
    proj,
    values_t,
    hot,
    far_keys,
    far_values_t,
    gctx_t,
    gstack,
    gscores,
    wide,
    acc,
    top,
    total,
    sems,
):
    length = proj.shape[0]
    width = heads * HEAD
    globs = pos_col_ref.shape[0]
    step = pl.program_id(0)

    @pl.when(step == 0)
    def _():
        join_pieces(order_ref, pieces, proj, sems, plan)
        wide[...] = jnp.zeros_like(wide)
        gstack[...] = jnp.zeros_like(gstack)
        hot[...] = one_hot_rows(pos_col_ref[...], length)
        hot_all = hot[...]
        far_keys[...] = mm(hot_all, proj[:, width : 2 * width], out=jnp.bfloat16)
        far_values_t[...] = mm(hot_all, proj[:, 2 * width : 3 * width]).T.astype(jnp.bfloat16)
        queries = (mm(hot_all, proj[:, 3 * width : 4 * width]) * score_scale).astype(jnp.bfloat16)
        for head in range(heads):
            cols = slice(head * HEAD, (head + 1) * HEAD)
            gstack[head * globs : (head + 1) * globs, cols] = queries[:, cols]

        def score_tile(tile, best):
            rows = pl.ds(pl.multiple_of(tile * KTILE, KTILE), KTILE)
            values_t[:, rows] = proj[rows, 2 * width : 3 * width].T
            scores = mm(proj[rows, 4 * width : 5 * width], gstack[...], NT)
            scores = jnp.where(doc_col_ref[rows, :] == gdoc_row_ref[...], scores, masked_fill)
            gscores[rows, :] = scores
            return jnp.maximum(best, jnp.max(scores, 0, keepdims=True))

        best = lax.fori_loop(
            0, length // KTILE, score_tile, jnp.full((1, heads * globs), masked_fill, jnp.float32)
        )

        def sum_tile(tile, sums):
            rows = pl.ds(pl.multiple_of(tile * KTILE, KTILE), KTILE)
            weights = jnp.exp(gscores[rows, :] - best)
            gscores[rows, :] = weights
            return sums + jnp.sum(weights, 0, keepdims=True)

        sums = lax.fori_loop(
            0, length // KTILE, sum_tile, jnp.zeros((1, heads * globs), jnp.float32)
        )

        def value_tile(tile, blocks):
            rows = pl.ds(pl.multiple_of(tile * KTILE, KTILE), KTILE)
            probs = (gscores[rows, :] / sums).T.astype(jnp.bfloat16)
            return blocks + mm(probs, proj[rows, 5 * width : 6 * width])

        blocks = lax.fori_loop(
            0, length // KTILE, value_tile, jnp.zeros((heads * globs, width), jnp.float32)
        )
        gctx_t[...] = diagonal_sum(blocks, heads, globs).T.astype(jnp.bfloat16)
        glse_ref[...] = best + jnp.log(sums)
        gpeak_ref[...] = best

    start = pl.multiple_of(step * QTILE, QTILE)
    query_rows = pl.ds(start, QTILE)
    query_t = proj[query_rows, 0:width].T * score_scale
    for head in range(heads):
        rows = slice(head * HEAD, (head + 1) * HEAD)
        wide[rows, head * QTILE : (head + 1) * QTILE] = query_t[rows].astype(jnp.bfloat16)
    query_docs = doc_row_ref[:, query_rows]

    scores = mm(far_keys[...], wide[...])
    bias = far_bias(pos_col_ref[...], start, gdoc_col_ref[...], query_docs, globs, QTILE)
    for head in range(heads):
        cols = slice(head * QTILE, (head + 1) * QTILE)
        rows = slice(head * HEAD, (head + 1) * HEAD)
        part = scores[:, cols] + bias
        best = jnp.max(part, 0, keepdims=True)
        weights = jnp.exp(part - best)
        top[:, cols] = best
        total[:, cols] = jnp.sum(weights, 0, keepdims=True)
        acc[rows, :] = mm(far_values_t[rows, :], weights.astype(jnp.bfloat16))

    def key_tile(tile, carry):
        key_start = pl.multiple_of(tile * KTILE, KTILE)
        keys = pl.ds(key_start, KTILE)
        scores = mm(proj[keys, width : 2 * width], wide[...])
        bias = tile_bias(key_start, start, doc_col_ref[keys, :], query_docs, KTILE, QTILE)
        for head in range(heads):
            cols = slice(head * QTILE, (head + 1) * QTILE)
            rows = slice(head * HEAD, (head + 1) * HEAD)
            part = scores[:, cols] + bias
            old = top[:, cols]
            best = jnp.maximum(old, jnp.max(part, 0, keepdims=True))
            weights = jnp.exp(part - best)
            shrink = jnp.exp(old - best)
            top[:, cols] = best
            total[:, cols] = total[:, cols] * shrink + jnp.sum(weights, 0, keepdims=True)
            acc[rows, :] = acc[rows, :] * shrink + mm(
                values_t[rows, keys], weights.astype(jnp.bfloat16)
            )
        return carry

    lax.fori_loop(first_ref[step], last_ref[step], key_tile, 0)

    hot_tile = hot[:, query_rows]
    is_glob = jnp.max(hot_tile.astype(jnp.float32), 0, keepdims=True) > 0.5
    for head in range(heads):
        cols = slice(head * QTILE, (head + 1) * QTILE)
        rows = slice(head * HEAD, (head + 1) * HEAD)
        acc[rows, :] = acc[rows, :] / total[:, cols]
        lse_ref[head : head + 1, :] = top[:, cols] + jnp.log(total[:, cols])
    merged = jnp.where(is_glob, mm(gctx_t[...], hot_tile), acc[...])
    store_local(ctx_ref, step, slice(None), merged.T.astype(jnp.bfloat16), order_ref, plan)

    @pl.when(step == 0)
    def _():
        peak_ref[...] = top[...]

    @pl.when(step > 0)
    def _():
        peak_ref[...] = jnp.maximum(peak_ref[...], top[...])


def whole_block(shape):
    return pl.BlockSpec(shape, lambda *_: (0,) * len(shape), pipeline_mode=pl.Buffered(1))


def attend(proj, info, plan):
    length = sum(piece.shape[0] for piece in proj)
    columns = proj[0].shape[1]
    heads = columns // (6 * HEAD)
    width = heads * HEAD
    order, first, last, doc_row, doc_col, pos_col, gdoc_col, gdoc_row, _ = info
    globs = pos_col.shape[0]
    tiles = length // QTILE
    bf16, f32 = jnp.bfloat16, jnp.float32

    anywhere = pl.BlockSpec(memory_space=pl.ANY)
    return pl.pallas_call(
        partial(attend_kernel, heads, plan, len(proj)),
        out_shape=(
            jax.ShapeDtypeStruct((length, width), bf16),
            jax.ShapeDtypeStruct((heads, length), f32),
            jax.ShapeDtypeStruct((1, heads * globs), f32),
            jax.ShapeDtypeStruct((1, heads * QTILE), f32),
            jax.ShapeDtypeStruct((1, heads * globs), f32),
        ),
        grid_spec=pltpu.PrefetchScalarGridSpec(
            num_scalar_prefetch=3,
            grid=(tiles,),
            in_specs=[anywhere] * len(proj) + [
                whole_block((1, length)),
                whole_block((length, 1)),
                whole_block((globs, 1)),
                whole_block((globs, 1)),
                whole_block((1, heads * globs)),
            ],
            out_specs=(
                whole_block((length, width)),
                pl.BlockSpec((heads, QTILE), lambda step, *_: (0, step)),
                pl.BlockSpec((1, heads * globs), lambda *_: (0, 0)),
                pl.BlockSpec((1, heads * QTILE), lambda *_: (0, 0)),
                pl.BlockSpec((1, heads * globs), lambda *_: (0, 0)),
            ),
            scratch_shapes=[
                pltpu.VMEM((length, columns), bf16),
                pltpu.VMEM((width, length), bf16),
                pltpu.VMEM((globs, length), bf16),
                pltpu.VMEM((globs, width), bf16),
                pltpu.VMEM((width, globs), bf16),
                pltpu.VMEM((width, globs), bf16),
                pltpu.VMEM((heads * globs, width), bf16),
                pltpu.VMEM((length, heads * globs), f32),
                pltpu.VMEM((width, heads * QTILE), bf16),
                pltpu.VMEM((width, QTILE), f32),
                pltpu.VMEM((1, heads * QTILE), f32),
                pltpu.VMEM((1, heads * QTILE), f32),
                pltpu.SemaphoreType.DMA((length // plan[2],)),
            ],
        ),
        compiler_params=pltpu.CompilerParams(
            dimension_semantics=("arbitrary",), vmem_limit_bytes=VMEM_BYTES
        ),
        cost_estimate=pl.CostEstimate(
            flops=20 * length * 1024 * width, bytes_accessed=14 * length * width,
            transcendentals=length * 1024 * heads,
        ),
        name="attend",
    )(order, first, last, *proj, doc_row, doc_col, pos_col, gdoc_col, gdoc_row)


def attend_back_kernel(
    heads,
    plan,
    counts,
    order_ref,
    first_ref,
    last_ref,
    *refs,
):
    pieces, refs = refs[: counts[0]], refs[counts[0] :]
    grad_pieces, refs = refs[: counts[1]], refs[counts[1] :]
    attend_back_body(heads, plan, order_ref, first_ref, last_ref, pieces, grad_pieces, *refs)


def attend_back_body(
    heads,
    plan,
    order_ref,
    first_ref,
    last_ref,
    pieces,
    grad_pieces,
    ctx_piece_ref,
    lse_ref,
    glse_ref,
    doc_row_ref,
    doc_col_ref,
    pos_col_ref,
    gdoc_col_ref,
    gdoc_row_ref,
    plain_col_ref,
    out_ref,
    proj,
    ctx,
    grad,
    keys_t,
    hot,
    far_keys,
    far_keys_t,
    far_values,
    far_key_grad,
    far_value_grad,
    key_grad,
    value_grad,
    gquery,
    gout,
    gquery_grad,
    wide,
    wide_grad,
    stack,
    stack_grad,
    probs_low,
    grads_low,
    query_grad_t,
    proj_sems,
    ctx_sems,
    grad_sems,
):
    length = proj.shape[0]
    width = heads * HEAD
    globs = pos_col_ref.shape[0]
    tiles = length // KTILE
    step = pl.program_id(0)
    bf16 = jnp.bfloat16

    def store(tile, block, value):
        cols = slice(block * width, (block + 1) * width)
        store_local(out_ref, tile, cols, value.astype(bf16), order_ref, plan)

    @pl.when(step == 0)
    def _():
        join_pieces(order_ref, pieces, proj, proj_sems, plan)
        join_pieces(order_ref, [ctx_piece_ref], ctx, ctx_sems, plan)
        join_pieces(order_ref, grad_pieces, grad, grad_sems, plan)
        for ref in (wide, wide_grad, stack, stack_grad, gquery, gout):
            ref[...] = jnp.zeros_like(ref)
        for ref in (key_grad, value_grad, far_key_grad, far_value_grad):
            ref[...] = jnp.zeros_like(ref)
        gquery_grad[...] = jnp.zeros_like(gquery_grad)
        hot[...] = one_hot_rows(pos_col_ref[...], length)
        hot_all = hot[...]
        near = mm(hot_all, proj[:, width : 2 * width])
        far_keys[...] = near.astype(bf16)
        far_keys_t[...] = near.T.astype(bf16)
        far_values[...] = mm(hot_all, proj[:, 2 * width : 3 * width], out=bf16)
        queries = (mm(hot_all, proj[:, 3 * width : 4 * width]) * score_scale).astype(bf16)
        out_grad = mm(hot_all, grad[...])
        glob_ctx = mm(hot_all, ctx[...])
        product = out_grad * glob_ctx
        owner = lax.broadcasted_iota(jnp.int32, (globs, width), 1) // HEAD
        dots = []
        for head in range(heads):
            cols = slice(head * HEAD, (head + 1) * HEAD)
            rows = slice(head * globs, (head + 1) * globs)
            gquery[rows, cols] = queries[:, cols]
            gout[rows, cols] = out_grad[:, cols].astype(bf16)
            own = jnp.where(owner == head, product, 0.0)
            dots.append(jnp.sum(own, 1, keepdims=True))
        dot_row = jnp.broadcast_to(jnp.concatenate(dots, 0), (heads * globs, 128)).T[0:1]

        def glob_tile(tile, carry):
            rows = pl.ds(pl.multiple_of(tile * KTILE, KTILE), KTILE)
            keys_t[:, rows] = proj[rows, width : 2 * width].T
            scores = mm(proj[rows, 4 * width : 5 * width], gquery[...], NT)
            scores = jnp.where(doc_col_ref[rows, :] == gdoc_row_ref[...], scores, masked_fill)
            probs = jnp.exp(scores - glse_ref[...])
            grad_p = mm(proj[rows, 5 * width : 6 * width], gout[...], NT)
            grad_s = probs * (grad_p - dot_row)
            store(tile, 5, mm(probs.astype(bf16), gout[...]))
            store(tile, 4, mm(grad_s.astype(bf16), gquery[...]))
            gquery_grad[...] += mm(grad_s.T.astype(bf16), proj[rows, 4 * width : 5 * width])
            return carry

        lax.fori_loop(0, tiles, glob_tile, 0)
        query_grad = diagonal_sum(gquery_grad[...], heads, globs) * score_scale
        query_grad = query_grad.astype(bf16)

        def spread_tile(tile, carry):
            rows = pl.ds(pl.multiple_of(tile * KTILE, KTILE), KTILE)
            store(tile, 3, mm(hot[:, rows], query_grad, TN))
            return carry

        lax.fori_loop(0, tiles, spread_tile, 0)

    start = pl.multiple_of(step * QTILE, QTILE)
    query_rows = pl.ds(start, QTILE)
    query = proj[query_rows, 0:width].astype(jnp.float32) * score_scale
    query_t = query.T.astype(bf16)
    query = query.astype(bf16)
    grad_out = grad[query_rows, :].astype(jnp.float32) * plain_col_ref[query_rows, :]
    grad_out_t = grad_out.T
    product_t = grad_out_t * ctx[query_rows, :].astype(jnp.float32).T
    grad_out = grad_out.astype(bf16)
    grad_out_t = grad_out_t.astype(bf16)
    dots = []
    for head in range(heads):
        own = slice(head * HEAD, (head + 1) * HEAD)
        cols = slice(head * QTILE, (head + 1) * QTILE)
        wide[own, cols] = query_t[own]
        wide_grad[own, cols] = grad_out_t[own]
        stack[cols, own] = query[:, own]
        stack_grad[cols, own] = grad_out[:, own]
        dots.append(jnp.sum(product_t[own], 0, keepdims=True))
    query_docs = doc_row_ref[:, query_rows]

    def parts(scores, grad_p, bias, head):
        cols = slice(head * QTILE, (head + 1) * QTILE)
        shift = lse_ref[head : head + 1, query_rows]
        probs = jnp.exp(scores[:, cols] + bias - shift)
        grad_s = probs * (grad_p[:, cols] - dots[head])
        return probs.astype(bf16), grad_s.astype(bf16)

    scores = mm(far_keys[...], wide[...])
    grad_p = mm(far_values[...], wide_grad[...])
    bias = far_bias(pos_col_ref[...], start, gdoc_col_ref[...], query_docs, globs, QTILE)
    for head in range(heads):
        cols = slice(head * QTILE, (head + 1) * QTILE)
        own = slice(head * HEAD, (head + 1) * HEAD)
        probs, grad_s = parts(scores, grad_p, bias, head)
        probs_low[0:globs, cols] = probs
        grads_low[0:globs, cols] = grad_s
        query_grad_t[own, :] = mm(far_keys_t[own, :], grad_s)
    far_value_grad[...] += mm(probs_low[0:globs, :], stack_grad[...])
    far_key_grad[...] += mm(grads_low[0:globs, :], stack[...])

    def key_tile(tile, carry):
        key_start = pl.multiple_of(tile * KTILE, KTILE)
        keys = pl.ds(key_start, KTILE)
        scores = mm(proj[keys, width : 2 * width], wide[...])
        grad_p = mm(proj[keys, 2 * width : 3 * width], wide_grad[...])
        bias = tile_bias(key_start, start, doc_col_ref[keys, :], query_docs, KTILE, QTILE)
        for head in range(heads):
            cols = slice(head * QTILE, (head + 1) * QTILE)
            own = slice(head * HEAD, (head + 1) * HEAD)
            probs, grad_s = parts(scores, grad_p, bias, head)
            probs_low[:, cols] = probs
            grads_low[:, cols] = grad_s
            query_grad_t[own, :] += mm(keys_t[own, keys], grad_s)
        value_grad[keys, :] += mm(probs_low[...], stack_grad[...])
        key_grad[keys, :] += mm(grads_low[...], stack[...])
        return carry

    lax.fori_loop(first_ref[step], last_ref[step], key_tile, 0)
    store(step, 0, (query_grad_t[...] * score_scale).T)

    @pl.when(step == pl.num_programs(0) - 1)
    def _():
        far_key = far_key_grad[...].astype(bf16)
        far_value = far_value_grad[...].astype(bf16)

        def close_tile(tile, carry):
            rows = pl.ds(pl.multiple_of(tile * KTILE, KTILE), KTILE)
            hot_tile = hot[:, rows]
            key_sum = key_grad[rows, :] + mm(hot_tile, far_key, TN)
            value_sum = value_grad[rows, :] + mm(hot_tile, far_value, TN)
            store(tile, 1, key_sum)
            store(tile, 2, value_sum)
            return carry

        lax.fori_loop(0, tiles, close_tile, 0)


def attend_back(proj, context, log_sums, grad_context, info, plan):
    length = context.shape[0]
    columns = proj[0].shape[1]
    heads = columns // (6 * HEAD)
    width = heads * HEAD
    order, first, last, doc_row, doc_col, pos_col, gdoc_col, gdoc_row, plain_col = info
    globs = pos_col.shape[0]
    tiles = length // QTILE
    bf16, f32 = jnp.bfloat16, jnp.float32
    wide = heads * QTILE
    anywhere = pl.BlockSpec(memory_space=pl.ANY)
    return pl.pallas_call(
        partial(attend_back_kernel, heads, plan, (len(proj), len(grad_context))),
        out_shape=jax.ShapeDtypeStruct((length, columns), bf16),
        grid_spec=pltpu.PrefetchScalarGridSpec(
            num_scalar_prefetch=3,
            grid=(tiles,),
            in_specs=[anywhere] * (len(proj) + len(grad_context) + 1) + [
                whole_block((heads, length)),
                whole_block((1, heads * globs)),
                whole_block((1, length)),
                whole_block((length, 1)),
                whole_block((globs, 1)),
                whole_block((globs, 1)),
                whole_block((1, heads * globs)),
                whole_block((length, 1)),
            ],
            out_specs=whole_block((length, columns)),
            scratch_shapes=[
                pltpu.VMEM((length, columns), bf16),
                pltpu.VMEM((length, width), bf16),
                pltpu.VMEM((length, width), bf16),
                pltpu.VMEM((width, length), bf16),
                pltpu.VMEM((globs, length), bf16),
                pltpu.VMEM((globs, width), bf16),
                pltpu.VMEM((width, globs), bf16),
                pltpu.VMEM((globs, width), bf16),
                pltpu.VMEM((globs, width), f32),
                pltpu.VMEM((globs, width), f32),
                pltpu.VMEM((length, width), f32),
                pltpu.VMEM((length, width), f32),
                pltpu.VMEM((heads * globs, width), bf16),
                pltpu.VMEM((heads * globs, width), bf16),
                pltpu.VMEM((heads * globs, width), f32),
                pltpu.VMEM((width, wide), bf16),
                pltpu.VMEM((width, wide), bf16),
                pltpu.VMEM((wide, width), bf16),
                pltpu.VMEM((wide, width), bf16),
                pltpu.VMEM((KTILE, wide), bf16),
                pltpu.VMEM((KTILE, wide), bf16),
                pltpu.VMEM((width, QTILE), f32),
                pltpu.SemaphoreType.DMA((length // plan[2],)),
                pltpu.SemaphoreType.DMA((length // plan[2],)),
                pltpu.SemaphoreType.DMA((length // plan[2],)),
            ],
        ),
        compiler_params=pltpu.CompilerParams(
            dimension_semantics=("arbitrary",), vmem_limit_bytes=VMEM_BYTES
        ),
        cost_estimate=pl.CostEstimate(
            flops=4 * length * 1024 * width, bytes_accessed=4 * length * width,
            transcendentals=length * 1024 * heads,
        ),
        name="attend_back",
    )(
        order, first, last, *proj, *grad_context, context, *log_sums,
        doc_row, doc_col, pos_col, gdoc_col, gdoc_row, plain_col,
    )


def sequence_info(docs_row, glob_pos, order, heads):
    length = docs_row.shape[0]
    tiles = length // QTILE
    firsts = jnp.arange(tiles, dtype=jnp.int32) * QTILE
    tile_docs = docs_row.reshape(tiles, QTILE)
    doc_start = jnp.sum(docs_row[None, :] < tile_docs[:, :1], 1, dtype=jnp.int32)
    doc_end = jnp.sum(docs_row[None, :] <= tile_docs[:, -1:], 1, dtype=jnp.int32)
    first = jnp.maximum(firsts - HALF, doc_start) // KTILE
    last = (jnp.minimum(firsts + QTILE + HALF, doc_end) + KTILE - 1) // KTILE
    hit = glob_pos[:, None] == jnp.arange(length, dtype=jnp.int32)[None, :]
    glob_docs = jnp.sum(jnp.where(hit, docs_row[None, :], 0), 1, dtype=jnp.int32)
    plain_col = jnp.where(jnp.any(hit, 0), 0.0, 1.0)[:, None]
    return (
        order,
        first,
        last,
        docs_row[None, :],
        docs_row[:, None],
        glob_pos[:, None],
        glob_docs[:, None],
        jnp.tile(glob_docs, heads)[None, :],
        plain_col.astype(jnp.float32),
    )


def norm_forward(resid, gain, shift):
    centred = resid - jnp.mean(resid, -1, keepdims=True)
    scale = lax.rsqrt(jnp.mean(centred * centred, -1, keepdims=True) + 1e-05)
    normed = centred * scale
    return normed * gain + shift, normed, scale


def norm_backward(grad, normed, scale, gain):
    weighted = grad * gain
    mean_one = jnp.mean(weighted, -1, keepdims=True)
    mean_two = jnp.mean(weighted * normed, -1, keepdims=True)
    grad_in = (weighted - mean_one - normed * mean_two) * scale
    return grad_in, jnp.stack([jnp.sum(grad * normed, 0), jnp.sum(grad, 0)])


def gelu_pair(up):
    cdf = 0.5 * (1.0 + lax.erf(up * (0.5**0.5)))
    slope = cdf + up * (jnp.exp(-0.5 * up * up) * (1.0 / math.sqrt(2.0 * math.pi)))
    return (up * cdf).astype(jnp.bfloat16), slope.astype(jnp.bfloat16)


def after(value, *others):
    return lax.optimization_barrier((value,) + others)[0]


def unpack_kernel(blocks, each, per_half, home_ref, mine_ref, theirs_ref, out_ref):
    upper = pl.program_id(0) < per_half
    take_mine = upper == (home_ref[0] == 1)
    for index in range(blocks):
        cols = slice(index * each, (index + 1) * each)
        value = jnp.where(
            take_mine, mine_ref[:, cols].astype(jnp.float32), theirs_ref[:, cols].astype(jnp.float32)
        )
        out_ref[index] = value


def unpack(home, mine, theirs, blocks, each):
    half, columns = mine.shape
    tile = min(128, half)
    per_half = half // tile
    source = pl.BlockSpec((tile, columns), lambda step, _: (lax.rem(step, per_half), 0))
    return pl.pallas_call(
        partial(unpack_kernel, blocks, each, per_half),
        out_shape=jax.ShapeDtypeStruct((blocks, 2 * half, each), jnp.float32),
        grid_spec=pltpu.PrefetchScalarGridSpec(
            num_scalar_prefetch=1,
            grid=(2 * per_half,),
            in_specs=[source, source],
            out_specs=pl.BlockSpec((blocks, tile, each), lambda step, _: (0, step, 0)),
        ),
        compiler_params=pltpu.CompilerParams(dimension_semantics=("arbitrary",)),
        name="unpack",
    )(home, mine, theirs)


def gated(value, *others):
    zero = 0.0
    for other in others:
        corner = lax.slice(other, (0,) * other.ndim, (1,) * other.ndim)
        zero = zero + corner.reshape(()).astype(jnp.float32) * 0.0
    return (value.astype(jnp.float32) + zero).astype(value.dtype)


def shards(tokens, cotangent, doc_ids, global_flags, w_attn, w_out, w_up, w_down, ln_gain, ln_bias):
    bf16, f32 = jnp.bfloat16, jnp.float32
    sections = lax.axis_size("section")
    slots = lax.axis_size("tensor")
    copies = lax.axis_size("dp")
    micro = tokens.shape[0]
    inner = slots // micro
    section = lax.axis_index("section")
    slot = lax.axis_index("tensor")
    row = slot // inner
    lane = slot % inner
    width = tokens.shape[3]
    chunk = tokens.shape[2]
    rows = min(QTILE, chunk)
    parts = chunk // rows
    plan = (inner, parts, rows)
    crossed = inner == 2
    joint = ("section", "tensor")
    groups = [[a * inner + b for b in range(inner)] for a in range(micro)]

    def device(s, a, b):
        return s * slots + a * inner + b

    def route(value, link):
        pairs = []
        for s in range(sections):
            for a in range(micro):
                for b in range(inner):
                    target = link(s, a, b)
                    if target is not None and target != (s, a, b):
                        pairs.append((device(s, a, b), device(*target)))
        return lax.ppermute(value, joint, pairs)

    def other_core(value):
        return lax.ppermute(value, "section", [(0, 1), (1, 0)])

    def other_row(value):
        return route(value, lambda s, a, b: (s, 1 - a, b))

    def other_lane(value):
        return route(value, lambda s, a, b: (s, a, 1 - b))

    class ByLane:
        home = section == row
        swap = staticmethod(other_lane)

        @staticmethod
        def keeper(s, a, b):
            return a

        @staticmethod
        def across(s, a, b):
            return (s, 1 - a, b)

    class ByRow:
        home = section == lane
        swap = staticmethod(other_row)

        @staticmethod
        def keeper(s, a, b):
            return b

        @staticmethod
        def across(s, a, b):
            return (s, a, 1 - b)

    split_attn = ByLane
    split_mlp = ByRow if crossed else ByLane

    def gather(own, split, hop=None):
        with jax.named_scope("gsec"):
            near = jnp.concatenate([own, other_core(own)], 0)
        if not crossed:
            if inner == 1:
                return [near]
            return [lax.all_gather(near, "tensor", axis=0, tiled=True, axis_index_groups=groups)]
        if hop is None:
            with jax.named_scope("ghop"):
                hop = split.swap(own)
        with jax.named_scope("gsec2"):
            return [near, jnp.concatenate([hop, other_core(hop)], 0)]

    def scatter_begin(partials, gates=()):
        if not crossed:
            blocks = partials[0].reshape(inner, 2, rows, -1)
            ours, theirs = blocks[:, 0], blocks[:, 1].astype(bf16)
            total = (ours + other_core(theirs).astype(f32)).reshape(inner * rows, -1)
            return total.astype(bf16), None
        near, far = partials
        with jax.named_scope("ssec"):
            leaving = far[:rows] + other_core(far[rows:].astype(bf16)).astype(f32)
            leaving = gated(leaving, *gates)
        with jax.named_scope("ssec2"):
            staying = near[:rows] + other_core(near[rows:].astype(bf16)).astype(f32)
        return leaving.astype(bf16), staying

    def scatter_end(begun, split):
        leaving, staying = begun
        if not crossed:
            if inner == 1:
                return leaving.astype(f32)
            return lax.psum_scatter(
                leaving, "tensor", scatter_dimension=0, tiled=True, axis_index_groups=groups
            ).astype(f32)
        with jax.named_scope("shop"):
            return staying + split.swap(leaving).astype(f32)

    def scatter_all(begun, split):
        sums = [scatter_end(item, split) for item in begun]
        if not crossed:
            return sums
        return [
            gated(item, begun[p + 1][0]) if p + 1 < len(sums) else item
            for p, item in enumerate(sums)
        ]

    def cut(array):
        per_part = 2 * inner * rows
        per_group = 2 * rows if crossed else per_part
        return [
            [array[p * per_part + g : p * per_part + g + per_group] for g in range(0, per_part, per_group)]
            for p in range(parts)
        ]

    def joined(pieces):
        return jnp.concatenate([piece for part in pieces for piece in part], 0)

    def flat(pieces):
        return [piece for part in pieces for piece in part]

    def part_rows(array):
        return [array[p * rows : (p + 1) * rows] for p in range(parts)]

    def own_rows(array):
        mine = lax.dynamic_index_in_dim(array[:, 0], row, 0, False)
        theirs = lax.dynamic_index_in_dim(array[:, 0], 1 - row, 0, False)
        moved = route(theirs, lambda s, a, b: (s, 1 - a, b) if s == a else None)
        return mine, moved

    def fetch(weight, layer, split):
        def across(s, a, b):
            if s != layer:
                return None
            _, a2, b2 = split.across(s, a, b)
            return (split.keeper(s, a, b), a2, b2)

        def within(s, a, b):
            return (split.keeper(s, a, b), a, b) if s == layer else None

        far = route(weight, across)
        near = route(weight, within)
        return jnp.where(split.home, jnp.where(section == layer, weight, near), far)

    attn_table = w_attn[0].reshape(width, -1)
    mlp_pack = jnp.concatenate([w_up[0], w_down[0].reshape(width, -1)], 1)

    def attn_unpack(pack):
        columns = w_attn.shape[2] * w_attn.shape[3]
        return pack[:, :columns], pack[:, columns:].reshape(w_out.shape[1:])

    def mlp_unpack(pack):
        columns = w_up.shape[2]
        return pack[:, :columns], pack[:, columns:].reshape(w_down.shape[1:])

    mine, moved = own_rows(tokens)
    own = part_rows(jnp.where(ByLane.home, mine, moved))
    hops = []
    if crossed:
        early = route(mine, lambda s, a, b: (s, a, 1 - b) if s == a else None)
        late = route(moved, lambda s, a, b: (s, a, 1 - b) if s != a else None)
        hops = part_rows(jnp.where(ByLane.home, early, late))
    attn_weights = [None] * sections
    mlp_weights = [None] * sections
    with jax.named_scope("W0attn"):
        first_weight = fetch(attn_table, 0, split_attn)
    with jax.named_scope("W0out"):
        second_weight = fetch(after(w_out[0], *hops), 0, split_attn)
    with jax.named_scope("W0mlp"):
        arriving = fetch(after(mlp_pack, *own, *hops), 0, split_mlp)

    heads = w_attn.shape[3] // HEAD
    docs = lax.dynamic_index_in_dim(doc_ids[:, 0], row, 0, False)
    flags = lax.dynamic_index_in_dim(global_flags[:, 0], row, 0, False)
    order = jnp.stack([section, lane if crossed else jnp.zeros_like(lane)]).astype(jnp.int32)
    info = sequence_info(docs, flags, order, heads)
    attn_pack = jnp.concatenate([attn_table, w_out[0].reshape(width, -1)], 1)
    first_weight, second_weight, attn_pack, mlp_pack, *info = lax.optimization_barrier(
        (first_weight, second_weight, attn_pack, mlp_pack, *info)
    )
    attn_weights[0] = (first_weight, second_weight)

    gains_own = jnp.stack([ln_gain[0], ln_bias[0]])
    gains_other = other_core(gains_own)
    norms = [jnp.where(section == layer, gains_own, gains_other) for layer in range(sections)]

    saved, outputs, peaks = [], [], []
    for layer in range(sections):
        gains, shifts = norms[layer]
        attn_w, out_w = attn_weights[layer]
        with jax.named_scope(f"F{layer}in"):
            inputs = [
                gather(own[p], split_attn, hops[p] if layer == 0 and crossed else None)
                for p in range(parts)
            ]
            proj = [[mm(piece, attn_w, NN, bf16) for piece in part] for part in inputs]
        context, lse, glse, *tops = attend(flat(proj), info, plan)
        peaks.append(tops)
        if layer == 0:
            with jax.named_scope("W1attn"):
                pack = fetch(after(attn_pack, *flat(proj)), 1, split_attn)
            context, arriving, pack = lax.optimization_barrier((context, arriving, pack))
            mlp_weights[0], attn_weights[1] = mlp_unpack(arriving), attn_unpack(pack)
        else:
            with jax.named_scope("W1mlp"):
                pack = fetch(after(mlp_pack, *flat(proj)), 1, split_mlp)
            with jax.named_scope("COT"):
                mine, moved = own_rows(after(cotangent, *flat(proj)))
            context, pack, mine, moved = lax.optimization_barrier((context, pack, mine, moved))
            mlp_weights[1] = mlp_unpack(pack)
            grad_out = part_rows(jnp.where(ByLane.home, mine, moved).astype(f32))
        up_w, down_w = mlp_weights[layer]
        with jax.named_scope(f"F{layer}out"):
            sums = scatter_all(
                [scatter_begin([mm(piece, out_w) for piece in part]) for part in cut(context)],
                split_attn,
            )
        hidden, hidden_low, norms_one = [], [], []
        for p in range(parts):
            with jax.named_scope(f"F{layer}norm1"):
                value = gated(sums[p], hidden_low[-1]) if p else sums[p]
                value, normed, scale = norm_forward(own[p].astype(f32) + value, gains[0], shifts[0])
                hidden.append(value)
                hidden_low.append(value.astype(bf16))
                norms_one.append((normed, scale))
        hidden_rows, acts, slopes, begun = [], [], [], []
        for p in range(parts):
            with jax.named_scope(f"F{layer}mlp{p}"):
                hidden_rows.append(gather(hidden_low[p], split_mlp))
                pairs = [gelu_pair(mm(piece, up_w)) for piece in hidden_rows[p]]
                acts.append([act for act, _ in pairs])
                slopes.append([slope for _, slope in pairs])
                begun.append(
                    scatter_begin([mm(act, down_w) for act in acts[p]], hidden_low[p + 1 : p + 2])
                )
        with jax.named_scope(f"F{layer}mlp"):
            sums = scatter_all(begun, split_mlp)
        outs, norms_two = [], []
        for p in range(parts):
            with jax.named_scope(f"F{layer}norm2"):
                value = gated(sums[p], outs[-1]) if p else sums[p]
                value, normed, scale = norm_forward(hidden[p] + value, gains[1], shifts[1])
                norms_two.append((normed, scale))
                outs.append(value.astype(bf16))
        own = outs
        outputs.append(jnp.concatenate(outs, 0))
        saved.append(
            (inputs, proj, context, (lse, glse), norms_one, hidden_rows, acts, slopes, norms_two)
        )

    def to_owner(upper, lower, split, gates=()):
        def first_link(s, a, b):
            if s == split.keeper(s, a, b):
                return (1 - s, a, b)
            return split.across(s, a, b)

        def second_link(s, a, b):
            if s == split.keeper(s, a, b):
                return None
            _, a2, b2 = split.across(s, a, b)
            return (1 - s, a2, b2)

        first = route(gated(jnp.where(split.home, lower, upper), *gates), first_link)
        second = route(lower, second_link)
        part = first.astype(f32) + jnp.where(split.home, upper, second).astype(f32)
        return part.astype(bf16)

    earlier = ()

    def dp_sum(*terms):
        nonlocal earlier
        terms = [after(term, *earlier) for term in terms]
        earlier = lax.psum(tuple(terms), "dp")
        return earlier

    def pick(values):
        return jnp.where(section == 0, values[0], values[1])

    def placed(chunk, layer):
        arrived = []
        for index in range(micro):
            moved = route(chunk, lambda s, a, b: (layer, s, b) if a == index else None)
            stays = (section == layer) & ByLane.home & (row == index)
            arrived.append(jnp.where(stays, chunk, moved))
        return arrived

    def send_attn(pack, gates):
        half = width // 2
        return to_owner(pack[:half], pack[half:], split_attn, gates)

    attn_sums = [None] * sections
    mlp_sums = [None] * sections
    norm_sums = [None] * sections
    out_rows = [None] * sections
    grad_rows = [None] * sections
    for layer in reversed(range(sections)):
        (attn_w, out_w), (up_w, down_w) = attn_weights[layer], mlp_weights[layer]
        gains, _ = norms[layer]
        inputs, proj, context, log_sums, norms_one, hidden_rows, acts, slopes, norms_two = saved[layer]
        grads_two, low, sums_two = [], [], []
        for p in range(parts):
            with jax.named_scope(f"B{layer}norm2"):
                value = gated(grad_out[p], low[-1]) if p else grad_out[p]
                value, sums = norm_backward(value, *norms_two[p], gains[1])
                grads_two.append(value)
                low.append(value.astype(bf16))
                sums_two.append(sums)
        grad_mlp, grad_up, begun = [], [], []
        for p in range(parts):
            with jax.named_scope(f"B{layer}mlp{p}"):
                grad_mlp.append(gather(low[p], split_mlp))
                grad_up.append(
                    [
                        (mm(piece, down_w, NT) * slope.astype(f32)).astype(bf16)
                        for piece, slope in zip(grad_mlp[p], slopes[p])
                    ]
                )
                begun.append(
                    scatter_begin([mm(piece, up_w, NT) for piece in grad_up[p]], low[p + 1 : p + 2])
                )
        with jax.named_scope(f"B{layer}mlp"):
            sums = scatter_all(begun, split_mlp)
        with jax.named_scope(f"B{layer}wmlp"):
            grad_up_w = mm(joined(hidden_rows), joined(grad_up), TN, bf16)
            grad_down_w = mm(joined(acts), joined(grad_mlp), TN, bf16)
            sums[-1] = gated(sums[-1], grad_up_w, grad_down_w)
        grads_one, low, sums_one = [], [], []
        for p in range(parts):
            with jax.named_scope(f"B{layer}norm1"):
                value = gated(sums[p], low[-1]) if p else sums[p]
                value, total = norm_backward(value + grads_two[p], *norms_one[p], gains[0])
                grads_one.append(value)
                low.append(value.astype(bf16))
                sums_one.append(total)
        norm_sums[layer] = (sums_one, sums_two)
        grad_attn, grad_context = [], []
        for p in range(parts):
            with jax.named_scope(f"B{layer}ctx{p}"):
                grad_attn.append(gather(low[p], split_attn))
                grad_context.append([mm(piece, out_w, NT, bf16) for piece in grad_attn[p]])
        with jax.named_scope(f"B{layer}wmlp"):
            mlp_parts = to_owner(
                grad_up_w.reshape(width, -1), grad_down_w.reshape(width, -1), split_mlp,
                flat(grad_context) if layer else low,
            )
        if layer == 0:
            *grad_context[-1], mlp_sums[1] = lax.optimization_barrier(
                (*grad_context[-1], mlp_sums[1])
            )
        grad_context = flat(grad_context)
        if layer == 0:
            with jax.named_scope("B1wattn"):
                attn_parts = send_attn(pack, grad_context)
            *grad_context, mlp_parts = lax.optimization_barrier((*grad_context, mlp_parts))
            mlp_sums[0] = dp_sum(mlp_parts)[0]
        grad_proj = attend_back(flat(proj), context, log_sums, grad_context, info, plan)
        if layer == 1:
            with jax.named_scope("OUTROWS"):
                ready = lax.optimization_barrier((*outputs, *grad_context))[:sections]
                for index in range(sections):
                    out_rows[index] = placed(ready[index], index)
        if layer == 1:
            grad_proj, mlp_parts = lax.optimization_barrier((grad_proj, mlp_parts))
            mlp_sums[1] = dp_sum(mlp_parts)[0]
        else:
            grad_proj, attn_parts = lax.optimization_barrier((grad_proj, attn_parts))
        with jax.named_scope(f"B{layer}wattn"):
            grad_attn_w = mm(joined(inputs), grad_proj, TN, bf16)
            grad_out_w = mm(context, joined(grad_attn), TN, bf16)
            pack = jnp.concatenate([grad_attn_w, grad_out_w.reshape(width, -1)], 1)
        if layer == 0:
            grad_proj = after(grad_proj, pack)
        grad_low = []
        grad_proj_parts = cut(grad_proj)
        if layer == 0:
            *grad_proj_parts[-1], mlp_sums[0] = lax.optimization_barrier(
                (*grad_proj_parts[-1], mlp_sums[0])
            )
        with jax.named_scope(f"B{layer}in"):
            sums = scatter_all(
                [
                    scatter_begin(
                        [mm(piece, attn_w, NT) for piece in part],
                        (),
                    )
                    for part in grad_proj_parts
                ],
                split_attn,
            )
        for p in range(parts):
            with jax.named_scope(f"B{layer}in"):
                value = gated(sums[p], grad_low[-1]) if p else sums[p]
                grad_low.append((value + grads_one[p]).astype(bf16))
        grad_out = [piece.astype(f32) for piece in grad_low]
        if layer == 0:
            with jax.named_scope("B0wattn"):
                last_parts = send_attn(pack, ())
                attn_sums[1], attn_sums[0] = dp_sum(attn_parts, last_parts)
        with jax.named_scope("GRADROWS"):
            grad_rows[layer] = placed(jnp.concatenate(grad_low, 0), layer)

    def stacked_rows(by_layer):
        return jnp.stack([pick([by_layer[0][m], by_layer[1][m]]) for m in range(micro)])[None, :, None]

    def placed_weight(terms, split):
        mine = pick(terms)
        theirs = other_core(pick(terms[::-1]))
        first = jnp.where(split.home, mine, theirs)
        second = jnp.where(split.home, theirs, mine)
        return first.astype(f32), second.astype(f32)

    def dp_butterfly(value, combine):
        if copies & (copies - 1):
            gathered = lax.all_gather(value, "dp", axis=0)
            total = gathered[0]
            for index in range(1, copies):
                total = combine(total, gathered[index])
            return total
        distance = 1
        while distance < copies:
            pairs = [(d, d ^ distance) for d in range(copies)]
            value = combine(value, lax.ppermute(value, "dp", pairs))
            distance *= 2
        return value

    with jax.named_scope("NORMSUM"):
        mine = [
            jnp.stack([sum(sums_one[1:], sums_one[0]), sum(sums_two[1:], sums_two[0])])
            for sums_one, sums_two in norm_sums
        ]
        mine = lax.optimization_barrier((*mine, last_parts))[:sections]
        norm_sum = pick(mine) + other_core(pick(mine[::-1]))
        if crossed:
            norm_sum = norm_sum + other_row(norm_sum)
            norm_sum = norm_sum + other_lane(norm_sum)
        else:
            norm_sum = lax.psum(norm_sum, "tensor")
        norm_sum = dp_butterfly(norm_sum, jnp.add)
    with jax.named_scope("PEAK"):
        peak_all = lax.optimization_barrier((*flat(peaks), last_parts))[:-1]
        peak_all = jnp.stack(
            [jnp.max(value.reshape(heads, -1), 1) for value in peak_all]
        ).reshape(sections, 2, heads)
        peak_all = jnp.maximum(peak_all, other_row(peak_all))
        peak_all = dp_butterfly(peak_all, jnp.maximum)
        peak_here = jnp.where(ByLane.home, pick(peak_all), other_core(pick(peak_all[::-1])))
    factors = jnp.sqrt(clip_limit / jnp.maximum(peak_here, clip_limit))
    columns = jnp.repeat(factors, HEAD, axis=1)
    attn_local = w_attn[0].astype(f32)
    clipped = jnp.stack(
        [
            attn_local[:, 0] * columns[0][None, :],
            attn_local[:, 1] * columns[0][None, :],
            attn_local[:, 3] * columns[1][None, :],
            attn_local[:, 4] * columns[1][None, :],
        ],
        1,
    )
    out_rows, grad_rows = stacked_rows(out_rows), stacked_rows(grad_rows)
    grad_up_w, grad_down_w = placed_weight(mlp_sums, split_mlp)
    attn_sums = [
        gated(term, out_rows, grad_rows, grad_up_w, grad_down_w, norm_sum, clipped)
        for term in attn_sums
    ]
    mine, theirs = pick(attn_sums), other_core(pick(attn_sums[::-1]))
    blocks, each = w_attn.shape[2:]
    home = split_attn.home.astype(jnp.int32).reshape(1)
    grad_attn_w = unpack(home, mine, theirs, blocks, each).transpose(1, 0, 2)
    halves = [half[:, blocks * each :].reshape(-1, w_out.shape[2]) for half in (mine, theirs)]
    grad_out_w = jnp.where(
        split_attn.home, jnp.concatenate(halves, 0), jnp.concatenate(halves[::-1], 0)
    ).astype(f32)

    return (
        out_rows,
        grad_rows,
        grad_attn_w[None],
        grad_out_w.reshape(w_out.shape),
        grad_up_w.reshape(w_up.shape),
        grad_down_w.reshape(w_down.shape),
        norm_sum[:, 0][None],
        norm_sum[:, 1][None],
        clipped[None],
    )


def solution(mesh):
    in_specs = (
        P(None, "dp", "tensor", None),
        P(None, "dp", "tensor", None),
        P(None, "dp", None),
        P(None, "dp", None),
        P("section", None, None, "tensor"),
        P("section", "tensor", None),
        P("section", None, "tensor"),
        P("section", "tensor", None),
        P("section", None, None),
        P("section", None, None),
    )
    out_specs = (
        P("section", None, "dp", "tensor", None),
        P("section", None, "dp", "tensor", None),
        P("section", None, None, "tensor"),
        P("section", "tensor", None),
        P("section", None, "tensor"),
        P("section", "tensor", None),
        P("section", None, None),
        P("section", None, None),
        P("section", None, None, "tensor"),
    )
    return jax.shard_map(shards, mesh=mesh, in_specs=in_specs, out_specs=out_specs, check_vma=False)
```

```python
import math
from functools import partial

import jax
import jax.numpy as jnp
from jax import lax
from jax.experimental import pallas as pl
from jax.experimental.pallas import tpu as pltpu
from jax.sharding import PartitionSpec as P

HEAD = 64
HALF = 512
QTILE = 256
KTILE = 512
VMEM_BYTES = 56 * 1024 * 1024

masked_fill = -1e30
clip_limit = 10.0
score_scale = HEAD ** (-0.5)

NN = (((1,), (0,)), ((), ()))
NT = (((1,), (1,)), ((), ()))
TN = (((0,), (0,)), ((), ()))


def mm(left, right, dims=NN, out=jnp.float32):
    return lax.dot_general(left, right, dims, preferred_element_type=jnp.float32).astype(out)


def tile_bias(first_key, first_query, key_docs, query_docs, keys, queries):
    key_pos = first_key + lax.broadcasted_iota(jnp.int32, (keys, queries), 0)
    query_pos = first_query + lax.broadcasted_iota(jnp.int32, (keys, queries), 1)
    gap = jnp.abs(key_pos - query_pos)
    return jnp.where((key_docs == query_docs) & (gap <= HALF), 0.0, masked_fill)


def far_bias(glob_pos, first_query, glob_docs, query_docs, globs, queries):
    query_pos = first_query + lax.broadcasted_iota(jnp.int32, (globs, queries), 1)
    gap = jnp.abs(glob_pos - query_pos)
    return jnp.where((glob_docs == query_docs) & (gap > HALF), 0.0, masked_fill)


def one_hot_rows(glob_pos, length):
    globs = glob_pos.shape[0]
    hit = lax.broadcasted_iota(jnp.int32, (globs, length), 1) == glob_pos
    return jnp.where(hit, 1.0, 0.0).astype(jnp.bfloat16)


def true_unit(place, order_ref, plan):
    inner, parts, _ = plan
    part, rest = place // (2 * inner), place % (2 * inner)
    side = (rest % 2) ^ order_ref[0]
    lane = (rest // 2) ^ order_ref[1]
    return (side * inner + lane) * parts + part


def local_unit(unit, order_ref, plan):
    inner, parts, _ = plan
    block, part = lax.div(unit, parts), lax.rem(unit, parts)
    side = lax.div(block, inner) ^ order_ref[0]
    lane = lax.rem(block, inner) ^ order_ref[1]
    return part * (2 * inner) + lane * 2 + side


def join_pieces(order_ref, pieces, joined_ref, sems, plan):
    rows = plan[2]
    copies = []
    place = 0
    for piece in pieces:
        for index in range(piece.shape[0] // rows):
            start = pl.multiple_of(true_unit(place, order_ref, plan) * rows, rows)
            copies.append(
                pltpu.make_async_copy(
                    piece.at[pl.ds(index * rows, rows), :],
                    joined_ref.at[pl.ds(start, rows), :],
                    sems.at[place],
                )
            )
            place += 1
    for copy in copies:
        copy.start()
    for copy in copies:
        copy.wait()


def store_local(out_ref, tile, cols, value, order_ref, plan):
    rows = plan[2]
    size = min(rows, value.shape[0])
    for index in range(value.shape[0] // size):
        row = tile * value.shape[0] + index * size
        place = local_unit(lax.div(row, rows), order_ref, plan)
        start = pl.multiple_of(place * rows + lax.rem(row, rows), size)
        out_ref[pl.ds(start, size), cols] = value[index * size : (index + 1) * size]


def diagonal_sum(blocks, heads, rows):
    owner = lax.broadcasted_iota(jnp.int32, (rows, heads * HEAD), 1) // HEAD
    total = jnp.zeros((rows, heads * HEAD), jnp.float32)
    for head in range(heads):
        total = total + jnp.where(owner == head, blocks[head * rows : (head + 1) * rows], 0.0)
    return total


def attend_kernel(
    heads,
    plan,
    count,
    order_ref,
    first_ref,
    last_ref,
    *refs,
):
    pieces, refs = refs[:count], refs[count:]
    attend_body(heads, plan, order_ref, first_ref, last_ref, pieces, *refs)


def attend_body(
    heads,
    plan,
    order_ref,
    first_ref,
    last_ref,
    pieces,
    doc_row_ref,
    doc_col_ref,
    pos_col_ref,
    gdoc_col_ref,
    gdoc_row_ref,
    ctx_ref,
    lse_ref,
    glse_ref,
    peak_ref,
    gpeak_ref,
    proj,
    values_t,
    hot,
    far_keys,
    far_values_t,
    gctx_t,
    gstack,
    gscores,
    wide,
    acc,
    top,
    total,
    sems,
):
    length = proj.shape[0]
    width = heads * HEAD
    globs = pos_col_ref.shape[0]
    step = pl.program_id(0)

    @pl.when(step == 0)
    def _():
        join_pieces(order_ref, pieces, proj, sems, plan)
        wide[...] = jnp.zeros_like(wide)
        gstack[...] = jnp.zeros_like(gstack)
        hot[...] = one_hot_rows(pos_col_ref[...], length)
        hot_all = hot[...]
        far_keys[...] = mm(hot_all, proj[:, width : 2 * width], out=jnp.bfloat16)
        far_values_t[...] = mm(hot_all, proj[:, 2 * width : 3 * width]).T.astype(jnp.bfloat16)
        queries = (mm(hot_all, proj[:, 3 * width : 4 * width]) * score_scale).astype(jnp.bfloat16)
        for head in range(heads):
            cols = slice(head * HEAD, (head + 1) * HEAD)
            gstack[head * globs : (head + 1) * globs, cols] = queries[:, cols]

        def score_tile(tile, best):
            rows = pl.ds(pl.multiple_of(tile * KTILE, KTILE), KTILE)
            values_t[:, rows] = proj[rows, 2 * width : 3 * width].T
            scores = mm(proj[rows, 4 * width : 5 * width], gstack[...], NT)
            scores = jnp.where(doc_col_ref[rows, :] == gdoc_row_ref[...], scores, masked_fill)
            gscores[rows, :] = scores
            return jnp.maximum(best, jnp.max(scores, 0, keepdims=True))

        best = lax.fori_loop(
            0, length // KTILE, score_tile, jnp.full((1, heads * globs), masked_fill, jnp.float32)
        )

        def sum_tile(tile, sums):
            rows = pl.ds(pl.multiple_of(tile * KTILE, KTILE), KTILE)
            weights = jnp.exp(gscores[rows, :] - best)
            gscores[rows, :] = weights
            return sums + jnp.sum(weights, 0, keepdims=True)

        sums = lax.fori_loop(
            0, length // KTILE, sum_tile, jnp.zeros((1, heads * globs), jnp.float32)
        )

        def value_tile(tile, blocks):
            rows = pl.ds(pl.multiple_of(tile * KTILE, KTILE), KTILE)
            probs = (gscores[rows, :] / sums).T.astype(jnp.bfloat16)
            return blocks + mm(probs, proj[rows, 5 * width : 6 * width])

        blocks = lax.fori_loop(
            0, length // KTILE, value_tile, jnp.zeros((heads * globs, width), jnp.float32)
        )
        gctx_t[...] = diagonal_sum(blocks, heads, globs).T.astype(jnp.bfloat16)
        glse_ref[...] = best + jnp.log(sums)
        gpeak_ref[...] = best

    start = pl.multiple_of(step * QTILE, QTILE)
    query_rows = pl.ds(start, QTILE)
    query_t = proj[query_rows, 0:width].T * score_scale
    for head in range(heads):
        rows = slice(head * HEAD, (head + 1) * HEAD)
        wide[rows, head * QTILE : (head + 1) * QTILE] = query_t[rows].astype(jnp.bfloat16)
    query_docs = doc_row_ref[:, query_rows]

    scores = mm(far_keys[...], wide[...])
    bias = far_bias(pos_col_ref[...], start, gdoc_col_ref[...], query_docs, globs, QTILE)
    for head in range(heads):
        cols = slice(head * QTILE, (head + 1) * QTILE)
        rows = slice(head * HEAD, (head + 1) * HEAD)
        part = scores[:, cols] + bias
        best = jnp.max(part, 0, keepdims=True)
        weights = jnp.exp(part - best)
        top[:, cols] = best
        total[:, cols] = jnp.sum(weights, 0, keepdims=True)
        acc[rows, :] = mm(far_values_t[rows, :], weights.astype(jnp.bfloat16))

    def key_tile(tile, carry):
        key_start = pl.multiple_of(tile * KTILE, KTILE)
        keys = pl.ds(key_start, KTILE)
        scores = mm(proj[keys, width : 2 * width], wide[...])
        bias = tile_bias(key_start, start, doc_col_ref[keys, :], query_docs, KTILE, QTILE)
        for head in range(heads):
            cols = slice(head * QTILE, (head + 1) * QTILE)
            rows = slice(head * HEAD, (head + 1) * HEAD)
            part = scores[:, cols] + bias
            old = top[:, cols]
            best = jnp.maximum(old, jnp.max(part, 0, keepdims=True))
            weights = jnp.exp(part - best)
            shrink = jnp.exp(old - best)
            top[:, cols] = best
            total[:, cols] = total[:, cols] * shrink + jnp.sum(weights, 0, keepdims=True)
            acc[rows, :] = acc[rows, :] * shrink + mm(
                values_t[rows, keys], weights.astype(jnp.bfloat16)
            )
        return carry

    lax.fori_loop(first_ref[step], last_ref[step], key_tile, 0)

    hot_tile = hot[:, query_rows]
    is_glob = jnp.max(hot_tile.astype(jnp.float32), 0, keepdims=True) > 0.5
    for head in range(heads):
        cols = slice(head * QTILE, (head + 1) * QTILE)
        rows = slice(head * HEAD, (head + 1) * HEAD)
        acc[rows, :] = acc[rows, :] / total[:, cols]
        lse_ref[head : head + 1, :] = top[:, cols] + jnp.log(total[:, cols])
    merged = jnp.where(is_glob, mm(gctx_t[...], hot_tile), acc[...])
    store_local(ctx_ref, step, slice(None), merged.T.astype(jnp.bfloat16), order_ref, plan)

    @pl.when(step == 0)
    def _():
        peak_ref[...] = top[...]

    @pl.when(step > 0)
    def _():
        peak_ref[...] = jnp.maximum(peak_ref[...], top[...])


def whole_block(shape):
    return pl.BlockSpec(shape, lambda *_: (0,) * len(shape), pipeline_mode=pl.Buffered(1))


def attend(proj, info, plan):
    length = sum(piece.shape[0] for piece in proj)
    columns = proj[0].shape[1]
    heads = columns // (6 * HEAD)
    width = heads * HEAD
    order, first, last, doc_row, doc_col, pos_col, gdoc_col, gdoc_row, _ = info
    globs = pos_col.shape[0]
    tiles = length // QTILE
    bf16, f32 = jnp.bfloat16, jnp.float32

    anywhere = pl.BlockSpec(memory_space=pl.ANY)
    return pl.pallas_call(
        partial(attend_kernel, heads, plan, len(proj)),
        out_shape=(
            jax.ShapeDtypeStruct((length, width), bf16),
            jax.ShapeDtypeStruct((heads, length), f32),
            jax.ShapeDtypeStruct((1, heads * globs), f32),
            jax.ShapeDtypeStruct((1, heads * QTILE), f32),
            jax.ShapeDtypeStruct((1, heads * globs), f32),
        ),
        grid_spec=pltpu.PrefetchScalarGridSpec(
            num_scalar_prefetch=3,
            grid=(tiles,),
            in_specs=[anywhere] * len(proj) + [
                whole_block((1, length)),
                whole_block((length, 1)),
                whole_block((globs, 1)),
                whole_block((globs, 1)),
                whole_block((1, heads * globs)),
            ],
            out_specs=(
                whole_block((length, width)),
                pl.BlockSpec((heads, QTILE), lambda step, *_: (0, step)),
                pl.BlockSpec((1, heads * globs), lambda *_: (0, 0)),
                pl.BlockSpec((1, heads * QTILE), lambda *_: (0, 0)),
                pl.BlockSpec((1, heads * globs), lambda *_: (0, 0)),
            ),
            scratch_shapes=[
                pltpu.VMEM((length, columns), bf16),
                pltpu.VMEM((width, length), bf16),
                pltpu.VMEM((globs, length), bf16),
                pltpu.VMEM((globs, width), bf16),
                pltpu.VMEM((width, globs), bf16),
                pltpu.VMEM((width, globs), bf16),
                pltpu.VMEM((heads * globs, width), bf16),
                pltpu.VMEM((length, heads * globs), f32),
                pltpu.VMEM((width, heads * QTILE), bf16),
                pltpu.VMEM((width, QTILE), f32),
                pltpu.VMEM((1, heads * QTILE), f32),
                pltpu.VMEM((1, heads * QTILE), f32),
                pltpu.SemaphoreType.DMA((length // plan[2],)),
            ],
        ),
        compiler_params=pltpu.CompilerParams(
            dimension_semantics=("arbitrary",), vmem_limit_bytes=VMEM_BYTES
        ),
        cost_estimate=pl.CostEstimate(
            flops=20 * length * 1024 * width, bytes_accessed=14 * length * width,
            transcendentals=length * 1024 * heads,
        ),
        name="attend",
    )(order, first, last, *proj, doc_row, doc_col, pos_col, gdoc_col, gdoc_row)


def attend_back_kernel(
    heads,
    plan,
    counts,
    order_ref,
    first_ref,
    last_ref,
    *refs,
):
    pieces, refs = refs[: counts[0]], refs[counts[0] :]
    grad_pieces, refs = refs[: counts[1]], refs[counts[1] :]
    attend_back_body(heads, plan, order_ref, first_ref, last_ref, pieces, grad_pieces, *refs)


def attend_back_body(
    heads,
    plan,
    order_ref,
    first_ref,
    last_ref,
    pieces,
    grad_pieces,
    ctx_piece_ref,
    lse_ref,
    glse_ref,
    doc_row_ref,
    doc_col_ref,
    pos_col_ref,
    gdoc_col_ref,
    gdoc_row_ref,
    plain_col_ref,
    out_ref,
    proj,
    ctx,
    grad,
    keys_t,
    hot,
    far_keys,
    far_keys_t,
    far_values,
    far_key_grad,
    far_value_grad,
    key_grad,
    value_grad,
    gquery,
    gout,
    gquery_grad,
    wide,
    wide_grad,
    stack,
    stack_grad,
    probs_low,
    grads_low,
    query_grad_t,
    proj_sems,
    ctx_sems,
    grad_sems,
):
    length = proj.shape[0]
    width = heads * HEAD
    globs = pos_col_ref.shape[0]
    tiles = length // KTILE
    step = pl.program_id(0)
    bf16 = jnp.bfloat16

    def store(tile, block, value):
        cols = slice(block * width, (block + 1) * width)
        store_local(out_ref, tile, cols, value.astype(bf16), order_ref, plan)

    @pl.when(step == 0)
    def _():
        join_pieces(order_ref, pieces, proj, proj_sems, plan)
        join_pieces(order_ref, [ctx_piece_ref], ctx, ctx_sems, plan)
        join_pieces(order_ref, grad_pieces, grad, grad_sems, plan)
        for ref in (wide, wide_grad, stack, stack_grad, gquery, gout):
            ref[...] = jnp.zeros_like(ref)
        for ref in (key_grad, value_grad, far_key_grad, far_value_grad):
            ref[...] = jnp.zeros_like(ref)
        gquery_grad[...] = jnp.zeros_like(gquery_grad)
        hot[...] = one_hot_rows(pos_col_ref[...], length)
        hot_all = hot[...]
        near = mm(hot_all, proj[:, width : 2 * width])
        far_keys[...] = near.astype(bf16)
        far_keys_t[...] = near.T.astype(bf16)
        far_values[...] = mm(hot_all, proj[:, 2 * width : 3 * width], out=bf16)
        queries = (mm(hot_all, proj[:, 3 * width : 4 * width]) * score_scale).astype(bf16)
        out_grad = mm(hot_all, grad[...])
        glob_ctx = mm(hot_all, ctx[...])
        product = out_grad * glob_ctx
        owner = lax.broadcasted_iota(jnp.int32, (globs, width), 1) // HEAD
        dots = []
        for head in range(heads):
            cols = slice(head * HEAD, (head + 1) * HEAD)
            rows = slice(head * globs, (head + 1) * globs)
            gquery[rows, cols] = queries[:, cols]
            gout[rows, cols] = out_grad[:, cols].astype(bf16)
            own = jnp.where(owner == head, product, 0.0)
            dots.append(jnp.sum(own, 1, keepdims=True))
        dot_row = jnp.broadcast_to(jnp.concatenate(dots, 0), (heads * globs, 128)).T[0:1]

        def glob_tile(tile, carry):
            rows = pl.ds(pl.multiple_of(tile * KTILE, KTILE), KTILE)
            keys_t[:, rows] = proj[rows, width : 2 * width].T
            scores = mm(proj[rows, 4 * width : 5 * width], gquery[...], NT)
            scores = jnp.where(doc_col_ref[rows, :] == gdoc_row_ref[...], scores, masked_fill)
            probs = jnp.exp(scores - glse_ref[...])
            grad_p = mm(proj[rows, 5 * width : 6 * width], gout[...], NT)
            grad_s = probs * (grad_p - dot_row)
            store(tile, 5, mm(probs.astype(bf16), gout[...]))
            store(tile, 4, mm(grad_s.astype(bf16), gquery[...]))
            gquery_grad[...] += mm(grad_s.T.astype(bf16), proj[rows, 4 * width : 5 * width])
            return carry

        lax.fori_loop(0, tiles, glob_tile, 0)
        query_grad = diagonal_sum(gquery_grad[...], heads, globs) * score_scale
        query_grad = query_grad.astype(bf16)

        def spread_tile(tile, carry):
            rows = pl.ds(pl.multiple_of(tile * KTILE, KTILE), KTILE)
            store(tile, 3, mm(hot[:, rows], query_grad, TN))
            return carry

        lax.fori_loop(0, tiles, spread_tile, 0)

    start = pl.multiple_of(step * QTILE, QTILE)
    query_rows = pl.ds(start, QTILE)
    query = proj[query_rows, 0:width].astype(jnp.float32) * score_scale
    query_t = query.T.astype(bf16)
    query = query.astype(bf16)
    grad_out = grad[query_rows, :].astype(jnp.float32) * plain_col_ref[query_rows, :]
    grad_out_t = grad_out.T
    product_t = grad_out_t * ctx[query_rows, :].astype(jnp.float32).T
    grad_out = grad_out.astype(bf16)
    grad_out_t = grad_out_t.astype(bf16)
    dots = []
    for head in range(heads):
        own = slice(head * HEAD, (head + 1) * HEAD)
        cols = slice(head * QTILE, (head + 1) * QTILE)
        wide[own, cols] = query_t[own]
        wide_grad[own, cols] = grad_out_t[own]
        stack[cols, own] = query[:, own]
        stack_grad[cols, own] = grad_out[:, own]
        dots.append(jnp.sum(product_t[own], 0, keepdims=True))
    query_docs = doc_row_ref[:, query_rows]

    def parts(scores, grad_p, bias, head):
        cols = slice(head * QTILE, (head + 1) * QTILE)
        shift = lse_ref[head : head + 1, query_rows]
        probs = jnp.exp(scores[:, cols] + bias - shift)
        grad_s = probs * (grad_p[:, cols] - dots[head])
        return probs.astype(bf16), grad_s.astype(bf16)

    scores = mm(far_keys[...], wide[...])
    grad_p = mm(far_values[...], wide_grad[...])
    bias = far_bias(pos_col_ref[...], start, gdoc_col_ref[...], query_docs, globs, QTILE)
    for head in range(heads):
        cols = slice(head * QTILE, (head + 1) * QTILE)
        own = slice(head * HEAD, (head + 1) * HEAD)
        probs, grad_s = parts(scores, grad_p, bias, head)
        probs_low[0:globs, cols] = probs
        grads_low[0:globs, cols] = grad_s
        query_grad_t[own, :] = mm(far_keys_t[own, :], grad_s)
    far_value_grad[...] += mm(probs_low[0:globs, :], stack_grad[...])
    far_key_grad[...] += mm(grads_low[0:globs, :], stack[...])

    def key_tile(tile, carry):
        key_start = pl.multiple_of(tile * KTILE, KTILE)
        keys = pl.ds(key_start, KTILE)
        scores = mm(proj[keys, width : 2 * width], wide[...])
        grad_p = mm(proj[keys, 2 * width : 3 * width], wide_grad[...])
        bias = tile_bias(key_start, start, doc_col_ref[keys, :], query_docs, KTILE, QTILE)
        for head in range(heads):
            cols = slice(head * QTILE, (head + 1) * QTILE)
            own = slice(head * HEAD, (head + 1) * HEAD)
            probs, grad_s = parts(scores, grad_p, bias, head)
            probs_low[:, cols] = probs
            grads_low[:, cols] = grad_s
            query_grad_t[own, :] += mm(keys_t[own, keys], grad_s)
        value_grad[keys, :] += mm(probs_low[...], stack_grad[...])
        key_grad[keys, :] += mm(grads_low[...], stack[...])
        return carry

    lax.fori_loop(first_ref[step], last_ref[step], key_tile, 0)
    store(step, 0, (query_grad_t[...] * score_scale).T)

    @pl.when(step == pl.num_programs(0) - 1)
    def _():
        far_key = far_key_grad[...].astype(bf16)
        far_value = far_value_grad[...].astype(bf16)

        def close_tile(tile, carry):
            rows = pl.ds(pl.multiple_of(tile * KTILE, KTILE), KTILE)
            hot_tile = hot[:, rows]
            key_sum = key_grad[rows, :] + mm(hot_tile, far_key, TN)
            value_sum = value_grad[rows, :] + mm(hot_tile, far_value, TN)
            store(tile, 1, key_sum)
            store(tile, 2, value_sum)
            return carry

        lax.fori_loop(0, tiles, close_tile, 0)


def attend_back(proj, context, log_sums, grad_context, info, plan):
    length = context.shape[0]
    columns = proj[0].shape[1]
    heads = columns // (6 * HEAD)
    width = heads * HEAD
    order, first, last, doc_row, doc_col, pos_col, gdoc_col, gdoc_row, plain_col = info
    globs = pos_col.shape[0]
    tiles = length // QTILE
    bf16, f32 = jnp.bfloat16, jnp.float32
    wide = heads * QTILE
    anywhere = pl.BlockSpec(memory_space=pl.ANY)
    return pl.pallas_call(
        partial(attend_back_kernel, heads, plan, (len(proj), len(grad_context))),
        out_shape=jax.ShapeDtypeStruct((length, columns), bf16),
        grid_spec=pltpu.PrefetchScalarGridSpec(
            num_scalar_prefetch=3,
            grid=(tiles,),
            in_specs=[anywhere] * (len(proj) + len(grad_context) + 1) + [
                whole_block((heads, length)),
                whole_block((1, heads * globs)),
                whole_block((1, length)),
                whole_block((length, 1)),
                whole_block((globs, 1)),
                whole_block((globs, 1)),
                whole_block((1, heads * globs)),
                whole_block((length, 1)),
            ],
            out_specs=whole_block((length, columns)),
            scratch_shapes=[
                pltpu.VMEM((length, columns), bf16),
                pltpu.VMEM((length, width), bf16),
                pltpu.VMEM((length, width), bf16),
                pltpu.VMEM((width, length), bf16),
                pltpu.VMEM((globs, length), bf16),
                pltpu.VMEM((globs, width), bf16),
                pltpu.VMEM((width, globs), bf16),
                pltpu.VMEM((globs, width), bf16),
                pltpu.VMEM((globs, width), f32),
                pltpu.VMEM((globs, width), f32),
                pltpu.VMEM((length, width), f32),
                pltpu.VMEM((length, width), f32),
                pltpu.VMEM((heads * globs, width), bf16),
                pltpu.VMEM((heads * globs, width), bf16),
                pltpu.VMEM((heads * globs, width), f32),
                pltpu.VMEM((width, wide), bf16),
                pltpu.VMEM((width, wide), bf16),
                pltpu.VMEM((wide, width), bf16),
                pltpu.VMEM((wide, width), bf16),
                pltpu.VMEM((KTILE, wide), bf16),
                pltpu.VMEM((KTILE, wide), bf16),
                pltpu.VMEM((width, QTILE), f32),
                pltpu.SemaphoreType.DMA((length // plan[2],)),
                pltpu.SemaphoreType.DMA((length // plan[2],)),
                pltpu.SemaphoreType.DMA((length // plan[2],)),
            ],
        ),
        compiler_params=pltpu.CompilerParams(
            dimension_semantics=("arbitrary",), vmem_limit_bytes=VMEM_BYTES
        ),
        cost_estimate=pl.CostEstimate(
            flops=4 * length * 1024 * width, bytes_accessed=4 * length * width,
            transcendentals=length * 1024 * heads,
        ),
        name="attend_back",
    )(
        order, first, last, *proj, *grad_context, context, *log_sums,
        doc_row, doc_col, pos_col, gdoc_col, gdoc_row, plain_col,
    )


def sequence_info(docs_row, glob_pos, order, heads):
    length = docs_row.shape[0]
    tiles = length // QTILE
    firsts = jnp.arange(tiles, dtype=jnp.int32) * QTILE
    tile_docs = docs_row.reshape(tiles, QTILE)
    doc_start = jnp.sum(docs_row[None, :] < tile_docs[:, :1], 1, dtype=jnp.int32)
    doc_end = jnp.sum(docs_row[None, :] <= tile_docs[:, -1:], 1, dtype=jnp.int32)
    first = jnp.maximum(firsts - HALF, doc_start) // KTILE
    last = (jnp.minimum(firsts + QTILE + HALF, doc_end) + KTILE - 1) // KTILE
    hit = glob_pos[:, None] == jnp.arange(length, dtype=jnp.int32)[None, :]
    glob_docs = jnp.sum(jnp.where(hit, docs_row[None, :], 0), 1, dtype=jnp.int32)
    plain_col = jnp.where(jnp.any(hit, 0), 0.0, 1.0)[:, None]
    return (
        order,
        first,
        last,
        docs_row[None, :],
        docs_row[:, None],
        glob_pos[:, None],
        glob_docs[:, None],
        jnp.tile(glob_docs, heads)[None, :],
        plain_col.astype(jnp.float32),
    )


def norm_forward(resid, gain, shift):
    centred = resid - jnp.mean(resid, -1, keepdims=True)
    scale = lax.rsqrt(jnp.mean(centred * centred, -1, keepdims=True) + 1e-05)
    normed = centred * scale
    return normed * gain + shift, normed, scale


def norm_backward(grad, normed, scale, gain):
    weighted = grad * gain
    mean_one = jnp.mean(weighted, -1, keepdims=True)
    mean_two = jnp.mean(weighted * normed, -1, keepdims=True)
    grad_in = (weighted - mean_one - normed * mean_two) * scale
    return grad_in, jnp.stack([jnp.sum(grad * normed, 0), jnp.sum(grad, 0)])


def gelu_pair(up):
    cdf = 0.5 * (1.0 + lax.erf(up * (0.5**0.5)))
    slope = cdf + up * (jnp.exp(-0.5 * up * up) * (1.0 / math.sqrt(2.0 * math.pi)))
    return (up * cdf).astype(jnp.bfloat16), slope.astype(jnp.bfloat16)


def after(value, *others):
    return lax.optimization_barrier((value,) + others)[0]


def unpack_kernel(blocks, each, per_half, home_ref, mine_ref, theirs_ref, out_ref):
    upper = pl.program_id(0) < per_half
    take_mine = upper == (home_ref[0] == 1)
    for index in range(blocks):
        cols = slice(index * each, (index + 1) * each)
        value = jnp.where(
            take_mine, mine_ref[:, cols].astype(jnp.float32), theirs_ref[:, cols].astype(jnp.float32)
        )
        out_ref[index] = value


def unpack(home, mine, theirs, blocks, each):
    half, columns = mine.shape
    tile = min(128, half)
    per_half = half // tile
    source = pl.BlockSpec((tile, columns), lambda step, _: (lax.rem(step, per_half), 0))
    return pl.pallas_call(
        partial(unpack_kernel, blocks, each, per_half),
        out_shape=jax.ShapeDtypeStruct((blocks, 2 * half, each), jnp.float32),
        grid_spec=pltpu.PrefetchScalarGridSpec(
            num_scalar_prefetch=1,
            grid=(2 * per_half,),
            in_specs=[source, source],
            out_specs=pl.BlockSpec((blocks, tile, each), lambda step, _: (0, step, 0)),
        ),
        compiler_params=pltpu.CompilerParams(dimension_semantics=("arbitrary",)),
        name="unpack",
    )(home, mine, theirs)


def clip_kernel(kept, weight_ref, factor_ref, out_ref):
    for index, block in enumerate(kept):
        out_ref[:, index, :] = weight_ref[block].astype(jnp.float32) * factor_ref[index // 2]


def clip_weights(weight, factors):
    blocks, length, each = weight.shape
    kept = (0, 1, 3, 4)
    tile = min(128, length)
    return pl.pallas_call(
        partial(clip_kernel, kept),
        out_shape=jax.ShapeDtypeStruct((length, len(kept), each), jnp.float32),
        grid=(length // tile,),
        in_specs=[
            pl.BlockSpec((blocks, tile, each), lambda step: (0, step, 0)),
            pl.BlockSpec((2, 1, each), lambda step: (0, 0, 0)),
        ],
        out_specs=pl.BlockSpec((tile, len(kept), each), lambda step: (step, 0, 0)),
        compiler_params=pltpu.CompilerParams(dimension_semantics=("arbitrary",)),
        name="clip_weights",
    )(weight, factors)


def gated(value, *others):
    zero = 0.0
    for other in others:
        corner = lax.slice(other, (0,) * other.ndim, (1,) * other.ndim)
        zero = zero + corner.reshape(()).astype(jnp.float32) * 0.0
    return (value.astype(jnp.float32) + zero).astype(value.dtype)


def shards(tokens, cotangent, doc_ids, global_flags, w_attn, w_out, w_up, w_down, ln_gain, ln_bias):
    bf16, f32 = jnp.bfloat16, jnp.float32
    sections = lax.axis_size("section")
    slots = lax.axis_size("tensor")
    copies = lax.axis_size("dp")
    micro = tokens.shape[0]
    inner = slots // micro
    section = lax.axis_index("section")
    slot = lax.axis_index("tensor")
    row = slot // inner
    lane = slot % inner
    width = tokens.shape[3]
    chunk = tokens.shape[2]
    rows = min(QTILE, chunk)
    parts = chunk // rows
    plan = (inner, parts, rows)
    crossed = inner == 2
    joint = ("section", "tensor")
    groups = [[a * inner + b for b in range(inner)] for a in range(micro)]

    def device(s, a, b):
        return s * slots + a * inner + b

    def route(value, link):
        pairs = []
        for s in range(sections):
            for a in range(micro):
                for b in range(inner):
                    target = link(s, a, b)
                    if target is not None and target != (s, a, b):
                        pairs.append((device(s, a, b), device(*target)))
        return lax.ppermute(value, joint, pairs)

    def other_core(value):
        return lax.ppermute(value, "section", [(0, 1), (1, 0)])

    def other_row(value):
        return route(value, lambda s, a, b: (s, 1 - a, b))

    def other_lane(value):
        return route(value, lambda s, a, b: (s, a, 1 - b))

    class ByLane:
        home = section == row
        swap = staticmethod(other_lane)

        @staticmethod
        def keeper(s, a, b):
            return a

        @staticmethod
        def across(s, a, b):
            return (s, 1 - a, b)

    class ByRow:
        home = section == lane
        swap = staticmethod(other_row)

        @staticmethod
        def keeper(s, a, b):
            return b

        @staticmethod
        def across(s, a, b):
            return (s, a, 1 - b)

    split_attn = ByLane
    split_mlp = ByRow if crossed else ByLane

    def gather(own, split, hop=None):
        with jax.named_scope("gsec"):
            near = jnp.concatenate([own, other_core(own)], 0)
        if not crossed:
            if inner == 1:
                return [near]
            return [lax.all_gather(near, "tensor", axis=0, tiled=True, axis_index_groups=groups)]
        if hop is None:
            with jax.named_scope("ghop"):
                hop = split.swap(own)
        with jax.named_scope("gsec2"):
            return [near, jnp.concatenate([hop, other_core(hop)], 0)]

    def scatter_begin(partials, gates=()):
        if not crossed:
            blocks = partials[0].reshape(inner, 2, rows, -1)
            ours, theirs = blocks[:, 0], blocks[:, 1].astype(bf16)
            total = (ours + other_core(theirs).astype(f32)).reshape(inner * rows, -1)
            return total.astype(bf16), None
        near, far = partials
        with jax.named_scope("ssec"):
            leaving = far[:rows] + other_core(far[rows:].astype(bf16)).astype(f32)
            leaving = gated(leaving, *gates)
        with jax.named_scope("ssec2"):
            staying = near[:rows] + other_core(near[rows:].astype(bf16)).astype(f32)
        return leaving.astype(bf16), staying

    def scatter_end(begun, split):
        leaving, staying = begun
        if not crossed:
            if inner == 1:
                return leaving.astype(f32)
            return lax.psum_scatter(
                leaving, "tensor", scatter_dimension=0, tiled=True, axis_index_groups=groups
            ).astype(f32)
        with jax.named_scope("shop"):
            return staying + split.swap(leaving).astype(f32)

    def scatter_all(begun, split):
        sums = [scatter_end(item, split) for item in begun]
        if not crossed:
            return sums
        return [
            gated(item, begun[p + 1][0]) if p + 1 < len(sums) else item
            for p, item in enumerate(sums)
        ]

    def cut(array):
        per_part = 2 * inner * rows
        per_group = 2 * rows if crossed else per_part
        return [
            [array[p * per_part + g : p * per_part + g + per_group] for g in range(0, per_part, per_group)]
            for p in range(parts)
        ]

    def joined(pieces):
        return jnp.concatenate([piece for part in pieces for piece in part], 0)

    def flat(pieces):
        return [piece for part in pieces for piece in part]

    def part_rows(array):
        return [array[p * rows : (p + 1) * rows] for p in range(parts)]

    def own_rows(array):
        mine = lax.dynamic_index_in_dim(array[:, 0], row, 0, False)
        theirs = lax.dynamic_index_in_dim(array[:, 0], 1 - row, 0, False)
        moved = route(theirs, lambda s, a, b: (s, 1 - a, b) if s == a else None)
        return mine, moved

    def fetch(weight, layer, split):
        def across(s, a, b):
            if s != layer:
                return None
            _, a2, b2 = split.across(s, a, b)
            return (split.keeper(s, a, b), a2, b2)

        def within(s, a, b):
            return (split.keeper(s, a, b), a, b) if s == layer else None

        return route(weight, within), route(weight, across)

    def chosen(weight, arrived, layer, split):
        near, far = arrived
        return jnp.where(split.home, jnp.where(section == layer, weight, near), far)

    attn_table = w_attn[0].reshape(width, -1)
    mlp_pack = jnp.concatenate([w_up[0], w_down[0].reshape(width, -1)], 1)

    def attn_unpack(pack):
        columns = w_attn.shape[2] * w_attn.shape[3]
        return pack[:, :columns], pack[:, columns:].reshape(w_out.shape[1:])

    def mlp_unpack(pack):
        columns = w_up.shape[2]
        return pack[:, :columns], pack[:, columns:].reshape(w_down.shape[1:])

    mine, moved = own_rows(tokens)
    own = part_rows(jnp.where(ByLane.home, mine, moved))
    hops = []
    if crossed:
        early = route(mine, lambda s, a, b: (s, a, 1 - b) if s == a else None)
        late = route(moved, lambda s, a, b: (s, a, 1 - b) if s != a else None)
        hops = part_rows(jnp.where(ByLane.home, early, late))
    attn_weights = [None] * sections
    mlp_weights = [None] * sections
    attn_pack = jnp.concatenate([attn_table, w_out[0].reshape(width, -1)], 1)
    with jax.named_scope("W0attn"):
        first_pack = chosen(attn_pack, fetch(attn_pack, 0, split_attn), 0, split_attn)
    with jax.named_scope("W0mlp"):
        arriving = fetch(after(mlp_pack, *own, *hops), 0, split_mlp)

    heads = w_attn.shape[3] // HEAD
    docs = lax.dynamic_index_in_dim(doc_ids[:, 0], row, 0, False)
    flags = lax.dynamic_index_in_dim(global_flags[:, 0], row, 0, False)
    order = jnp.stack([section, lane if crossed else jnp.zeros_like(lane)]).astype(jnp.int32)
    info = sequence_info(docs, flags, order, heads)
    first_pack, mlp_pack, *info = lax.optimization_barrier((first_pack, mlp_pack, *info))
    attn_weights[0] = attn_unpack(first_pack)

    gains_own = jnp.stack([ln_gain[0], ln_bias[0]])
    gains_other = other_core(gains_own)
    norms = [jnp.where(section == layer, gains_own, gains_other) for layer in range(sections)]

    saved, outputs, peaks = [], [], []
    for layer in range(sections):
        gains, shifts = norms[layer]
        attn_w, out_w = attn_weights[layer]
        with jax.named_scope(f"F{layer}in"):
            inputs = [
                gather(own[p], split_attn, hops[p] if layer == 0 and crossed else None)
                for p in range(parts)
            ]
            proj = [[mm(piece, attn_w, NN, bf16) for piece in part] for part in inputs]
        context, lse, glse, *tops = attend(flat(proj), info, plan)
        peaks.append(tops)
        if layer == 0:
            with jax.named_scope("W1attn"):
                pack = fetch(after(attn_pack, *flat(proj)), 1, split_attn)
            context, arriving, pack = lax.optimization_barrier((context, arriving, pack))
            mlp_weights[0] = mlp_unpack(chosen(mlp_pack, arriving, 0, split_mlp))
            attn_weights[1] = attn_unpack(chosen(attn_pack, pack, 1, split_attn))
        else:
            with jax.named_scope("W1mlp"):
                pack = fetch(after(mlp_pack, *flat(proj)), 1, split_mlp)
            with jax.named_scope("COT"):
                mine, moved = own_rows(after(cotangent, *flat(proj)))
            context, pack, mine, moved = lax.optimization_barrier((context, pack, mine, moved))
            mlp_weights[1] = mlp_unpack(chosen(mlp_pack, pack, 1, split_mlp))
            grad_out = part_rows(jnp.where(ByLane.home, mine, moved).astype(f32))
        up_w, down_w = mlp_weights[layer]
        with jax.named_scope(f"F{layer}out"):
            sums = scatter_all(
                [scatter_begin([mm(piece, out_w) for piece in part]) for part in cut(context)],
                split_attn,
            )
        hidden, hidden_low, norms_one = [], [], []
        for p in range(parts):
            with jax.named_scope(f"F{layer}norm1"):
                value = gated(sums[p], hidden_low[-1]) if p else sums[p]
                value, normed, scale = norm_forward(own[p].astype(f32) + value, gains[0], shifts[0])
                hidden.append(value)
                hidden_low.append(value.astype(bf16))
                norms_one.append((normed, scale))
        hidden_rows, acts, slopes, begun = [], [], [], []
        for p in range(parts):
            with jax.named_scope(f"F{layer}mlp{p}"):
                hidden_rows.append(gather(hidden_low[p], split_mlp))
                pairs = [gelu_pair(mm(piece, up_w)) for piece in hidden_rows[p]]
                acts.append([act for act, _ in pairs])
                slopes.append([slope for _, slope in pairs])
                begun.append(
                    scatter_begin([mm(act, down_w) for act in acts[p]], hidden_low[p + 1 : p + 2])
                )
        with jax.named_scope(f"F{layer}mlp"):
            sums = scatter_all(begun, split_mlp)
        outs, norms_two = [], []
        for p in range(parts):
            with jax.named_scope(f"F{layer}norm2"):
                value = gated(sums[p], outs[-1]) if p else sums[p]
                value, normed, scale = norm_forward(hidden[p] + value, gains[1], shifts[1])
                norms_two.append((normed, scale))
                outs.append(value.astype(bf16))
        own = outs
        outputs.append(jnp.concatenate(outs, 0))
        saved.append(
            (inputs, proj, context, (lse, glse), norms_one, hidden_rows, acts, slopes, norms_two)
        )

    def to_owner(upper, lower, split, gates=()):
        def first_link(s, a, b):
            if s == split.keeper(s, a, b):
                return (1 - s, a, b)
            return split.across(s, a, b)

        def second_link(s, a, b):
            if s == split.keeper(s, a, b):
                return None
            _, a2, b2 = split.across(s, a, b)
            return (1 - s, a2, b2)

        first = route(gated(jnp.where(split.home, lower, upper), *gates), first_link)
        second = route(lower, second_link)
        part = first.astype(f32) + jnp.where(split.home, upper, second).astype(f32)
        return part.astype(bf16)

    earlier = ()

    def dp_sum(*terms):
        nonlocal earlier
        terms = [after(term, *earlier) for term in terms]
        earlier = lax.psum(tuple(terms), "dp")
        return earlier

    def pick(values):
        return jnp.where(section == 0, values[0], values[1])

    def placed(chunk, layer):
        arrived = []
        for index in range(micro):
            moved = route(chunk, lambda s, a, b: (layer, s, b) if a == index else None)
            stays = (section == layer) & ByLane.home & (row == index)
            arrived.append(jnp.where(stays, chunk, moved))
        return arrived

    def send_attn(pack, gates):
        half = width // 2
        return to_owner(pack[:half], pack[half:], split_attn, gates)

    attn_sums = [None] * sections
    mlp_sums = [None] * sections
    norm_sums = [None] * sections
    out_rows = [None] * sections
    grad_rows = [None] * sections
    for layer in reversed(range(sections)):
        (attn_w, out_w), (up_w, down_w) = attn_weights[layer], mlp_weights[layer]
        gains, _ = norms[layer]
        inputs, proj, context, log_sums, norms_one, hidden_rows, acts, slopes, norms_two = saved[layer]
        grads_two, low, sums_two = [], [], []
        for p in range(parts):
            with jax.named_scope(f"B{layer}norm2"):
                value = gated(grad_out[p], low[-1]) if p else grad_out[p]
                value, sums = norm_backward(value, *norms_two[p], gains[1])
                grads_two.append(value)
                low.append(value.astype(bf16))
                sums_two.append(sums)
        grad_mlp, grad_up, begun = [], [], []
        for p in range(parts):
            with jax.named_scope(f"B{layer}mlp{p}"):
                grad_mlp.append(gather(low[p], split_mlp))
                grad_up.append(
                    [
                        (mm(piece, down_w, NT) * slope.astype(f32)).astype(bf16)
                        for piece, slope in zip(grad_mlp[p], slopes[p])
                    ]
                )
                begun.append(
                    scatter_begin([mm(piece, up_w, NT) for piece in grad_up[p]], low[p + 1 : p + 2])
                )
        with jax.named_scope(f"B{layer}mlp"):
            sums = scatter_all(begun, split_mlp)
        with jax.named_scope(f"B{layer}wmlp"):
            grad_up_w = mm(joined(hidden_rows), joined(grad_up), TN, bf16)
            grad_down_w = mm(joined(acts), joined(grad_mlp), TN, bf16)
            sums[-1] = gated(sums[-1], grad_up_w, grad_down_w)
        grads_one, low, sums_one = [], [], []
        for p in range(parts):
            with jax.named_scope(f"B{layer}norm1"):
                value = gated(sums[p], low[-1]) if p else sums[p]
                value, total = norm_backward(value + grads_two[p], *norms_one[p], gains[0])
                grads_one.append(value)
                low.append(value.astype(bf16))
                sums_one.append(total)
        norm_sums[layer] = (sums_one, sums_two)
        grad_attn, grad_context = [], []
        for p in range(parts):
            with jax.named_scope(f"B{layer}ctx{p}"):
                grad_attn.append(gather(low[p], split_attn))
                grad_context.append([mm(piece, out_w, NT, bf16) for piece in grad_attn[p]])
        with jax.named_scope(f"B{layer}wmlp"):
            mlp_parts = to_owner(
                grad_up_w.reshape(width, -1), grad_down_w.reshape(width, -1), split_mlp,
                flat(grad_context) if layer else low,
            )
        if layer == 0:
            *grad_context[-1], mlp_sums[1] = lax.optimization_barrier(
                (*grad_context[-1], mlp_sums[1])
            )
        grad_context = flat(grad_context)
        if layer == 0:
            with jax.named_scope("B1wattn"):
                attn_parts = send_attn(pack, grad_context)
            *grad_context, mlp_parts = lax.optimization_barrier((*grad_context, mlp_parts))
            mlp_sums[0] = dp_sum(mlp_parts)[0]
        grad_proj = attend_back(flat(proj), context, log_sums, grad_context, info, plan)
        if layer == 1:
            with jax.named_scope("OUTROWS"):
                ready = lax.optimization_barrier((*outputs, *grad_context))[:sections]
                for index in range(sections):
                    out_rows[index] = placed(ready[index], index)
        if layer == 1:
            grad_proj, mlp_parts = lax.optimization_barrier((grad_proj, mlp_parts))
            mlp_sums[1] = dp_sum(mlp_parts)[0]
        else:
            grad_proj, attn_parts = lax.optimization_barrier((grad_proj, attn_parts))
        with jax.named_scope(f"B{layer}wattn"):
            grad_attn_w = mm(joined(inputs), grad_proj, TN, bf16)
            grad_out_w = mm(context, joined(grad_attn), TN, bf16)
            pack = jnp.concatenate([grad_attn_w, grad_out_w.reshape(width, -1)], 1)
        if layer == 0:
            grad_proj = after(grad_proj, pack)
        grad_low = []
        grad_proj_parts = cut(grad_proj)
        if layer == 0:
            *grad_proj_parts[-1], mlp_sums[0] = lax.optimization_barrier(
                (*grad_proj_parts[-1], mlp_sums[0])
            )
        with jax.named_scope(f"B{layer}in"):
            sums = scatter_all(
                [
                    scatter_begin(
                        [mm(piece, attn_w, NT) for piece in part],
                        (),
                    )
                    for part in grad_proj_parts
                ],
                split_attn,
            )
        for p in range(parts):
            with jax.named_scope(f"B{layer}in"):
                value = gated(sums[p], grad_low[-1]) if p else sums[p]
                grad_low.append((value + grads_one[p]).astype(bf16))
        grad_out = [piece.astype(f32) for piece in grad_low]
        if layer == 0:
            with jax.named_scope("B0wattn"):
                last_parts = send_attn(pack, ())
                attn_sums[1], attn_sums[0] = dp_sum(attn_parts, last_parts)
        with jax.named_scope("GRADROWS"):
            grad_rows[layer] = placed(jnp.concatenate(grad_low, 0), layer)

    def stacked_rows(by_layer):
        return jnp.stack([pick([by_layer[0][m], by_layer[1][m]]) for m in range(micro)])[None, :, None]

    def placed_weight(terms, split):
        mine = pick(terms)
        theirs = other_core(pick(terms[::-1]))
        first = jnp.where(split.home, mine, theirs)
        second = jnp.where(split.home, theirs, mine)
        return first.astype(f32), second.astype(f32)

    def dp_butterfly(value, combine):
        if copies & (copies - 1):
            gathered = lax.all_gather(value, "dp", axis=0)
            total = gathered[0]
            for index in range(1, copies):
                total = combine(total, gathered[index])
            return total
        distance = 1
        while distance < copies:
            pairs = [(d, d ^ distance) for d in range(copies)]
            value = combine(value, lax.ppermute(value, "dp", pairs))
            distance *= 2
        return value

    with jax.named_scope("NORMSUM"):
        mine = [
            jnp.stack([sum(sums_one[1:], sums_one[0]), sum(sums_two[1:], sums_two[0])])
            for sums_one, sums_two in norm_sums
        ]
        mine = lax.optimization_barrier((*mine, last_parts))[:sections]
        norm_sum = pick(mine) + other_core(pick(mine[::-1]))
        if crossed:
            norm_sum = norm_sum + other_row(norm_sum)
            norm_sum = norm_sum + other_lane(norm_sum)
        else:
            norm_sum = lax.psum(norm_sum, "tensor")
        norm_sum = dp_butterfly(norm_sum, jnp.add)
    with jax.named_scope("PEAK"):
        peak_all = lax.optimization_barrier((*flat(peaks), last_parts))[:-1]
        peak_all = jnp.stack(
            [jnp.max(value.reshape(heads, -1), 1) for value in peak_all]
        ).reshape(sections, 2, heads)
        peak_all = jnp.maximum(peak_all, other_row(peak_all))
        peak_all = dp_butterfly(peak_all, jnp.maximum)
        peak_here = jnp.where(ByLane.home, pick(peak_all), other_core(pick(peak_all[::-1])))
    factors = jnp.sqrt(clip_limit / jnp.maximum(peak_here, clip_limit))
    columns = jnp.repeat(factors, HEAD, axis=1)
    clipped = clip_weights(w_attn[0].transpose(1, 0, 2), columns[:, None, :])
    out_rows, grad_rows = stacked_rows(out_rows), stacked_rows(grad_rows)
    grad_up_w, grad_down_w = placed_weight(mlp_sums, split_mlp)
    attn_sums = [
        gated(term, out_rows, grad_rows, grad_up_w, grad_down_w, norm_sum, clipped)
        for term in attn_sums
    ]
    mine, theirs = pick(attn_sums), other_core(pick(attn_sums[::-1]))
    blocks, each = w_attn.shape[2:]
    home = split_attn.home.astype(jnp.int32).reshape(1)
    grad_attn_w = unpack(home, mine, theirs, blocks, each).transpose(1, 0, 2)
    halves = [half[:, blocks * each :].reshape(-1, w_out.shape[2]) for half in (mine, theirs)]
    grad_out_w = jnp.where(
        split_attn.home, jnp.concatenate(halves, 0), jnp.concatenate(halves[::-1], 0)
    ).astype(f32)

    return (
        out_rows,
        grad_rows,
        grad_attn_w[None],
        grad_out_w.reshape(w_out.shape),
        grad_up_w.reshape(w_up.shape),
        grad_down_w.reshape(w_down.shape),
        norm_sum[:, 0][None],
        norm_sum[:, 1][None],
        clipped[None],
    )


def solution(mesh):
    in_specs = (
        P(None, "dp", "tensor", None),
        P(None, "dp", "tensor", None),
        P(None, "dp", None),
        P(None, "dp", None),
        P("section", None, None, "tensor"),
        P("section", "tensor", None),
        P("section", None, "tensor"),
        P("section", "tensor", None),
        P("section", None, None),
        P("section", None, None),
    )
    out_specs = (
        P("section", None, "dp", "tensor", None),
        P("section", None, "dp", "tensor", None),
        P("section", None, None, "tensor"),
        P("section", "tensor", None),
        P("section", None, "tensor"),
        P("section", "tensor", None),
        P("section", None, None),
        P("section", None, None),
        P("section", None, None, "tensor"),
    )
    return jax.shard_map(shards, mesh=mesh, in_specs=in_specs, out_specs=out_specs, check_vma=False)
```

```python
import math
from functools import partial

import jax
import jax.numpy as jnp
from jax import lax
from jax.experimental import pallas as pl
from jax.experimental.pallas import tpu as pltpu
from jax.sharding import PartitionSpec as P

HEAD = 64
HALF = 512
QTILE = 256
KTILE = 512
VMEM_BYTES = 56 * 1024 * 1024

masked_fill = -1e30
clip_limit = 10.0
score_scale = HEAD ** (-0.5)

NN = (((1,), (0,)), ((), ()))
NT = (((1,), (1,)), ((), ()))
TN = (((0,), (0,)), ((), ()))


def mm(left, right, dims=NN, out=jnp.float32):
    return lax.dot_general(left, right, dims, preferred_element_type=jnp.float32).astype(out)


def tile_bias(first_key, first_query, key_docs, query_docs, keys, queries):
    key_pos = first_key + lax.broadcasted_iota(jnp.int32, (keys, queries), 0)
    query_pos = first_query + lax.broadcasted_iota(jnp.int32, (keys, queries), 1)
    gap = jnp.abs(key_pos - query_pos)
    return jnp.where((key_docs == query_docs) & (gap <= HALF), 0.0, masked_fill)


def far_bias(glob_pos, first_query, glob_docs, query_docs, globs, queries):
    query_pos = first_query + lax.broadcasted_iota(jnp.int32, (globs, queries), 1)
    gap = jnp.abs(glob_pos - query_pos)
    return jnp.where((glob_docs == query_docs) & (gap > HALF), 0.0, masked_fill)


def one_hot_rows(glob_pos, length):
    globs = glob_pos.shape[0]
    hit = lax.broadcasted_iota(jnp.int32, (globs, length), 1) == glob_pos
    return jnp.where(hit, 1.0, 0.0).astype(jnp.bfloat16)


def true_unit(place, order_ref, plan):
    inner, parts, _ = plan
    part, rest = place // (2 * inner), place % (2 * inner)
    side = (rest % 2) ^ order_ref[0]
    lane = (rest // 2) ^ order_ref[1]
    return (side * inner + lane) * parts + part


def local_unit(unit, order_ref, plan):
    inner, parts, _ = plan
    block, part = lax.div(unit, parts), lax.rem(unit, parts)
    side = lax.div(block, inner) ^ order_ref[0]
    lane = lax.rem(block, inner) ^ order_ref[1]
    return part * (2 * inner) + lane * 2 + side


def join_pieces(order_ref, pieces, joined_ref, sems, plan):
    rows = plan[2]
    copies = []
    place = 0
    for piece in pieces:
        for index in range(piece.shape[0] // rows):
            start = pl.multiple_of(true_unit(place, order_ref, plan) * rows, rows)
            copies.append(
                pltpu.make_async_copy(
                    piece.at[pl.ds(index * rows, rows), :],
                    joined_ref.at[pl.ds(start, rows), :],
                    sems.at[place],
                )
            )
            place += 1
    for copy in copies:
        copy.start()
    for copy in copies:
        copy.wait()


def store_local(out_ref, tile, cols, value, order_ref, plan):
    rows = plan[2]
    size = min(rows, value.shape[0])
    for index in range(value.shape[0] // size):
        row = tile * value.shape[0] + index * size
        place = local_unit(lax.div(row, rows), order_ref, plan)
        start = pl.multiple_of(place * rows + lax.rem(row, rows), size)
        out_ref[pl.ds(start, size), cols] = value[index * size : (index + 1) * size]


def diagonal_sum(blocks, heads, rows):
    owner = lax.broadcasted_iota(jnp.int32, (rows, heads * HEAD), 1) // HEAD
    total = jnp.zeros((rows, heads * HEAD), jnp.float32)
    for head in range(heads):
        total = total + jnp.where(owner == head, blocks[head * rows : (head + 1) * rows], 0.0)
    return total


def attend_kernel(
    heads,
    plan,
    count,
    order_ref,
    first_ref,
    last_ref,
    *refs,
):
    pieces, refs = refs[:count], refs[count:]
    attend_body(heads, plan, order_ref, first_ref, last_ref, pieces, *refs)


def attend_body(
    heads,
    plan,
    order_ref,
    first_ref,
    last_ref,
    pieces,
    doc_row_ref,
    doc_col_ref,
    pos_col_ref,
    gdoc_col_ref,
    gdoc_row_ref,
    ctx_ref,
    lse_ref,
    glse_ref,
    peak_ref,
    gpeak_ref,
    proj,
    values_t,
    hot,
    far_keys,
    far_values_t,
    gctx_t,
    gstack,
    gscores,
    wide,
    acc,
    top,
    total,
    sems,
):
    length = proj.shape[0]
    width = heads * HEAD
    globs = pos_col_ref.shape[0]
    step = pl.program_id(0)

    @pl.when(step == 0)
    def _():
        join_pieces(order_ref, pieces, proj, sems, plan)
        wide[...] = jnp.zeros_like(wide)
        gstack[...] = jnp.zeros_like(gstack)
        hot[...] = one_hot_rows(pos_col_ref[...], length)
        hot_all = hot[...]
        far_keys[...] = mm(hot_all, proj[:, width : 2 * width], out=jnp.bfloat16)
        far_values_t[...] = mm(hot_all, proj[:, 2 * width : 3 * width]).T.astype(jnp.bfloat16)
        queries = (mm(hot_all, proj[:, 3 * width : 4 * width]) * score_scale).astype(jnp.bfloat16)
        for head in range(heads):
            cols = slice(head * HEAD, (head + 1) * HEAD)
            gstack[head * globs : (head + 1) * globs, cols] = queries[:, cols]

        def score_tile(tile, best):
            rows = pl.ds(pl.multiple_of(tile * KTILE, KTILE), KTILE)
            values_t[:, rows] = proj[rows, 2 * width : 3 * width].T
            scores = mm(proj[rows, 4 * width : 5 * width], gstack[...], NT)
            scores = jnp.where(doc_col_ref[rows, :] == gdoc_row_ref[...], scores, masked_fill)
            gscores[rows, :] = scores
            return jnp.maximum(best, jnp.max(scores, 0, keepdims=True))

        best = lax.fori_loop(
            0, length // KTILE, score_tile, jnp.full((1, heads * globs), masked_fill, jnp.float32)
        )

        def sum_tile(tile, sums):
            rows = pl.ds(pl.multiple_of(tile * KTILE, KTILE), KTILE)
            weights = jnp.exp(gscores[rows, :] - best)
            gscores[rows, :] = weights
            return sums + jnp.sum(weights, 0, keepdims=True)

        sums = lax.fori_loop(
            0, length // KTILE, sum_tile, jnp.zeros((1, heads * globs), jnp.float32)
        )

        def value_tile(tile, blocks):
            rows = pl.ds(pl.multiple_of(tile * KTILE, KTILE), KTILE)
            probs = (gscores[rows, :] / sums).T.astype(jnp.bfloat16)
            return blocks + mm(probs, proj[rows, 5 * width : 6 * width])

        blocks = lax.fori_loop(
            0, length // KTILE, value_tile, jnp.zeros((heads * globs, width), jnp.float32)
        )
        gctx_t[...] = diagonal_sum(blocks, heads, globs).T.astype(jnp.bfloat16)
        glse_ref[...] = best + jnp.log(sums)
        gpeak_ref[...] = best

    start = pl.multiple_of(step * QTILE, QTILE)
    query_rows = pl.ds(start, QTILE)
    query_t = proj[query_rows, 0:width].T * score_scale
    for head in range(heads):
        rows = slice(head * HEAD, (head + 1) * HEAD)
        wide[rows, head * QTILE : (head + 1) * QTILE] = query_t[rows].astype(jnp.bfloat16)
    query_docs = doc_row_ref[:, query_rows]

    scores = mm(far_keys[...], wide[...])
    bias = far_bias(pos_col_ref[...], start, gdoc_col_ref[...], query_docs, globs, QTILE)
    for head in range(heads):
        cols = slice(head * QTILE, (head + 1) * QTILE)
        rows = slice(head * HEAD, (head + 1) * HEAD)
        part = scores[:, cols] + bias
        best = jnp.max(part, 0, keepdims=True)
        weights = jnp.exp(part - best)
        top[:, cols] = best
        total[:, cols] = jnp.sum(weights, 0, keepdims=True)
        acc[rows, :] = mm(far_values_t[rows, :], weights.astype(jnp.bfloat16))

    def key_tile(tile, carry):
        key_start = pl.multiple_of(tile * KTILE, KTILE)
        keys = pl.ds(key_start, KTILE)
        scores = mm(proj[keys, width : 2 * width], wide[...])
        bias = tile_bias(key_start, start, doc_col_ref[keys, :], query_docs, KTILE, QTILE)
        for head in range(heads):
            cols = slice(head * QTILE, (head + 1) * QTILE)
            rows = slice(head * HEAD, (head + 1) * HEAD)
            part = scores[:, cols] + bias
            old = top[:, cols]
            best = jnp.maximum(old, jnp.max(part, 0, keepdims=True))
            weights = jnp.exp(part - best)
            shrink = jnp.exp(old - best)
            top[:, cols] = best
            total[:, cols] = total[:, cols] * shrink + jnp.sum(weights, 0, keepdims=True)
            acc[rows, :] = acc[rows, :] * shrink + mm(
                values_t[rows, keys], weights.astype(jnp.bfloat16)
            )
        return carry

    lax.fori_loop(first_ref[step], last_ref[step], key_tile, 0)

    hot_tile = hot[:, query_rows]
    is_glob = jnp.max(hot_tile.astype(jnp.float32), 0, keepdims=True) > 0.5
    for head in range(heads):
        cols = slice(head * QTILE, (head + 1) * QTILE)
        rows = slice(head * HEAD, (head + 1) * HEAD)
        acc[rows, :] = acc[rows, :] / total[:, cols]
        lse_ref[head : head + 1, :] = top[:, cols] + jnp.log(total[:, cols])
    merged = jnp.where(is_glob, mm(gctx_t[...], hot_tile), acc[...])
    store_local(ctx_ref, step, slice(None), merged.T.astype(jnp.bfloat16), order_ref, plan)

    @pl.when(step == 0)
    def _():
        peak_ref[...] = top[...]

    @pl.when(step > 0)
    def _():
        peak_ref[...] = jnp.maximum(peak_ref[...], top[...])


def whole_block(shape):
    return pl.BlockSpec(shape, lambda *_: (0,) * len(shape), pipeline_mode=pl.Buffered(1))


def attend(proj, info, plan):
    length = sum(piece.shape[0] for piece in proj)
    columns = proj[0].shape[1]
    heads = columns // (6 * HEAD)
    width = heads * HEAD
    order, first, last, doc_row, doc_col, pos_col, gdoc_col, gdoc_row, _ = info
    globs = pos_col.shape[0]
    tiles = length // QTILE
    bf16, f32 = jnp.bfloat16, jnp.float32

    anywhere = pl.BlockSpec(memory_space=pl.ANY)
    return pl.pallas_call(
        partial(attend_kernel, heads, plan, len(proj)),
        out_shape=(
            jax.ShapeDtypeStruct((length, width), bf16),
            jax.ShapeDtypeStruct((heads, length), f32),
            jax.ShapeDtypeStruct((1, heads * globs), f32),
            jax.ShapeDtypeStruct((1, heads * QTILE), f32),
            jax.ShapeDtypeStruct((1, heads * globs), f32),
        ),
        grid_spec=pltpu.PrefetchScalarGridSpec(
            num_scalar_prefetch=3,
            grid=(tiles,),
            in_specs=[anywhere] * len(proj) + [
                whole_block((1, length)),
                whole_block((length, 1)),
                whole_block((globs, 1)),
                whole_block((globs, 1)),
                whole_block((1, heads * globs)),
            ],
            out_specs=(
                whole_block((length, width)),
                pl.BlockSpec((heads, QTILE), lambda step, *_: (0, step)),
                pl.BlockSpec((1, heads * globs), lambda *_: (0, 0)),
                pl.BlockSpec((1, heads * QTILE), lambda *_: (0, 0)),
                pl.BlockSpec((1, heads * globs), lambda *_: (0, 0)),
            ),
            scratch_shapes=[
                pltpu.VMEM((length, columns), bf16),
                pltpu.VMEM((width, length), bf16),
                pltpu.VMEM((globs, length), bf16),
                pltpu.VMEM((globs, width), bf16),
                pltpu.VMEM((width, globs), bf16),
                pltpu.VMEM((width, globs), bf16),
                pltpu.VMEM((heads * globs, width), bf16),
                pltpu.VMEM((length, heads * globs), f32),
                pltpu.VMEM((width, heads * QTILE), bf16),
                pltpu.VMEM((width, QTILE), f32),
                pltpu.VMEM((1, heads * QTILE), f32),
                pltpu.VMEM((1, heads * QTILE), f32),
                pltpu.SemaphoreType.DMA((length // plan[2],)),
            ],
        ),
        compiler_params=pltpu.CompilerParams(
            dimension_semantics=("arbitrary",), vmem_limit_bytes=VMEM_BYTES
        ),
        cost_estimate=pl.CostEstimate(
            flops=20 * length * 1024 * width, bytes_accessed=14 * length * width,
            transcendentals=length * 1024 * heads,
        ),
        name="attend",
    )(order, first, last, *proj, doc_row, doc_col, pos_col, gdoc_col, gdoc_row)


def attend_back_kernel(
    heads,
    plan,
    counts,
    order_ref,
    first_ref,
    last_ref,
    *refs,
):
    pieces, refs = refs[: counts[0]], refs[counts[0] :]
    grad_pieces, refs = refs[: counts[1]], refs[counts[1] :]
    attend_back_body(heads, plan, order_ref, first_ref, last_ref, pieces, grad_pieces, *refs)


def attend_back_body(
    heads,
    plan,
    order_ref,
    first_ref,
    last_ref,
    pieces,
    grad_pieces,
    ctx_piece_ref,
    lse_ref,
    glse_ref,
    doc_row_ref,
    doc_col_ref,
    pos_col_ref,
    gdoc_col_ref,
    gdoc_row_ref,
    plain_col_ref,
    out_ref,
    proj,
    ctx,
    grad,
    keys_t,
    hot,
    far_keys,
    far_keys_t,
    far_values,
    far_key_grad,
    far_value_grad,
    key_grad,
    value_grad,
    gquery,
    gout,
    gquery_grad,
    wide,
    wide_grad,
    stack,
    stack_grad,
    probs_low,
    grads_low,
    query_grad_t,
    proj_sems,
    ctx_sems,
    grad_sems,
):
    length = proj.shape[0]
    width = heads * HEAD
    globs = pos_col_ref.shape[0]
    tiles = length // KTILE
    step = pl.program_id(0)
    bf16 = jnp.bfloat16

    def store(tile, block, value):
        cols = slice(block * width, (block + 1) * width)
        store_local(out_ref, tile, cols, value.astype(bf16), order_ref, plan)

    @pl.when(step == 0)
    def _():
        join_pieces(order_ref, pieces, proj, proj_sems, plan)
        join_pieces(order_ref, [ctx_piece_ref], ctx, ctx_sems, plan)
        join_pieces(order_ref, grad_pieces, grad, grad_sems, plan)
        for ref in (wide, wide_grad, stack, stack_grad, gquery, gout):
            ref[...] = jnp.zeros_like(ref)
        for ref in (key_grad, value_grad, far_key_grad, far_value_grad):
            ref[...] = jnp.zeros_like(ref)
        gquery_grad[...] = jnp.zeros_like(gquery_grad)
        hot[...] = one_hot_rows(pos_col_ref[...], length)
        hot_all = hot[...]
        near = mm(hot_all, proj[:, width : 2 * width])
        far_keys[...] = near.astype(bf16)
        far_keys_t[...] = near.T.astype(bf16)
        far_values[...] = mm(hot_all, proj[:, 2 * width : 3 * width], out=bf16)
        queries = (mm(hot_all, proj[:, 3 * width : 4 * width]) * score_scale).astype(bf16)
        out_grad = mm(hot_all, grad[...])
        glob_ctx = mm(hot_all, ctx[...])
        product = out_grad * glob_ctx
        owner = lax.broadcasted_iota(jnp.int32, (globs, width), 1) // HEAD
        dots = []
        for head in range(heads):
            cols = slice(head * HEAD, (head + 1) * HEAD)
            rows = slice(head * globs, (head + 1) * globs)
            gquery[rows, cols] = queries[:, cols]
            gout[rows, cols] = out_grad[:, cols].astype(bf16)
            own = jnp.where(owner == head, product, 0.0)
            dots.append(jnp.sum(own, 1, keepdims=True))
        dot_row = jnp.broadcast_to(jnp.concatenate(dots, 0), (heads * globs, 128)).T[0:1]

        def glob_tile(tile, carry):
            rows = pl.ds(pl.multiple_of(tile * KTILE, KTILE), KTILE)
            keys_t[:, rows] = proj[rows, width : 2 * width].T
            scores = mm(proj[rows, 4 * width : 5 * width], gquery[...], NT)
            scores = jnp.where(doc_col_ref[rows, :] == gdoc_row_ref[...], scores, masked_fill)
            probs = jnp.exp(scores - glse_ref[...])
            grad_p = mm(proj[rows, 5 * width : 6 * width], gout[...], NT)
            grad_s = probs * (grad_p - dot_row)
            store(tile, 5, mm(probs.astype(bf16), gout[...]))
            store(tile, 4, mm(grad_s.astype(bf16), gquery[...]))
            gquery_grad[...] += mm(grad_s.T.astype(bf16), proj[rows, 4 * width : 5 * width])
            return carry

        lax.fori_loop(0, tiles, glob_tile, 0)
        query_grad = diagonal_sum(gquery_grad[...], heads, globs) * score_scale
        query_grad = query_grad.astype(bf16)

        def spread_tile(tile, carry):
            rows = pl.ds(pl.multiple_of(tile * KTILE, KTILE), KTILE)
            store(tile, 3, mm(hot[:, rows], query_grad, TN))
            return carry

        lax.fori_loop(0, tiles, spread_tile, 0)

    start = pl.multiple_of(step * QTILE, QTILE)
    query_rows = pl.ds(start, QTILE)
    query = proj[query_rows, 0:width].astype(jnp.float32) * score_scale
    query_t = query.T.astype(bf16)
    query = query.astype(bf16)
    grad_out = grad[query_rows, :].astype(jnp.float32) * plain_col_ref[query_rows, :]
    grad_out_t = grad_out.T
    product_t = grad_out_t * ctx[query_rows, :].astype(jnp.float32).T
    grad_out = grad_out.astype(bf16)
    grad_out_t = grad_out_t.astype(bf16)
    dots = []
    for head in range(heads):
        own = slice(head * HEAD, (head + 1) * HEAD)
        cols = slice(head * QTILE, (head + 1) * QTILE)
        wide[own, cols] = query_t[own]
        wide_grad[own, cols] = grad_out_t[own]
        stack[cols, own] = query[:, own]
        stack_grad[cols, own] = grad_out[:, own]
        dots.append(jnp.sum(product_t[own], 0, keepdims=True))
    query_docs = doc_row_ref[:, query_rows]

    def parts(scores, grad_p, bias, head):
        cols = slice(head * QTILE, (head + 1) * QTILE)
        shift = lse_ref[head : head + 1, query_rows]
        probs = jnp.exp(scores[:, cols] + bias - shift)
        grad_s = probs * (grad_p[:, cols] - dots[head])
        return probs.astype(bf16), grad_s.astype(bf16)

    scores = mm(far_keys[...], wide[...])
    grad_p = mm(far_values[...], wide_grad[...])
    bias = far_bias(pos_col_ref[...], start, gdoc_col_ref[...], query_docs, globs, QTILE)
    for head in range(heads):
        cols = slice(head * QTILE, (head + 1) * QTILE)
        own = slice(head * HEAD, (head + 1) * HEAD)
        probs, grad_s = parts(scores, grad_p, bias, head)
        probs_low[0:globs, cols] = probs
        grads_low[0:globs, cols] = grad_s
        query_grad_t[own, :] = mm(far_keys_t[own, :], grad_s)
    far_value_grad[...] += mm(probs_low[0:globs, :], stack_grad[...])
    far_key_grad[...] += mm(grads_low[0:globs, :], stack[...])

    def key_tile(tile, carry):
        key_start = pl.multiple_of(tile * KTILE, KTILE)
        keys = pl.ds(key_start, KTILE)
        scores = mm(proj[keys, width : 2 * width], wide[...])
        grad_p = mm(proj[keys, 2 * width : 3 * width], wide_grad[...])
        bias = tile_bias(key_start, start, doc_col_ref[keys, :], query_docs, KTILE, QTILE)
        for head in range(heads):
            cols = slice(head * QTILE, (head + 1) * QTILE)
            own = slice(head * HEAD, (head + 1) * HEAD)
            probs, grad_s = parts(scores, grad_p, bias, head)
            probs_low[:, cols] = probs
            grads_low[:, cols] = grad_s
            query_grad_t[own, :] += mm(keys_t[own, keys], grad_s)
        value_grad[keys, :] += mm(probs_low[...], stack_grad[...])
        key_grad[keys, :] += mm(grads_low[...], stack[...])
        return carry

    lax.fori_loop(first_ref[step], last_ref[step], key_tile, 0)
    store(step, 0, (query_grad_t[...] * score_scale).T)

    @pl.when(step == pl.num_programs(0) - 1)
    def _():
        far_key = far_key_grad[...].astype(bf16)
        far_value = far_value_grad[...].astype(bf16)

        def close_tile(tile, carry):
            rows = pl.ds(pl.multiple_of(tile * KTILE, KTILE), KTILE)
            hot_tile = hot[:, rows]
            key_sum = key_grad[rows, :] + mm(hot_tile, far_key, TN)
            value_sum = value_grad[rows, :] + mm(hot_tile, far_value, TN)
            store(tile, 1, key_sum)
            store(tile, 2, value_sum)
            return carry

        lax.fori_loop(0, tiles, close_tile, 0)


def attend_back(proj, context, log_sums, grad_context, info, plan):
    length = context.shape[0]
    columns = proj[0].shape[1]
    heads = columns // (6 * HEAD)
    width = heads * HEAD
    order, first, last, doc_row, doc_col, pos_col, gdoc_col, gdoc_row, plain_col = info
    globs = pos_col.shape[0]
    tiles = length // QTILE
    bf16, f32 = jnp.bfloat16, jnp.float32
    wide = heads * QTILE
    anywhere = pl.BlockSpec(memory_space=pl.ANY)
    return pl.pallas_call(
        partial(attend_back_kernel, heads, plan, (len(proj), len(grad_context))),
        out_shape=jax.ShapeDtypeStruct((length, columns), bf16),
        grid_spec=pltpu.PrefetchScalarGridSpec(
            num_scalar_prefetch=3,
            grid=(tiles,),
            in_specs=[anywhere] * (len(proj) + len(grad_context) + 1) + [
                whole_block((heads, length)),
                whole_block((1, heads * globs)),
                whole_block((1, length)),
                whole_block((length, 1)),
                whole_block((globs, 1)),
                whole_block((globs, 1)),
                whole_block((1, heads * globs)),
                whole_block((length, 1)),
            ],
            out_specs=whole_block((length, columns)),
            scratch_shapes=[
                pltpu.VMEM((length, columns), bf16),
                pltpu.VMEM((length, width), bf16),
                pltpu.VMEM((length, width), bf16),
                pltpu.VMEM((width, length), bf16),
                pltpu.VMEM((globs, length), bf16),
                pltpu.VMEM((globs, width), bf16),
                pltpu.VMEM((width, globs), bf16),
                pltpu.VMEM((globs, width), bf16),
                pltpu.VMEM((globs, width), f32),
                pltpu.VMEM((globs, width), f32),
                pltpu.VMEM((length, width), f32),
                pltpu.VMEM((length, width), f32),
                pltpu.VMEM((heads * globs, width), bf16),
                pltpu.VMEM((heads * globs, width), bf16),
                pltpu.VMEM((heads * globs, width), f32),
                pltpu.VMEM((width, wide), bf16),
                pltpu.VMEM((width, wide), bf16),
                pltpu.VMEM((wide, width), bf16),
                pltpu.VMEM((wide, width), bf16),
                pltpu.VMEM((KTILE, wide), bf16),
                pltpu.VMEM((KTILE, wide), bf16),
                pltpu.VMEM((width, QTILE), f32),
                pltpu.SemaphoreType.DMA((length // plan[2],)),
                pltpu.SemaphoreType.DMA((length // plan[2],)),
                pltpu.SemaphoreType.DMA((length // plan[2],)),
            ],
        ),
        compiler_params=pltpu.CompilerParams(
            dimension_semantics=("arbitrary",), vmem_limit_bytes=VMEM_BYTES
        ),
        cost_estimate=pl.CostEstimate(
            flops=4 * length * 1024 * width, bytes_accessed=4 * length * width,
            transcendentals=length * 1024 * heads,
        ),
        name="attend_back",
    )(
        order, first, last, *proj, *grad_context, context, *log_sums,
        doc_row, doc_col, pos_col, gdoc_col, gdoc_row, plain_col,
    )


def sequence_info(docs_row, glob_pos, order, heads):
    length = docs_row.shape[0]
    tiles = length // QTILE
    firsts = jnp.arange(tiles, dtype=jnp.int32) * QTILE
    tile_docs = docs_row.reshape(tiles, QTILE)
    doc_start = jnp.sum(docs_row[None, :] < tile_docs[:, :1], 1, dtype=jnp.int32)
    doc_end = jnp.sum(docs_row[None, :] <= tile_docs[:, -1:], 1, dtype=jnp.int32)
    first = jnp.maximum(firsts - HALF, doc_start) // KTILE
    last = (jnp.minimum(firsts + QTILE + HALF, doc_end) + KTILE - 1) // KTILE
    hit = glob_pos[:, None] == jnp.arange(length, dtype=jnp.int32)[None, :]
    glob_docs = jnp.sum(jnp.where(hit, docs_row[None, :], 0), 1, dtype=jnp.int32)
    plain_col = jnp.where(jnp.any(hit, 0), 0.0, 1.0)[:, None]
    return (
        order,
        first,
        last,
        docs_row[None, :],
        docs_row[:, None],
        glob_pos[:, None],
        glob_docs[:, None],
        jnp.tile(glob_docs, heads)[None, :],
        plain_col.astype(jnp.float32),
    )


def norm_forward(resid, gain, shift):
    centred = resid - jnp.mean(resid, -1, keepdims=True)
    scale = lax.rsqrt(jnp.mean(centred * centred, -1, keepdims=True) + 1e-05)
    normed = centred * scale
    return normed * gain + shift, normed, scale


def norm_backward(grad, normed, scale, gain):
    weighted = grad * gain
    mean_one = jnp.mean(weighted, -1, keepdims=True)
    mean_two = jnp.mean(weighted * normed, -1, keepdims=True)
    grad_in = (weighted - mean_one - normed * mean_two) * scale
    return grad_in, jnp.stack([jnp.sum(grad * normed, 0), jnp.sum(grad, 0)])


def gelu_pair(up):
    cdf = 0.5 * (1.0 + lax.erf(up * (0.5**0.5)))
    slope = cdf + up * (jnp.exp(-0.5 * up * up) * (1.0 / math.sqrt(2.0 * math.pi)))
    return (up * cdf).astype(jnp.bfloat16), slope.astype(jnp.bfloat16)


def after(value, *others):
    return lax.optimization_barrier((value,) + others)[0]


def unpack_kernel(blocks, each, per_half, home_ref, mine_ref, theirs_ref, out_ref):
    upper = pl.program_id(0) < per_half
    take_mine = upper == (home_ref[0] == 1)
    for index in range(blocks):
        cols = slice(index * each, (index + 1) * each)
        value = jnp.where(
            take_mine, mine_ref[:, cols].astype(jnp.float32), theirs_ref[:, cols].astype(jnp.float32)
        )
        out_ref[index] = value


def unpack(home, mine, theirs, blocks, each):
    half, columns = mine.shape
    tile = min(256, half)
    per_half = half // tile
    source = pl.BlockSpec((tile, columns), lambda step, _: (lax.rem(step, per_half), 0))
    return pl.pallas_call(
        partial(unpack_kernel, blocks, each, per_half),
        out_shape=jax.ShapeDtypeStruct((blocks, 2 * half, each), jnp.float32),
        grid_spec=pltpu.PrefetchScalarGridSpec(
            num_scalar_prefetch=1,
            grid=(2 * per_half,),
            in_specs=[source, source],
            out_specs=pl.BlockSpec((blocks, tile, each), lambda step, _: (0, step, 0)),
        ),
        compiler_params=pltpu.CompilerParams(dimension_semantics=("arbitrary",)),
        name="unpack",
    )(home, mine, theirs)


def clip_kernel(kept, weight_ref, factor_ref, out_ref):
    for index, block in enumerate(kept):
        out_ref[:, index, :] = weight_ref[block].astype(jnp.float32) * factor_ref[index // 2]


def clip_weights(weight, factors):
    blocks, length, each = weight.shape
    kept = (0, 1, 3, 4)
    tile = min(128, length)
    return pl.pallas_call(
        partial(clip_kernel, kept),
        out_shape=jax.ShapeDtypeStruct((length, len(kept), each), jnp.float32),
        grid=(length // tile,),
        in_specs=[
            pl.BlockSpec((blocks, tile, each), lambda step: (0, step, 0)),
            pl.BlockSpec((2, 1, each), lambda step: (0, 0, 0)),
        ],
        out_specs=pl.BlockSpec((tile, len(kept), each), lambda step: (step, 0, 0)),
        compiler_params=pltpu.CompilerParams(dimension_semantics=("arbitrary",)),
        name="clip_weights",
    )(weight, factors)


def gated(value, *others):
    zero = 0.0
    for other in others:
        corner = lax.slice(other, (0,) * other.ndim, (1,) * other.ndim)
        zero = zero + corner.reshape(()).astype(jnp.float32) * 0.0
    return (value.astype(jnp.float32) + zero).astype(value.dtype)


def shards(tokens, cotangent, doc_ids, global_flags, w_attn, w_out, w_up, w_down, ln_gain, ln_bias):
    bf16, f32 = jnp.bfloat16, jnp.float32
    sections = lax.axis_size("section")
    slots = lax.axis_size("tensor")
    copies = lax.axis_size("dp")
    micro = tokens.shape[0]
    inner = slots // micro
    section = lax.axis_index("section")
    slot = lax.axis_index("tensor")
    row = slot // inner
    lane = slot % inner
    width = tokens.shape[3]
    chunk = tokens.shape[2]
    rows = min(QTILE, chunk)
    parts = chunk // rows
    plan = (inner, parts, rows)
    crossed = inner == 2
    joint = ("section", "tensor")
    groups = [[a * inner + b for b in range(inner)] for a in range(micro)]

    def device(s, a, b):
        return s * slots + a * inner + b

    def route(value, link):
        pairs = []
        for s in range(sections):
            for a in range(micro):
                for b in range(inner):
                    target = link(s, a, b)
                    if target is not None and target != (s, a, b):
                        pairs.append((device(s, a, b), device(*target)))
        return lax.ppermute(value, joint, pairs)

    def other_core(value):
        return lax.ppermute(value, "section", [(0, 1), (1, 0)])

    def other_row(value):
        return route(value, lambda s, a, b: (s, 1 - a, b))

    def other_lane(value):
        return route(value, lambda s, a, b: (s, a, 1 - b))

    class ByLane:
        home = section == row
        swap = staticmethod(other_lane)

        @staticmethod
        def keeper(s, a, b):
            return a

        @staticmethod
        def across(s, a, b):
            return (s, 1 - a, b)

    class ByRow:
        home = section == lane
        swap = staticmethod(other_row)

        @staticmethod
        def keeper(s, a, b):
            return b

        @staticmethod
        def across(s, a, b):
            return (s, a, 1 - b)

    split_attn = ByLane
    split_mlp = ByRow if crossed else ByLane

    def gather(own, split, hop=None):
        with jax.named_scope("gsec"):
            near = jnp.concatenate([own, other_core(own)], 0)
        if not crossed:
            if inner == 1:
                return [near]
            return [lax.all_gather(near, "tensor", axis=0, tiled=True, axis_index_groups=groups)]
        if hop is None:
            with jax.named_scope("ghop"):
                hop = split.swap(own)
        with jax.named_scope("gsec2"):
            return [near, jnp.concatenate([hop, other_core(hop)], 0)]

    def scatter_begin(partials, gates=()):
        if not crossed:
            blocks = partials[0].reshape(inner, 2, rows, -1)
            ours, theirs = blocks[:, 0], blocks[:, 1].astype(bf16)
            total = (ours + other_core(theirs).astype(f32)).reshape(inner * rows, -1)
            return total.astype(bf16), None
        near, far = partials
        with jax.named_scope("ssec"):
            leaving = far[:rows] + other_core(far[rows:].astype(bf16)).astype(f32)
            leaving = gated(leaving, *gates)
        with jax.named_scope("ssec2"):
            staying = near[:rows] + other_core(near[rows:].astype(bf16)).astype(f32)
        return leaving.astype(bf16), staying

    def scatter_end(begun, split):
        leaving, staying = begun
        if not crossed:
            if inner == 1:
                return leaving.astype(f32)
            return lax.psum_scatter(
                leaving, "tensor", scatter_dimension=0, tiled=True, axis_index_groups=groups
            ).astype(f32)
        with jax.named_scope("shop"):
            return staying + split.swap(leaving).astype(f32)

    def scatter_all(begun, split):
        sums = [scatter_end(item, split) for item in begun]
        if not crossed:
            return sums
        return [
            gated(item, begun[p + 1][0]) if p + 1 < len(sums) else item
            for p, item in enumerate(sums)
        ]

    def cut(array):
        per_part = 2 * inner * rows
        per_group = 2 * rows if crossed else per_part
        return [
            [array[p * per_part + g : p * per_part + g + per_group] for g in range(0, per_part, per_group)]
            for p in range(parts)
        ]

    def joined(pieces):
        return jnp.concatenate([piece for part in pieces for piece in part], 0)

    def flat(pieces):
        return [piece for part in pieces for piece in part]

    def part_rows(array):
        return [array[p * rows : (p + 1) * rows] for p in range(parts)]

    def own_rows(array):
        mine = lax.dynamic_index_in_dim(array[:, 0], row, 0, False)
        theirs = lax.dynamic_index_in_dim(array[:, 0], 1 - row, 0, False)
        moved = route(theirs, lambda s, a, b: (s, 1 - a, b) if s == a else None)
        return mine, moved

    def fetch(weight, layer, split):
        def across(s, a, b):
            if s != layer:
                return None
            _, a2, b2 = split.across(s, a, b)
            return (split.keeper(s, a, b), a2, b2)

        def within(s, a, b):
            return (split.keeper(s, a, b), a, b) if s == layer else None

        return route(weight, within), route(weight, across)

    def chosen(weight, arrived, layer, split):
        near, far = arrived
        return jnp.where(split.home, jnp.where(section == layer, weight, near), far)

    attn_table = w_attn[0].reshape(width, -1)
    mlp_pack = jnp.concatenate([w_up[0], w_down[0].reshape(width, -1)], 1)

    def attn_unpack(pack):
        columns = w_attn.shape[2] * w_attn.shape[3]
        return pack[:, :columns], pack[:, columns:].reshape(w_out.shape[1:])

    def mlp_unpack(pack):
        columns = w_up.shape[2]
        return pack[:, :columns], pack[:, columns:].reshape(w_down.shape[1:])

    mine, moved = own_rows(tokens)
    own = part_rows(jnp.where(ByLane.home, mine, moved))
    hops = []
    if crossed:
        early = route(mine, lambda s, a, b: (s, a, 1 - b) if s == a else None)
        late = route(moved, lambda s, a, b: (s, a, 1 - b) if s != a else None)
        hops = part_rows(jnp.where(ByLane.home, early, late))
    attn_weights = [None] * sections
    mlp_weights = [None] * sections
    attn_pack = jnp.concatenate([attn_table, w_out[0].reshape(width, -1)], 1)
    with jax.named_scope("W0attn"):
        first_pack = chosen(attn_pack, fetch(attn_pack, 0, split_attn), 0, split_attn)
    with jax.named_scope("W0mlp"):
        arriving = fetch(after(mlp_pack, *own, *hops), 0, split_mlp)

    heads = w_attn.shape[3] // HEAD
    docs = lax.dynamic_index_in_dim(doc_ids[:, 0], row, 0, False)
    flags = lax.dynamic_index_in_dim(global_flags[:, 0], row, 0, False)
    order = jnp.stack([section, lane if crossed else jnp.zeros_like(lane)]).astype(jnp.int32)
    info = sequence_info(docs, flags, order, heads)
    first_pack, mlp_pack, *info = lax.optimization_barrier((first_pack, mlp_pack, *info))
    attn_weights[0] = attn_unpack(first_pack)

    gains_own = jnp.stack([ln_gain[0], ln_bias[0]])
    gains_other = other_core(gains_own)
    norms = [jnp.where(section == layer, gains_own, gains_other) for layer in range(sections)]

    saved, outputs, peaks = [], [], []
    for layer in range(sections):
        gains, shifts = norms[layer]
        attn_w, out_w = attn_weights[layer]
        with jax.named_scope(f"F{layer}in"):
            inputs = [
                gather(own[p], split_attn, hops[p] if layer == 0 and crossed else None)
                for p in range(parts)
            ]
            proj = [[mm(piece, attn_w, NN, bf16) for piece in part] for part in inputs]
        context, lse, glse, *tops = attend(flat(proj), info, plan)
        peaks.append(tops)
        if layer == 0:
            with jax.named_scope("W1attn"):
                pack = fetch(after(attn_pack, *flat(proj)), 1, split_attn)
            context, arriving, pack = lax.optimization_barrier((context, arriving, pack))
            mlp_weights[0] = mlp_unpack(chosen(mlp_pack, arriving, 0, split_mlp))
            attn_weights[1] = attn_unpack(chosen(attn_pack, pack, 1, split_attn))
        else:
            with jax.named_scope("W1mlp"):
                pack = fetch(after(mlp_pack, *flat(proj)), 1, split_mlp)
            with jax.named_scope("COT"):
                mine, moved = own_rows(after(cotangent, *flat(proj)))
            context, pack, mine, moved = lax.optimization_barrier((context, pack, mine, moved))
            mlp_weights[1] = mlp_unpack(chosen(mlp_pack, pack, 1, split_mlp))
            grad_out = part_rows(jnp.where(ByLane.home, mine, moved).astype(f32))
        up_w, down_w = mlp_weights[layer]
        with jax.named_scope(f"F{layer}out"):
            sums = scatter_all(
                [scatter_begin([mm(piece, out_w) for piece in part]) for part in cut(context)],
                split_attn,
            )
        hidden, hidden_low, norms_one = [], [], []
        for p in range(parts):
            with jax.named_scope(f"F{layer}norm1"):
                value = gated(sums[p], hidden_low[-1]) if p else sums[p]
                value, normed, scale = norm_forward(own[p].astype(f32) + value, gains[0], shifts[0])
                hidden.append(value)
                hidden_low.append(value.astype(bf16))
                norms_one.append((normed, scale))
        hidden_rows, acts, slopes, begun = [], [], [], []
        for p in range(parts):
            with jax.named_scope(f"F{layer}mlp{p}"):
                hidden_rows.append(gather(hidden_low[p], split_mlp))
                pairs = [gelu_pair(mm(piece, up_w)) for piece in hidden_rows[p]]
                acts.append([act for act, _ in pairs])
                slopes.append([slope for _, slope in pairs])
                begun.append(
                    scatter_begin([mm(act, down_w) for act in acts[p]], hidden_low[p + 1 : p + 2])
                )
        with jax.named_scope(f"F{layer}mlp"):
            sums = scatter_all(begun, split_mlp)
        outs, norms_two = [], []
        for p in range(parts):
            with jax.named_scope(f"F{layer}norm2"):
                value = gated(sums[p], outs[-1]) if p else sums[p]
                value, normed, scale = norm_forward(hidden[p] + value, gains[1], shifts[1])
                norms_two.append((normed, scale))
                outs.append(value.astype(bf16))
        own = outs
        outputs.append(jnp.concatenate(outs, 0))
        saved.append(
            (inputs, proj, context, (lse, glse), norms_one, hidden_rows, acts, slopes, norms_two)
        )

    def to_owner(upper, lower, split, gates=()):
        def first_link(s, a, b):
            if s == split.keeper(s, a, b):
                return (1 - s, a, b)
            return split.across(s, a, b)

        def second_link(s, a, b):
            if s == split.keeper(s, a, b):
                return None
            _, a2, b2 = split.across(s, a, b)
            return (1 - s, a2, b2)

        first = route(gated(jnp.where(split.home, lower, upper), *gates), first_link)
        second = route(lower, second_link)
        part = first.astype(f32) + jnp.where(split.home, upper, second).astype(f32)
        return part.astype(bf16)

    earlier = ()

    def dp_sum(*terms):
        nonlocal earlier
        terms = [after(term, *earlier) for term in terms]
        earlier = lax.psum(tuple(terms), "dp")
        return earlier

    def pick(values):
        return jnp.where(section == 0, values[0], values[1])

    def placed(chunk, layer):
        arrived = []
        for index in range(micro):
            moved = route(chunk, lambda s, a, b: (layer, s, b) if a == index else None)
            stays = (section == layer) & ByLane.home & (row == index)
            arrived.append(jnp.where(stays, chunk, moved))
        return arrived

    def send_attn(pack, gates):
        half = width // 2
        return to_owner(pack[:half], pack[half:], split_attn, gates)

    attn_sums = [None] * sections
    mlp_sums = [None] * sections
    norm_sums = [None] * sections
    out_rows = [None] * sections
    grad_rows = [None] * sections
    for layer in reversed(range(sections)):
        (attn_w, out_w), (up_w, down_w) = attn_weights[layer], mlp_weights[layer]
        gains, _ = norms[layer]
        inputs, proj, context, log_sums, norms_one, hidden_rows, acts, slopes, norms_two = saved[layer]
        grads_two, low, sums_two = [], [], []
        for p in range(parts):
            with jax.named_scope(f"B{layer}norm2"):
                value = gated(grad_out[p], low[-1]) if p else grad_out[p]
                value, sums = norm_backward(value, *norms_two[p], gains[1])
                grads_two.append(value)
                low.append(value.astype(bf16))
                sums_two.append(sums)
        grad_mlp, grad_up, begun = [], [], []
        for p in range(parts):
            with jax.named_scope(f"B{layer}mlp{p}"):
                grad_mlp.append(gather(low[p], split_mlp))
                grad_up.append(
                    [
                        (mm(piece, down_w, NT) * slope.astype(f32)).astype(bf16)
                        for piece, slope in zip(grad_mlp[p], slopes[p])
                    ]
                )
                begun.append(
                    scatter_begin([mm(piece, up_w, NT) for piece in grad_up[p]], low[p + 1 : p + 2])
                )
        with jax.named_scope(f"B{layer}mlp"):
            sums = scatter_all(begun, split_mlp)
        with jax.named_scope(f"B{layer}wmlp"):
            grad_up_w = mm(joined(hidden_rows), joined(grad_up), TN, bf16)
            grad_down_w = mm(joined(acts), joined(grad_mlp), TN, bf16)
            sums[-1] = gated(sums[-1], grad_up_w, grad_down_w)
        grads_one, low, sums_one = [], [], []
        for p in range(parts):
            with jax.named_scope(f"B{layer}norm1"):
                value = gated(sums[p], low[-1]) if p else sums[p]
                value, total = norm_backward(value + grads_two[p], *norms_one[p], gains[0])
                grads_one.append(value)
                low.append(value.astype(bf16))
                sums_one.append(total)
        norm_sums[layer] = (sums_one, sums_two)
        grad_attn, grad_context = [], []
        for p in range(parts):
            with jax.named_scope(f"B{layer}ctx{p}"):
                grad_attn.append(gather(low[p], split_attn))
                grad_context.append([mm(piece, out_w, NT, bf16) for piece in grad_attn[p]])
        with jax.named_scope(f"B{layer}wmlp"):
            mlp_parts = to_owner(
                grad_up_w.reshape(width, -1), grad_down_w.reshape(width, -1), split_mlp,
                flat(grad_context) if layer else low,
            )
        if layer == 0:
            *grad_context[-1], mlp_sums[1] = lax.optimization_barrier(
                (*grad_context[-1], mlp_sums[1])
            )
        grad_context = flat(grad_context)
        if layer == 0:
            with jax.named_scope("B1wattn"):
                attn_parts = send_attn(pack, grad_context)
            *grad_context, mlp_parts = lax.optimization_barrier((*grad_context, mlp_parts))
            mlp_sums[0] = dp_sum(mlp_parts)[0]
        grad_proj = attend_back(flat(proj), context, log_sums, grad_context, info, plan)
        if layer == 1:
            with jax.named_scope("OUTROWS"):
                ready = lax.optimization_barrier((*outputs, *grad_context))[:sections]
                for index in range(sections):
                    out_rows[index] = placed(ready[index], index)
        if layer == 1:
            grad_proj, mlp_parts = lax.optimization_barrier((grad_proj, mlp_parts))
            mlp_sums[1] = dp_sum(mlp_parts)[0]
        else:
            grad_proj, attn_parts = lax.optimization_barrier((grad_proj, attn_parts))
        with jax.named_scope(f"B{layer}wattn"):
            grad_attn_w = mm(joined(inputs), grad_proj, TN, bf16)
            grad_out_w = mm(context, joined(grad_attn), TN, bf16)
            pack = jnp.concatenate([grad_attn_w, grad_out_w.reshape(width, -1)], 1)
        if layer == 0:
            grad_proj = after(grad_proj, pack)
        grad_low = []
        grad_proj_parts = cut(grad_proj)
        if layer == 0:
            *grad_proj_parts[-1], mlp_sums[0] = lax.optimization_barrier(
                (*grad_proj_parts[-1], mlp_sums[0])
            )
        with jax.named_scope(f"B{layer}in"):
            sums = scatter_all(
                [
                    scatter_begin(
                        [mm(piece, attn_w, NT) for piece in part],
                        (),
                    )
                    for part in grad_proj_parts
                ],
                split_attn,
            )
        for p in range(parts):
            with jax.named_scope(f"B{layer}in"):
                value = gated(sums[p], grad_low[-1]) if p else sums[p]
                grad_low.append((value + grads_one[p]).astype(bf16))
        grad_out = [piece.astype(f32) for piece in grad_low]
        if layer == 0:
            with jax.named_scope("B0wattn"):
                last_parts = send_attn(pack, ())
                attn_sums[1], attn_sums[0] = dp_sum(attn_parts, last_parts)
        with jax.named_scope("GRADROWS"):
            grad_rows[layer] = placed(jnp.concatenate(grad_low, 0), layer)

    def stacked_rows(by_layer):
        return jnp.stack([pick([by_layer[0][m], by_layer[1][m]]) for m in range(micro)])[None, :, None]

    def placed_weight(terms, split):
        mine = pick(terms)
        theirs = other_core(pick(terms[::-1]))
        first = jnp.where(split.home, mine, theirs)
        second = jnp.where(split.home, theirs, mine)
        return first.astype(f32), second.astype(f32)

    def dp_butterfly(value, combine):
        if copies & (copies - 1):
            gathered = lax.all_gather(value, "dp", axis=0)
            total = gathered[0]
            for index in range(1, copies):
                total = combine(total, gathered[index])
            return total
        distance = 1
        while distance < copies:
            pairs = [(d, d ^ distance) for d in range(copies)]
            value = combine(value, lax.ppermute(value, "dp", pairs))
            distance *= 2
        return value

    with jax.named_scope("NORMSUM"):
        mine = [
            jnp.stack([sum(sums_one[1:], sums_one[0]), sum(sums_two[1:], sums_two[0])])
            for sums_one, sums_two in norm_sums
        ]
        mine = [gated(term, grad_low[-1]) for term in mine]
        norm_sum = pick(mine) + other_core(pick(mine[::-1]))
        if crossed:
            norm_sum = norm_sum + other_row(norm_sum)
            norm_sum = norm_sum + other_lane(norm_sum)
        else:
            norm_sum = lax.psum(norm_sum, "tensor")
        norm_sum = dp_butterfly(norm_sum, jnp.add)
    with jax.named_scope("PEAK"):
        peak_all = lax.optimization_barrier((*flat(peaks), last_parts))[:-1]
        peak_all = jnp.stack(
            [jnp.max(value.reshape(heads, -1), 1) for value in peak_all]
        ).reshape(sections, 2, heads)
        peak_all = jnp.maximum(peak_all, other_row(peak_all))
        peak_all = dp_butterfly(peak_all, jnp.maximum)
        peak_here = jnp.where(ByLane.home, pick(peak_all), other_core(pick(peak_all[::-1])))
    factors = jnp.sqrt(clip_limit / jnp.maximum(peak_here, clip_limit))
    columns = jnp.repeat(factors, HEAD, axis=1)
    clipped = clip_weights(w_attn[0].transpose(1, 0, 2), columns[:, None, :])
    out_rows, grad_rows = stacked_rows(out_rows), stacked_rows(grad_rows)
    grad_up_w, grad_down_w = placed_weight(mlp_sums, split_mlp)
    attn_sums = [
        gated(term, out_rows, grad_rows, grad_up_w, grad_down_w, norm_sum, clipped)
        for term in attn_sums
    ]
    mine, theirs = pick(attn_sums), other_core(pick(attn_sums[::-1]))
    blocks, each = w_attn.shape[2:]
    home = split_attn.home.astype(jnp.int32).reshape(1)
    grad_attn_w = unpack(home, mine, theirs, blocks, each).transpose(1, 0, 2)
    halves = [half[:, blocks * each :].reshape(-1, w_out.shape[2]) for half in (mine, theirs)]
    grad_out_w = jnp.where(
        split_attn.home, jnp.concatenate(halves, 0), jnp.concatenate(halves[::-1], 0)
    ).astype(f32)

    return (
        out_rows,
        grad_rows,
        grad_attn_w[None],
        grad_out_w.reshape(w_out.shape),
        grad_up_w.reshape(w_up.shape),
        grad_down_w.reshape(w_down.shape),
        norm_sum[:, 0][None],
        norm_sum[:, 1][None],
        clipped[None],
    )


def solution(mesh):
    in_specs = (
        P(None, "dp", "tensor", None),
        P(None, "dp", "tensor", None),
        P(None, "dp", None),
        P(None, "dp", None),
        P("section", None, None, "tensor"),
        P("section", "tensor", None),
        P("section", None, "tensor"),
        P("section", "tensor", None),
        P("section", None, None),
        P("section", None, None),
    )
    out_specs = (
        P("section", None, "dp", "tensor", None),
        P("section", None, "dp", "tensor", None),
        P("section", None, None, "tensor"),
        P("section", "tensor", None),
        P("section", None, "tensor"),
        P("section", "tensor", None),
        P("section", None, None),
        P("section", None, None),
        P("section", None, None, "tensor"),
    )
    return jax.shard_map(shards, mesh=mesh, in_specs=in_specs, out_specs=out_specs, check_vma=False)
```

```python
import math
from functools import partial

import jax
import jax.numpy as jnp
from jax import lax
from jax.experimental import pallas as pl
from jax.experimental.pallas import tpu as pltpu
from jax.sharding import PartitionSpec as P

HEAD = 64
HALF = 512
QTILE = 256
KTILE = 512
VMEM_BYTES = 56 * 1024 * 1024

masked_fill = -1e30
clip_limit = 10.0
score_scale = HEAD ** (-0.5)

NN = (((1,), (0,)), ((), ()))
NT = (((1,), (1,)), ((), ()))
TN = (((0,), (0,)), ((), ()))


def mm(left, right, dims=NN, out=jnp.float32):
    return lax.dot_general(left, right, dims, preferred_element_type=jnp.float32).astype(out)


def tile_bias(first_key, first_query, key_docs, query_docs, keys, queries):
    key_pos = first_key + lax.broadcasted_iota(jnp.int32, (keys, queries), 0)
    query_pos = first_query + lax.broadcasted_iota(jnp.int32, (keys, queries), 1)
    gap = jnp.abs(key_pos - query_pos)
    return jnp.where((key_docs == query_docs) & (gap <= HALF), 0.0, masked_fill)


def far_bias(glob_pos, first_query, glob_docs, query_docs, globs, queries):
    query_pos = first_query + lax.broadcasted_iota(jnp.int32, (globs, queries), 1)
    gap = jnp.abs(glob_pos - query_pos)
    return jnp.where((glob_docs == query_docs) & (gap > HALF), 0.0, masked_fill)


def one_hot_rows(glob_pos, length):
    globs = glob_pos.shape[0]
    hit = lax.broadcasted_iota(jnp.int32, (globs, length), 1) == glob_pos
    return jnp.where(hit, 1.0, 0.0).astype(jnp.bfloat16)


def true_unit(place, order_ref, plan):
    inner, parts, _ = plan
    part, rest = place // (2 * inner), place % (2 * inner)
    side = (rest % 2) ^ order_ref[0]
    lane = (rest // 2) ^ order_ref[1]
    return (side * inner + lane) * parts + part


def local_unit(unit, order_ref, plan):
    inner, parts, _ = plan
    block, part = lax.div(unit, parts), lax.rem(unit, parts)
    side = lax.div(block, inner) ^ order_ref[0]
    lane = lax.rem(block, inner) ^ order_ref[1]
    return part * (2 * inner) + lane * 2 + side


def join_pieces(order_ref, pieces, joined_ref, sems, plan):
    rows = plan[2]
    copies = []
    place = 0
    for piece in pieces:
        for index in range(piece.shape[0] // rows):
            start = pl.multiple_of(true_unit(place, order_ref, plan) * rows, rows)
            copies.append(
                pltpu.make_async_copy(
                    piece.at[pl.ds(index * rows, rows), :],
                    joined_ref.at[pl.ds(start, rows), :],
                    sems.at[place],
                )
            )
            place += 1
    for copy in copies:
        copy.start()
    for copy in copies:
        copy.wait()


def store_local(out_ref, tile, cols, value, order_ref, plan):
    rows = plan[2]
    size = min(rows, value.shape[0])
    for index in range(value.shape[0] // size):
        row = tile * value.shape[0] + index * size
        place = local_unit(lax.div(row, rows), order_ref, plan)
        start = pl.multiple_of(place * rows + lax.rem(row, rows), size)
        out_ref[pl.ds(start, size), cols] = value[index * size : (index + 1) * size]


def diagonal_sum(blocks, heads, rows):
    owner = lax.broadcasted_iota(jnp.int32, (rows, heads * HEAD), 1) // HEAD
    total = jnp.zeros((rows, heads * HEAD), jnp.float32)
    for head in range(heads):
        total = total + jnp.where(owner == head, blocks[head * rows : (head + 1) * rows], 0.0)
    return total


def attend_kernel(
    heads,
    plan,
    count,
    order_ref,
    first_ref,
    last_ref,
    *refs,
):
    pieces, refs = refs[:count], refs[count:]
    attend_body(heads, plan, order_ref, first_ref, last_ref, pieces, *refs)


def attend_body(
    heads,
    plan,
    order_ref,
    first_ref,
    last_ref,
    pieces,
    doc_row_ref,
    doc_col_ref,
    pos_col_ref,
    gdoc_col_ref,
    gdoc_row_ref,
    ctx_ref,
    lse_ref,
    glse_ref,
    peak_ref,
    gpeak_ref,
    proj,
    values_t,
    hot,
    far_keys,
    far_values_t,
    gctx_t,
    gstack,
    gscores,
    wide,
    acc,
    top,
    total,
    sems,
):
    length = proj.shape[0]
    width = heads * HEAD
    globs = pos_col_ref.shape[0]
    step = pl.program_id(0)

    @pl.when(step == 0)
    def _():
        join_pieces(order_ref, pieces, proj, sems, plan)
        wide[...] = jnp.zeros_like(wide)
        gstack[...] = jnp.zeros_like(gstack)
        hot[...] = one_hot_rows(pos_col_ref[...], length)
        hot_all = hot[...]
        far_keys[...] = mm(hot_all, proj[:, width : 2 * width], out=jnp.bfloat16)
        far_values_t[...] = mm(hot_all, proj[:, 2 * width : 3 * width]).T.astype(jnp.bfloat16)
        queries = (mm(hot_all, proj[:, 3 * width : 4 * width]) * score_scale).astype(jnp.bfloat16)
        for head in range(heads):
            cols = slice(head * HEAD, (head + 1) * HEAD)
            gstack[head * globs : (head + 1) * globs, cols] = queries[:, cols]

        def score_tile(tile, best):
            rows = pl.ds(pl.multiple_of(tile * KTILE, KTILE), KTILE)
            values_t[:, rows] = proj[rows, 2 * width : 3 * width].T
            scores = mm(proj[rows, 4 * width : 5 * width], gstack[...], NT)
            scores = jnp.where(doc_col_ref[rows, :] == gdoc_row_ref[...], scores, masked_fill)
            gscores[rows, :] = scores
            return jnp.maximum(best, jnp.max(scores, 0, keepdims=True))

        best = lax.fori_loop(
            0, length // KTILE, score_tile, jnp.full((1, heads * globs), masked_fill, jnp.float32)
        )

        def sum_tile(tile, sums):
            rows = pl.ds(pl.multiple_of(tile * KTILE, KTILE), KTILE)
            weights = jnp.exp(gscores[rows, :] - best)
            gscores[rows, :] = weights
            return sums + jnp.sum(weights, 0, keepdims=True)

        sums = lax.fori_loop(
            0, length // KTILE, sum_tile, jnp.zeros((1, heads * globs), jnp.float32)
        )

        def value_tile(tile, blocks):
            rows = pl.ds(pl.multiple_of(tile * KTILE, KTILE), KTILE)
            probs = (gscores[rows, :] / sums).T.astype(jnp.bfloat16)
            return blocks + mm(probs, proj[rows, 5 * width : 6 * width])

        blocks = lax.fori_loop(
            0, length // KTILE, value_tile, jnp.zeros((heads * globs, width), jnp.float32)
        )
        gctx_t[...] = diagonal_sum(blocks, heads, globs).T.astype(jnp.bfloat16)
        glse_ref[...] = best + jnp.log(sums)
        gpeak_ref[...] = best

    start = pl.multiple_of(step * QTILE, QTILE)
    query_rows = pl.ds(start, QTILE)
    query_t = proj[query_rows, 0:width].T * score_scale
    for head in range(heads):
        rows = slice(head * HEAD, (head + 1) * HEAD)
        wide[rows, head * QTILE : (head + 1) * QTILE] = query_t[rows].astype(jnp.bfloat16)
    query_docs = doc_row_ref[:, query_rows]

    scores = mm(far_keys[...], wide[...])
    bias = far_bias(pos_col_ref[...], start, gdoc_col_ref[...], query_docs, globs, QTILE)
    for head in range(heads):
        cols = slice(head * QTILE, (head + 1) * QTILE)
        rows = slice(head * HEAD, (head + 1) * HEAD)
        part = scores[:, cols] + bias
        best = jnp.max(part, 0, keepdims=True)
        weights = jnp.exp(part - best)
        top[:, cols] = best
        total[:, cols] = jnp.sum(weights, 0, keepdims=True)
        acc[rows, :] = mm(far_values_t[rows, :], weights.astype(jnp.bfloat16))

    def key_tile(tile, carry):
        key_start = pl.multiple_of(tile * KTILE, KTILE)
        keys = pl.ds(key_start, KTILE)
        scores = mm(proj[keys, width : 2 * width], wide[...])
        bias = tile_bias(key_start, start, doc_col_ref[keys, :], query_docs, KTILE, QTILE)
        for head in range(heads):
            cols = slice(head * QTILE, (head + 1) * QTILE)
            rows = slice(head * HEAD, (head + 1) * HEAD)
            part = scores[:, cols] + bias
            old = top[:, cols]
            best = jnp.maximum(old, jnp.max(part, 0, keepdims=True))
            weights = jnp.exp(part - best)
            shrink = jnp.exp(old - best)
            top[:, cols] = best
            total[:, cols] = total[:, cols] * shrink + jnp.sum(weights, 0, keepdims=True)
            acc[rows, :] = acc[rows, :] * shrink + mm(
                values_t[rows, keys], weights.astype(jnp.bfloat16)
            )
        return carry

    lax.fori_loop(first_ref[step], last_ref[step], key_tile, 0)

    hot_tile = hot[:, query_rows]
    is_glob = jnp.max(hot_tile.astype(jnp.float32), 0, keepdims=True) > 0.5
    for head in range(heads):
        cols = slice(head * QTILE, (head + 1) * QTILE)
        rows = slice(head * HEAD, (head + 1) * HEAD)
        acc[rows, :] = acc[rows, :] / total[:, cols]
        lse_ref[head : head + 1, :] = top[:, cols] + jnp.log(total[:, cols])
    merged = jnp.where(is_glob, mm(gctx_t[...], hot_tile), acc[...])
    store_local(ctx_ref, step, slice(None), merged.T.astype(jnp.bfloat16), order_ref, plan)

    @pl.when(step == 0)
    def _():
        peak_ref[...] = top[...]

    @pl.when(step > 0)
    def _():
        peak_ref[...] = jnp.maximum(peak_ref[...], top[...])


def whole_block(shape):
    return pl.BlockSpec(shape, lambda *_: (0,) * len(shape), pipeline_mode=pl.Buffered(1))


def attend(proj, info, plan):
    length = sum(piece.shape[0] for piece in proj)
    columns = proj[0].shape[1]
    heads = columns // (6 * HEAD)
    width = heads * HEAD
    order, first, last, doc_row, doc_col, pos_col, gdoc_col, gdoc_row, _ = info
    globs = pos_col.shape[0]
    tiles = length // QTILE
    bf16, f32 = jnp.bfloat16, jnp.float32

    anywhere = pl.BlockSpec(memory_space=pl.ANY)
    return pl.pallas_call(
        partial(attend_kernel, heads, plan, len(proj)),
        out_shape=(
            jax.ShapeDtypeStruct((length, width), bf16),
            jax.ShapeDtypeStruct((heads, length), f32),
            jax.ShapeDtypeStruct((1, heads * globs), f32),
            jax.ShapeDtypeStruct((1, heads * QTILE), f32),
            jax.ShapeDtypeStruct((1, heads * globs), f32),
        ),
        grid_spec=pltpu.PrefetchScalarGridSpec(
            num_scalar_prefetch=3,
            grid=(tiles,),
            in_specs=[anywhere] * len(proj) + [
                whole_block((1, length)),
                whole_block((length, 1)),
                whole_block((globs, 1)),
                whole_block((globs, 1)),
                whole_block((1, heads * globs)),
            ],
            out_specs=(
                whole_block((length, width)),
                pl.BlockSpec((heads, QTILE), lambda step, *_: (0, step)),
                pl.BlockSpec((1, heads * globs), lambda *_: (0, 0)),
                pl.BlockSpec((1, heads * QTILE), lambda *_: (0, 0)),
                pl.BlockSpec((1, heads * globs), lambda *_: (0, 0)),
            ),
            scratch_shapes=[
                pltpu.VMEM((length, columns), bf16),
                pltpu.VMEM((width, length), bf16),
                pltpu.VMEM((globs, length), bf16),
                pltpu.VMEM((globs, width), bf16),
                pltpu.VMEM((width, globs), bf16),
                pltpu.VMEM((width, globs), bf16),
                pltpu.VMEM((heads * globs, width), bf16),
                pltpu.VMEM((length, heads * globs), f32),
                pltpu.VMEM((width, heads * QTILE), bf16),
                pltpu.VMEM((width, QTILE), f32),
                pltpu.VMEM((1, heads * QTILE), f32),
                pltpu.VMEM((1, heads * QTILE), f32),
                pltpu.SemaphoreType.DMA((length // plan[2],)),
            ],
        ),
        compiler_params=pltpu.CompilerParams(
            dimension_semantics=("arbitrary",), vmem_limit_bytes=VMEM_BYTES
        ),
        cost_estimate=pl.CostEstimate(
            flops=20 * length * 1024 * width, bytes_accessed=14 * length * width,
            transcendentals=length * 1024 * heads,
        ),
        name="attend",
    )(order, first, last, *proj, doc_row, doc_col, pos_col, gdoc_col, gdoc_row)


def attend_back_kernel(
    heads,
    plan,
    counts,
    order_ref,
    first_ref,
    last_ref,
    *refs,
):
    pieces, refs = refs[: counts[0]], refs[counts[0] :]
    grad_pieces, refs = refs[: counts[1]], refs[counts[1] :]
    attend_back_body(heads, plan, order_ref, first_ref, last_ref, pieces, grad_pieces, *refs)


def attend_back_body(
    heads,
    plan,
    order_ref,
    first_ref,
    last_ref,
    pieces,
    grad_pieces,
    ctx_piece_ref,
    lse_ref,
    glse_ref,
    doc_row_ref,
    doc_col_ref,
    pos_col_ref,
    gdoc_col_ref,
    gdoc_row_ref,
    plain_col_ref,
    out_ref,
    proj,
    ctx,
    grad,
    keys_t,
    hot,
    far_keys,
    far_keys_t,
    far_values,
    far_key_grad,
    far_value_grad,
    key_grad,
    value_grad,
    gquery,
    gout,
    gquery_grad,
    wide,
    wide_grad,
    stack,
    stack_grad,
    probs_low,
    grads_low,
    query_grad_t,
    proj_sems,
    ctx_sems,
    grad_sems,
):
    length = proj.shape[0]
    width = heads * HEAD
    globs = pos_col_ref.shape[0]
    tiles = length // KTILE
    step = pl.program_id(0)
    bf16 = jnp.bfloat16

    def store(tile, block, value):
        cols = slice(block * width, (block + 1) * width)
        store_local(out_ref, tile, cols, value.astype(bf16), order_ref, plan)

    @pl.when(step == 0)
    def _():
        join_pieces(order_ref, pieces, proj, proj_sems, plan)
        join_pieces(order_ref, [ctx_piece_ref], ctx, ctx_sems, plan)
        join_pieces(order_ref, grad_pieces, grad, grad_sems, plan)
        for ref in (wide, wide_grad, stack, stack_grad, gquery, gout):
            ref[...] = jnp.zeros_like(ref)
        for ref in (key_grad, value_grad, far_key_grad, far_value_grad):
            ref[...] = jnp.zeros_like(ref)
        gquery_grad[...] = jnp.zeros_like(gquery_grad)
        hot[...] = one_hot_rows(pos_col_ref[...], length)
        hot_all = hot[...]
        near = mm(hot_all, proj[:, width : 2 * width])
        far_keys[...] = near.astype(bf16)
        far_keys_t[...] = near.T.astype(bf16)
        far_values[...] = mm(hot_all, proj[:, 2 * width : 3 * width], out=bf16)
        queries = (mm(hot_all, proj[:, 3 * width : 4 * width]) * score_scale).astype(bf16)
        out_grad = mm(hot_all, grad[...])
        glob_ctx = mm(hot_all, ctx[...])
        product = out_grad * glob_ctx
        owner = lax.broadcasted_iota(jnp.int32, (globs, width), 1) // HEAD
        dots = []
        for head in range(heads):
            cols = slice(head * HEAD, (head + 1) * HEAD)
            rows = slice(head * globs, (head + 1) * globs)
            gquery[rows, cols] = queries[:, cols]
            gout[rows, cols] = out_grad[:, cols].astype(bf16)
            own = jnp.where(owner == head, product, 0.0)
            dots.append(jnp.sum(own, 1, keepdims=True))
        dot_row = jnp.broadcast_to(jnp.concatenate(dots, 0), (heads * globs, 128)).T[0:1]

        def glob_tile(tile, carry):
            rows = pl.ds(pl.multiple_of(tile * KTILE, KTILE), KTILE)
            keys_t[:, rows] = proj[rows, width : 2 * width].T
            scores = mm(proj[rows, 4 * width : 5 * width], gquery[...], NT)
            scores = jnp.where(doc_col_ref[rows, :] == gdoc_row_ref[...], scores, masked_fill)
            probs = jnp.exp(scores - glse_ref[...])
            grad_p = mm(proj[rows, 5 * width : 6 * width], gout[...], NT)
            grad_s = probs * (grad_p - dot_row)
            store(tile, 5, mm(probs.astype(bf16), gout[...]))
            store(tile, 4, mm(grad_s.astype(bf16), gquery[...]))
            gquery_grad[...] += mm(grad_s.T.astype(bf16), proj[rows, 4 * width : 5 * width])
            return carry

        lax.fori_loop(0, tiles, glob_tile, 0)
        query_grad = diagonal_sum(gquery_grad[...], heads, globs) * score_scale
        query_grad = query_grad.astype(bf16)

        def spread_tile(tile, carry):
            rows = pl.ds(pl.multiple_of(tile * KTILE, KTILE), KTILE)
            store(tile, 3, mm(hot[:, rows], query_grad, TN))
            return carry

        lax.fori_loop(0, tiles, spread_tile, 0)

    start = pl.multiple_of(step * QTILE, QTILE)
    query_rows = pl.ds(start, QTILE)
    query = proj[query_rows, 0:width].astype(jnp.float32) * score_scale
    query_t = query.T.astype(bf16)
    query = query.astype(bf16)
    grad_out = grad[query_rows, :].astype(jnp.float32) * plain_col_ref[query_rows, :]
    grad_out_t = grad_out.T
    product_t = grad_out_t * ctx[query_rows, :].astype(jnp.float32).T
    grad_out = grad_out.astype(bf16)
    grad_out_t = grad_out_t.astype(bf16)
    dots = []
    for head in range(heads):
        own = slice(head * HEAD, (head + 1) * HEAD)
        cols = slice(head * QTILE, (head + 1) * QTILE)
        wide[own, cols] = query_t[own]
        wide_grad[own, cols] = grad_out_t[own]
        stack[cols, own] = query[:, own]
        stack_grad[cols, own] = grad_out[:, own]
        dots.append(jnp.sum(product_t[own], 0, keepdims=True))
    query_docs = doc_row_ref[:, query_rows]

    def parts(scores, grad_p, bias, head):
        cols = slice(head * QTILE, (head + 1) * QTILE)
        shift = lse_ref[head : head + 1, query_rows]
        probs = jnp.exp(scores[:, cols] + bias - shift)
        grad_s = probs * (grad_p[:, cols] - dots[head])
        return probs.astype(bf16), grad_s.astype(bf16)

    scores = mm(far_keys[...], wide[...])
    grad_p = mm(far_values[...], wide_grad[...])
    bias = far_bias(pos_col_ref[...], start, gdoc_col_ref[...], query_docs, globs, QTILE)
    for head in range(heads):
        cols = slice(head * QTILE, (head + 1) * QTILE)
        own = slice(head * HEAD, (head + 1) * HEAD)
        probs, grad_s = parts(scores, grad_p, bias, head)
        probs_low[0:globs, cols] = probs
        grads_low[0:globs, cols] = grad_s
        query_grad_t[own, :] = mm(far_keys_t[own, :], grad_s)
    far_value_grad[...] += mm(probs_low[0:globs, :], stack_grad[...])
    far_key_grad[...] += mm(grads_low[0:globs, :], stack[...])

    def key_tile(tile, carry):
        key_start = pl.multiple_of(tile * KTILE, KTILE)
        keys = pl.ds(key_start, KTILE)
        scores = mm(proj[keys, width : 2 * width], wide[...])
        grad_p = mm(proj[keys, 2 * width : 3 * width], wide_grad[...])
        bias = tile_bias(key_start, start, doc_col_ref[keys, :], query_docs, KTILE, QTILE)
        for head in range(heads):
            cols = slice(head * QTILE, (head + 1) * QTILE)
            own = slice(head * HEAD, (head + 1) * HEAD)
            probs, grad_s = parts(scores, grad_p, bias, head)
            probs_low[:, cols] = probs
            grads_low[:, cols] = grad_s
            query_grad_t[own, :] += mm(keys_t[own, keys], grad_s)
        value_grad[keys, :] += mm(probs_low[...], stack_grad[...])
        key_grad[keys, :] += mm(grads_low[...], stack[...])
        return carry

    lax.fori_loop(first_ref[step], last_ref[step], key_tile, 0)
    store(step, 0, (query_grad_t[...] * score_scale).T)

    @pl.when(step == pl.num_programs(0) - 1)
    def _():
        far_key = far_key_grad[...].astype(bf16)
        far_value = far_value_grad[...].astype(bf16)

        def close_tile(tile, carry):
            rows = pl.ds(pl.multiple_of(tile * KTILE, KTILE), KTILE)
            hot_tile = hot[:, rows]
            key_sum = key_grad[rows, :] + mm(hot_tile, far_key, TN)
            value_sum = value_grad[rows, :] + mm(hot_tile, far_value, TN)
            store(tile, 1, key_sum)
            store(tile, 2, value_sum)
            return carry

        lax.fori_loop(0, tiles, close_tile, 0)


def attend_back(proj, context, log_sums, grad_context, info, plan):
    length = context.shape[0]
    columns = proj[0].shape[1]
    heads = columns // (6 * HEAD)
    width = heads * HEAD
    order, first, last, doc_row, doc_col, pos_col, gdoc_col, gdoc_row, plain_col = info
    globs = pos_col.shape[0]
    tiles = length // QTILE
    bf16, f32 = jnp.bfloat16, jnp.float32
    wide = heads * QTILE
    anywhere = pl.BlockSpec(memory_space=pl.ANY)
    return pl.pallas_call(
        partial(attend_back_kernel, heads, plan, (len(proj), len(grad_context))),
        out_shape=jax.ShapeDtypeStruct((length, columns), bf16),
        grid_spec=pltpu.PrefetchScalarGridSpec(
            num_scalar_prefetch=3,
            grid=(tiles,),
            in_specs=[anywhere] * (len(proj) + len(grad_context) + 1) + [
                whole_block((heads, length)),
                whole_block((1, heads * globs)),
                whole_block((1, length)),
                whole_block((length, 1)),
                whole_block((globs, 1)),
                whole_block((globs, 1)),
                whole_block((1, heads * globs)),
                whole_block((length, 1)),
            ],
            out_specs=whole_block((length, columns)),
            scratch_shapes=[
                pltpu.VMEM((length, columns), bf16),
                pltpu.VMEM((length, width), bf16),
                pltpu.VMEM((length, width), bf16),
                pltpu.VMEM((width, length), bf16),
                pltpu.VMEM((globs, length), bf16),
                pltpu.VMEM((globs, width), bf16),
                pltpu.VMEM((width, globs), bf16),
                pltpu.VMEM((globs, width), bf16),
                pltpu.VMEM((globs, width), f32),
                pltpu.VMEM((globs, width), f32),
                pltpu.VMEM((length, width), f32),
                pltpu.VMEM((length, width), f32),
                pltpu.VMEM((heads * globs, width), bf16),
                pltpu.VMEM((heads * globs, width), bf16),
                pltpu.VMEM((heads * globs, width), f32),
                pltpu.VMEM((width, wide), bf16),
                pltpu.VMEM((width, wide), bf16),
                pltpu.VMEM((wide, width), bf16),
                pltpu.VMEM((wide, width), bf16),
                pltpu.VMEM((KTILE, wide), bf16),
                pltpu.VMEM((KTILE, wide), bf16),
                pltpu.VMEM((width, QTILE), f32),
                pltpu.SemaphoreType.DMA((length // plan[2],)),
                pltpu.SemaphoreType.DMA((length // plan[2],)),
                pltpu.SemaphoreType.DMA((length // plan[2],)),
            ],
        ),
        compiler_params=pltpu.CompilerParams(
            dimension_semantics=("arbitrary",), vmem_limit_bytes=VMEM_BYTES
        ),
        cost_estimate=pl.CostEstimate(
            flops=4 * length * 1024 * width, bytes_accessed=4 * length * width,
            transcendentals=length * 1024 * heads,
        ),
        name="attend_back",
    )(
        order, first, last, *proj, *grad_context, context, *log_sums,
        doc_row, doc_col, pos_col, gdoc_col, gdoc_row, plain_col,
    )


def sequence_info(docs_row, glob_pos, order, heads):
    length = docs_row.shape[0]
    tiles = length // QTILE
    firsts = jnp.arange(tiles, dtype=jnp.int32) * QTILE
    tile_docs = docs_row.reshape(tiles, QTILE)
    doc_start = jnp.sum(docs_row[None, :] < tile_docs[:, :1], 1, dtype=jnp.int32)
    doc_end = jnp.sum(docs_row[None, :] <= tile_docs[:, -1:], 1, dtype=jnp.int32)
    first = jnp.maximum(firsts - HALF, doc_start) // KTILE
    last = (jnp.minimum(firsts + QTILE + HALF, doc_end) + KTILE - 1) // KTILE
    hit = glob_pos[:, None] == jnp.arange(length, dtype=jnp.int32)[None, :]
    glob_docs = jnp.sum(jnp.where(hit, docs_row[None, :], 0), 1, dtype=jnp.int32)
    plain_col = jnp.where(jnp.any(hit, 0), 0.0, 1.0)[:, None]
    return (
        order,
        first,
        last,
        docs_row[None, :],
        docs_row[:, None],
        glob_pos[:, None],
        glob_docs[:, None],
        jnp.tile(glob_docs, heads)[None, :],
        plain_col.astype(jnp.float32),
    )


def norm_forward(resid, gain, shift):
    centred = resid - jnp.mean(resid, -1, keepdims=True)
    scale = lax.rsqrt(jnp.mean(centred * centred, -1, keepdims=True) + 1e-05)
    normed = centred * scale
    return normed * gain + shift, normed, scale


def norm_backward(grad, normed, scale, gain):
    weighted = grad * gain
    mean_one = jnp.mean(weighted, -1, keepdims=True)
    mean_two = jnp.mean(weighted * normed, -1, keepdims=True)
    grad_in = (weighted - mean_one - normed * mean_two) * scale
    return grad_in, jnp.stack([jnp.sum(grad * normed, 0), jnp.sum(grad, 0)])


def gelu_pair(up):
    cdf = 0.5 * (1.0 + lax.erf(up * (0.5**0.5)))
    slope = cdf + up * (jnp.exp(-0.5 * up * up) * (1.0 / math.sqrt(2.0 * math.pi)))
    return (up * cdf).astype(jnp.bfloat16), slope.astype(jnp.bfloat16)


def after(value, *others):
    return lax.optimization_barrier((value,) + others)[0]


def unpack_kernel(blocks, each, per_half, home_ref, mine_ref, theirs_ref, out_ref):
    upper = pl.program_id(0) < per_half
    take_mine = upper == (home_ref[0] == 1)
    for index in range(blocks):
        cols = slice(index * each, (index + 1) * each)
        value = jnp.where(
            take_mine, mine_ref[:, cols].astype(jnp.float32), theirs_ref[:, cols].astype(jnp.float32)
        )
        out_ref[index] = value


def unpack(home, mine, theirs, blocks, each):
    half, columns = mine.shape
    tile = min(256, half)
    per_half = half // tile
    source = pl.BlockSpec((tile, columns), lambda step, _: (lax.rem(step, per_half), 0))
    return pl.pallas_call(
        partial(unpack_kernel, blocks, each, per_half),
        out_shape=jax.ShapeDtypeStruct((blocks, 2 * half, each), jnp.float32),
        grid_spec=pltpu.PrefetchScalarGridSpec(
            num_scalar_prefetch=1,
            grid=(2 * per_half,),
            in_specs=[source, source],
            out_specs=pl.BlockSpec((blocks, tile, each), lambda step, _: (0, step, 0)),
        ),
        compiler_params=pltpu.CompilerParams(dimension_semantics=("arbitrary",)),
        name="unpack",
    )(home, mine, theirs)


def clip_kernel(kept, weight_ref, factor_ref, out_ref):
    for index, block in enumerate(kept):
        out_ref[:, index, :] = weight_ref[block].astype(jnp.float32) * factor_ref[index // 2]


def clip_weights(weight, factors):
    blocks, length, each = weight.shape
    kept = (0, 1, 3, 4)
    tile = min(128, length)
    return pl.pallas_call(
        partial(clip_kernel, kept),
        out_shape=jax.ShapeDtypeStruct((length, len(kept), each), jnp.float32),
        grid=(length // tile,),
        in_specs=[
            pl.BlockSpec((blocks, tile, each), lambda step: (0, step, 0)),
            pl.BlockSpec((2, 1, each), lambda step: (0, 0, 0)),
        ],
        out_specs=pl.BlockSpec((tile, len(kept), each), lambda step: (step, 0, 0)),
        compiler_params=pltpu.CompilerParams(dimension_semantics=("arbitrary",)),
        name="clip_weights",
    )(weight, factors)


def gated(value, *others):
    zero = 0.0
    for other in others:
        corner = lax.slice(other, (0,) * other.ndim, (1,) * other.ndim)
        zero = zero + corner.reshape(()).astype(jnp.float32) * 0.0
    return (value.astype(jnp.float32) + zero).astype(value.dtype)


def shards(tokens, cotangent, doc_ids, global_flags, w_attn, w_out, w_up, w_down, ln_gain, ln_bias):
    bf16, f32 = jnp.bfloat16, jnp.float32
    sections = lax.axis_size("section")
    slots = lax.axis_size("tensor")
    copies = lax.axis_size("dp")
    micro = tokens.shape[0]
    inner = slots // micro
    section = lax.axis_index("section")
    slot = lax.axis_index("tensor")
    row = slot // inner
    lane = slot % inner
    width = tokens.shape[3]
    chunk = tokens.shape[2]
    rows = min(QTILE, chunk)
    parts = chunk // rows
    plan = (inner, parts, rows)
    crossed = inner == 2
    joint = ("section", "tensor")
    groups = [[a * inner + b for b in range(inner)] for a in range(micro)]

    def device(s, a, b):
        return s * slots + a * inner + b

    def route(value, link):
        pairs = []
        for s in range(sections):
            for a in range(micro):
                for b in range(inner):
                    target = link(s, a, b)
                    if target is not None and target != (s, a, b):
                        pairs.append((device(s, a, b), device(*target)))
        return lax.ppermute(value, joint, pairs)

    def other_core(value):
        return lax.ppermute(value, "section", [(0, 1), (1, 0)])

    def other_row(value):
        return route(value, lambda s, a, b: (s, 1 - a, b))

    def other_lane(value):
        return route(value, lambda s, a, b: (s, a, 1 - b))

    class ByLane:
        home = section == row
        swap = staticmethod(other_lane)

        @staticmethod
        def keeper(s, a, b):
            return a

        @staticmethod
        def across(s, a, b):
            return (s, 1 - a, b)

    class ByRow:
        home = section == lane
        swap = staticmethod(other_row)

        @staticmethod
        def keeper(s, a, b):
            return b

        @staticmethod
        def across(s, a, b):
            return (s, a, 1 - b)

    split_attn = ByLane
    split_mlp = ByRow if crossed else ByLane

    def gather(own, split, hop=None):
        with jax.named_scope("gsec"):
            near = jnp.concatenate([own, other_core(own)], 0)
        if not crossed:
            if inner == 1:
                return [near]
            return [lax.all_gather(near, "tensor", axis=0, tiled=True, axis_index_groups=groups)]
        if hop is None:
            with jax.named_scope("ghop"):
                hop = split.swap(own)
        with jax.named_scope("gsec2"):
            return [near, jnp.concatenate([hop, other_core(hop)], 0)]

    def scatter_begin(partials, gates=()):
        if not crossed:
            blocks = partials[0].reshape(inner, 2, rows, -1)
            ours, theirs = blocks[:, 0], blocks[:, 1].astype(bf16)
            total = (ours + other_core(theirs).astype(f32)).reshape(inner * rows, -1)
            return total.astype(bf16), None
        near, far = partials
        with jax.named_scope("ssec"):
            leaving = far[:rows] + other_core(far[rows:].astype(bf16)).astype(f32)
            leaving = gated(leaving, *gates)
        with jax.named_scope("ssec2"):
            staying = near[:rows] + other_core(near[rows:].astype(bf16)).astype(f32)
        return leaving.astype(bf16), staying

    def scatter_end(begun, split):
        leaving, staying = begun
        if not crossed:
            if inner == 1:
                return leaving.astype(f32)
            return lax.psum_scatter(
                leaving, "tensor", scatter_dimension=0, tiled=True, axis_index_groups=groups
            ).astype(f32)
        with jax.named_scope("shop"):
            return staying + split.swap(leaving).astype(f32)

    def scatter_all(begun, split):
        sums = [scatter_end(item, split) for item in begun]
        if not crossed:
            return sums
        return [
            gated(item, begun[p + 1][0]) if p + 1 < len(sums) else item
            for p, item in enumerate(sums)
        ]

    def cut(array):
        per_part = 2 * inner * rows
        per_group = 2 * rows if crossed else per_part
        return [
            [array[p * per_part + g : p * per_part + g + per_group] for g in range(0, per_part, per_group)]
            for p in range(parts)
        ]

    def joined(pieces):
        return jnp.concatenate([piece for part in pieces for piece in part], 0)

    def flat(pieces):
        return [piece for part in pieces for piece in part]

    def part_rows(array):
        return [array[p * rows : (p + 1) * rows] for p in range(parts)]

    def own_rows(array):
        mine = lax.dynamic_index_in_dim(array[:, 0], row, 0, False)
        theirs = lax.dynamic_index_in_dim(array[:, 0], 1 - row, 0, False)
        moved = route(theirs, lambda s, a, b: (s, 1 - a, b) if s == a else None)
        return mine, moved

    def fetch(weight, layer, split):
        def across(s, a, b):
            if s != layer:
                return None
            _, a2, b2 = split.across(s, a, b)
            return (split.keeper(s, a, b), a2, b2)

        def within(s, a, b):
            return (split.keeper(s, a, b), a, b) if s == layer else None

        return route(weight, within), route(weight, across)

    def chosen(weight, arrived, layer, split):
        near, far = arrived
        return jnp.where(split.home, jnp.where(section == layer, weight, near), far)

    attn_table = w_attn[0].reshape(width, -1)
    mlp_pack = jnp.concatenate([w_up[0], w_down[0].reshape(width, -1)], 1)

    def attn_unpack(pack):
        columns = w_attn.shape[2] * w_attn.shape[3]
        return pack[:, :columns], pack[:, columns:].reshape(w_out.shape[1:])

    def mlp_unpack(pack):
        columns = w_up.shape[2]
        return pack[:, :columns], pack[:, columns:].reshape(w_down.shape[1:])

    mine, moved = own_rows(tokens)
    own = part_rows(jnp.where(ByLane.home, mine, moved))
    hops = []
    if crossed:
        early = route(mine, lambda s, a, b: (s, a, 1 - b) if s == a else None)
        late = route(moved, lambda s, a, b: (s, a, 1 - b) if s != a else None)
        hops = part_rows(jnp.where(ByLane.home, early, late))
    attn_weights = [None] * sections
    mlp_weights = [None] * sections
    attn_pack = jnp.concatenate([attn_table, w_out[0].reshape(width, -1)], 1)
    with jax.named_scope("W0attn"):
        first_pack = chosen(attn_pack, fetch(attn_pack, 0, split_attn), 0, split_attn)
    with jax.named_scope("W0mlp"):
        arriving = fetch(after(mlp_pack, *own, *hops), 0, split_mlp)

    heads = w_attn.shape[3] // HEAD
    docs = lax.dynamic_index_in_dim(doc_ids[:, 0], row, 0, False)
    flags = lax.dynamic_index_in_dim(global_flags[:, 0], row, 0, False)
    order = jnp.stack([section, lane if crossed else jnp.zeros_like(lane)]).astype(jnp.int32)
    info = sequence_info(docs, flags, order, heads)
    first_pack, mlp_pack, *info = lax.optimization_barrier((first_pack, mlp_pack, *info))
    attn_weights[0] = attn_unpack(first_pack)

    gains_own = jnp.stack([ln_gain[0], ln_bias[0]])
    gains_other = other_core(gains_own)
    norms = [jnp.where(section == layer, gains_own, gains_other) for layer in range(sections)]

    saved, outputs, peaks = [], [], []
    for layer in range(sections):
        gains, shifts = norms[layer]
        attn_w, out_w = attn_weights[layer]
        with jax.named_scope(f"F{layer}in"):
            inputs = [
                gather(own[p], split_attn, hops[p] if layer == 0 and crossed else None)
                for p in range(parts)
            ]
            proj = [[mm(piece, attn_w, NN, bf16) for piece in part] for part in inputs]
        context, lse, glse, *tops = attend(flat(proj), info, plan)
        peaks.append(tops)
        if layer == 0:
            with jax.named_scope("W1attn"):
                pack = fetch(after(attn_pack, *flat(proj)), 1, split_attn)
            context, arriving, pack = lax.optimization_barrier((context, arriving, pack))
            mlp_weights[0] = mlp_unpack(chosen(mlp_pack, arriving, 0, split_mlp))
            attn_weights[1] = attn_unpack(chosen(attn_pack, pack, 1, split_attn))
        else:
            with jax.named_scope("W1mlp"):
                pack = fetch(after(mlp_pack, *flat(proj)), 1, split_mlp)
            with jax.named_scope("COT"):
                mine, moved = own_rows(after(cotangent, *flat(proj)))
            context, pack, mine, moved = lax.optimization_barrier((context, pack, mine, moved))
            mlp_weights[1] = mlp_unpack(chosen(mlp_pack, pack, 1, split_mlp))
            grad_out = part_rows(jnp.where(ByLane.home, mine, moved).astype(f32))
        up_w, down_w = mlp_weights[layer]
        with jax.named_scope(f"F{layer}out"):
            sums = scatter_all(
                [scatter_begin([mm(piece, out_w) for piece in part]) for part in cut(context)],
                split_attn,
            )
        hidden, hidden_low, norms_one = [], [], []
        for p in range(parts):
            with jax.named_scope(f"F{layer}norm1"):
                value = gated(sums[p], hidden_low[-1]) if p else sums[p]
                value, normed, scale = norm_forward(own[p].astype(f32) + value, gains[0], shifts[0])
                hidden.append(value)
                hidden_low.append(value.astype(bf16))
                norms_one.append((normed, scale))
        hidden_rows, acts, slopes, begun = [], [], [], []
        for p in range(parts):
            with jax.named_scope(f"F{layer}mlp{p}"):
                hidden_rows.append(gather(hidden_low[p], split_mlp))
                pairs = [gelu_pair(mm(piece, up_w)) for piece in hidden_rows[p]]
                acts.append([act for act, _ in pairs])
                slopes.append([slope for _, slope in pairs])
                begun.append(
                    scatter_begin([mm(act, down_w) for act in acts[p]], hidden_low[p + 1 : p + 2])
                )
        with jax.named_scope(f"F{layer}mlp"):
            sums = scatter_all(begun, split_mlp)
        outs, norms_two = [], []
        for p in range(parts):
            with jax.named_scope(f"F{layer}norm2"):
                value = gated(sums[p], outs[-1]) if p else sums[p]
                value, normed, scale = norm_forward(hidden[p] + value, gains[1], shifts[1])
                norms_two.append((normed, scale))
                outs.append(value.astype(bf16))
        own = outs
        outputs.append(jnp.concatenate(outs, 0))
        saved.append(
            (inputs, proj, context, (lse, glse), norms_one, hidden_rows, acts, slopes, norms_two)
        )

    def to_owner(upper, lower, split, gates=()):
        def first_link(s, a, b):
            if s == split.keeper(s, a, b):
                return (1 - s, a, b)
            return split.across(s, a, b)

        def second_link(s, a, b):
            if s == split.keeper(s, a, b):
                return None
            _, a2, b2 = split.across(s, a, b)
            return (1 - s, a2, b2)

        first = route(gated(jnp.where(split.home, lower, upper), *gates), first_link)
        second = route(lower, second_link)
        part = first.astype(f32) + jnp.where(split.home, upper, second).astype(f32)
        return part.astype(bf16)

    earlier = ()

    def dp_sum(*terms):
        nonlocal earlier
        terms = [after(term, *earlier) for term in terms]
        earlier = lax.psum(tuple(terms), "dp")
        return earlier

    def pick(values):
        return jnp.where(section == 0, values[0], values[1])

    def placed(chunk, layer):
        arrived = []
        for index in range(micro):
            moved = route(chunk, lambda s, a, b: (layer, s, b) if a == index else None)
            stays = (section == layer) & ByLane.home & (row == index)
            arrived.append(jnp.where(stays, chunk, moved))
        return arrived

    def send_attn(pack, gates):
        half = width // 2
        return to_owner(pack[:half], pack[half:], split_attn, gates)

    attn_sums = [None] * sections
    mlp_sums = [None] * sections
    norm_sums = [None] * sections
    out_rows = [None] * sections
    grad_rows = [None] * sections
    for layer in reversed(range(sections)):
        (attn_w, out_w), (up_w, down_w) = attn_weights[layer], mlp_weights[layer]
        gains, _ = norms[layer]
        inputs, proj, context, log_sums, norms_one, hidden_rows, acts, slopes, norms_two = saved[layer]
        grads_two, low, sums_two = [], [], []
        for p in range(parts):
            with jax.named_scope(f"B{layer}norm2"):
                value = gated(grad_out[p], low[-1]) if p else grad_out[p]
                value, sums = norm_backward(value, *norms_two[p], gains[1])
                grads_two.append(value)
                low.append(value.astype(bf16))
                sums_two.append(sums)
        grad_mlp, grad_up, begun = [], [], []
        for p in range(parts):
            with jax.named_scope(f"B{layer}mlp{p}"):
                grad_mlp.append(gather(low[p], split_mlp))
                grad_up.append(
                    [
                        (mm(piece, down_w, NT) * slope.astype(f32)).astype(bf16)
                        for piece, slope in zip(grad_mlp[p], slopes[p])
                    ]
                )
                begun.append(
                    scatter_begin([mm(piece, up_w, NT) for piece in grad_up[p]], low[p + 1 : p + 2])
                )
        with jax.named_scope(f"B{layer}mlp"):
            sums = scatter_all(begun, split_mlp)
        with jax.named_scope(f"B{layer}wmlp"):
            grad_up_w = mm(joined(hidden_rows), joined(grad_up), TN, bf16)
            grad_down_w = mm(joined(acts), joined(grad_mlp), TN, bf16)
            sums[-1] = gated(sums[-1], grad_up_w, grad_down_w)
        grads_one, low, sums_one = [], [], []
        for p in range(parts):
            with jax.named_scope(f"B{layer}norm1"):
                value = gated(sums[p], low[-1]) if p else sums[p]
                value, total = norm_backward(value + grads_two[p], *norms_one[p], gains[0])
                grads_one.append(value)
                low.append(value.astype(bf16))
                sums_one.append(total)
        norm_sums[layer] = (sums_one, sums_two)
        grad_attn, grad_context = [], []
        for p in range(parts):
            with jax.named_scope(f"B{layer}ctx{p}"):
                grad_attn.append(gather(low[p], split_attn))
                grad_context.append([mm(piece, out_w, NT, bf16) for piece in grad_attn[p]])
        with jax.named_scope(f"B{layer}wmlp"):
            mlp_parts = to_owner(
                grad_up_w.reshape(width, -1), grad_down_w.reshape(width, -1), split_mlp,
                flat(grad_context) if layer else low,
            )
        if layer == 0:
            *grad_context[-1], mlp_sums[1] = lax.optimization_barrier(
                (*grad_context[-1], mlp_sums[1])
            )
        grad_context = flat(grad_context)
        if layer == 0:
            with jax.named_scope("B1wattn"):
                attn_parts = send_attn(pack, grad_context)
            *grad_context, mlp_parts = lax.optimization_barrier((*grad_context, mlp_parts))
            mlp_sums[0] = dp_sum(mlp_parts)[0]
        grad_proj = attend_back(flat(proj), context, log_sums, grad_context, info, plan)
        if layer == 1:
            with jax.named_scope("OUTROWS"):
                ready = lax.optimization_barrier((*outputs, *grad_context))[:sections]
                for index in range(sections):
                    out_rows[index] = placed(ready[index], index)
        if layer == 1:
            grad_proj, mlp_parts = lax.optimization_barrier((grad_proj, mlp_parts))
            mlp_sums[1] = dp_sum(mlp_parts)[0]
        else:
            grad_proj, attn_parts = lax.optimization_barrier((grad_proj, attn_parts))
        with jax.named_scope(f"B{layer}wattn"):
            grad_attn_w = mm(joined(inputs), grad_proj, TN, bf16)
            grad_out_w = mm(context, joined(grad_attn), TN, bf16)
            pack = jnp.concatenate([grad_attn_w, grad_out_w.reshape(width, -1)], 1)
        if layer == 0:
            grad_proj = after(grad_proj, pack)
        grad_low = []
        grad_proj_parts = cut(grad_proj)
        if layer == 0:
            *grad_proj_parts[-1], mlp_sums[0] = lax.optimization_barrier(
                (*grad_proj_parts[-1], mlp_sums[0])
            )
        with jax.named_scope(f"B{layer}in"):
            sums = scatter_all(
                [
                    scatter_begin(
                        [mm(piece, attn_w, NT) for piece in part],
                        (),
                    )
                    for part in grad_proj_parts
                ],
                split_attn,
            )
        for p in range(parts):
            with jax.named_scope(f"B{layer}in"):
                value = gated(sums[p], grad_low[-1]) if p else sums[p]
                grad_low.append((value + grads_one[p]).astype(bf16))
        grad_out = [piece.astype(f32) for piece in grad_low]
        if layer == 0:
            with jax.named_scope("B0wattn"):
                last_parts = send_attn(pack, ())
                attn_sums[1], attn_sums[0] = dp_sum(attn_parts, last_parts)
        with jax.named_scope("GRADROWS"):
            grad_rows[layer] = placed(jnp.concatenate(grad_low, 0), layer)

    def stacked_rows(by_layer):
        return jnp.stack([pick([by_layer[0][m], by_layer[1][m]]) for m in range(micro)])[None, :, None]

    def placed_weight(terms, split):
        mine = pick(terms)
        theirs = other_core(pick(terms[::-1]))
        first = jnp.where(split.home, mine, theirs)
        second = jnp.where(split.home, theirs, mine)
        return first.astype(f32), second.astype(f32)

    def dp_butterfly(value, combine):
        if copies & (copies - 1):
            gathered = lax.all_gather(value, "dp", axis=0)
            total = gathered[0]
            for index in range(1, copies):
                total = combine(total, gathered[index])
            return total
        distance = 1
        while distance < copies:
            pairs = [(d, d ^ distance) for d in range(copies)]
            value = combine(value, lax.ppermute(value, "dp", pairs))
            distance *= 2
        return value

    with jax.named_scope("NORMSUM"):
        mine = [
            jnp.stack([sum(sums_one[1:], sums_one[0]), sum(sums_two[1:], sums_two[0])])
            for sums_one, sums_two in norm_sums
        ]
        mine = [gated(term, grad_low[-1]) for term in mine]
        norm_sum = pick(mine) + other_core(pick(mine[::-1]))
        if crossed:
            norm_sum = norm_sum + other_row(norm_sum)
            norm_sum = norm_sum + other_lane(norm_sum)
        else:
            norm_sum = lax.psum(norm_sum, "tensor")
        norm_sum = dp_butterfly(norm_sum, jnp.add)
    with jax.named_scope("PEAK"):
        peak_all = [gated(value, grad_low[-1]) for value in flat(peaks)]
        peak_all = jnp.stack(
            [jnp.max(value.reshape(heads, -1), 1) for value in peak_all]
        ).reshape(sections, 2, heads)
        peak_all = jnp.maximum(peak_all, other_row(peak_all))
        peak_all = dp_butterfly(peak_all, jnp.maximum)
        peak_here = jnp.where(ByLane.home, pick(peak_all), other_core(pick(peak_all[::-1])))
    factors = jnp.sqrt(clip_limit / jnp.maximum(peak_here, clip_limit))
    columns = jnp.repeat(factors, HEAD, axis=1)
    clipped = clip_weights(w_attn[0].transpose(1, 0, 2), columns[:, None, :])
    out_rows, grad_rows = stacked_rows(out_rows), stacked_rows(grad_rows)
    grad_up_w, grad_down_w = placed_weight(mlp_sums, split_mlp)
    attn_sums = [
        gated(term, out_rows, grad_rows, grad_up_w, grad_down_w, norm_sum, clipped)
        for term in attn_sums
    ]
    mine, theirs = pick(attn_sums), other_core(pick(attn_sums[::-1]))
    blocks, each = w_attn.shape[2:]
    home = split_attn.home.astype(jnp.int32).reshape(1)
    grad_attn_w = unpack(home, mine, theirs, blocks, each).transpose(1, 0, 2)
    halves = [half[:, blocks * each :].reshape(-1, w_out.shape[2]) for half in (mine, theirs)]
    grad_out_w = jnp.where(
        split_attn.home, jnp.concatenate(halves, 0), jnp.concatenate(halves[::-1], 0)
    ).astype(f32)

    return (
        out_rows,
        grad_rows,
        grad_attn_w[None],
        grad_out_w.reshape(w_out.shape),
        grad_up_w.reshape(w_up.shape),
        grad_down_w.reshape(w_down.shape),
        norm_sum[:, 0][None],
        norm_sum[:, 1][None],
        clipped[None],
    )


def solution(mesh):
    in_specs = (
        P(None, "dp", "tensor", None),
        P(None, "dp", "tensor", None),
        P(None, "dp", None),
        P(None, "dp", None),
        P("section", None, None, "tensor"),
        P("section", "tensor", None),
        P("section", None, "tensor"),
        P("section", "tensor", None),
        P("section", None, None),
        P("section", None, None),
    )
    out_specs = (
        P("section", None, "dp", "tensor", None),
        P("section", None, "dp", "tensor", None),
        P("section", None, None, "tensor"),
        P("section", "tensor", None),
        P("section", None, "tensor"),
        P("section", "tensor", None),
        P("section", None, None),
        P("section", None, None),
        P("section", None, None, "tensor"),
    )
    return jax.shard_map(shards, mesh=mesh, in_specs=in_specs, out_specs=out_specs, check_vma=False)
```
